8 devices in a mesh: dp: 1 (over z), sp: 2 (over y), cp: 4 (over x, core).
Axes of the slice: x: 2, y: 2, z: 1, core: 2. Of those that a mesh axis runs over, the one named last changes fastest.
Arguments:
- x_act: bfloat16 [32, 96, 14, 1024], P('dp', 'sp', None, 'cp')
- w_one: bfloat16 [3, 3, 1024, 4096], P(None, None, 'cp')
- w_two: bfloat16 [3, 3, 4096, 1024], P(None, None, 'cp')
- bias_one: float32 [4096], replicated
Outputs:
- output: bfloat16 [32, 96, 14, 1024], P('dp', 'sp', None, 'cp')
All inputs are finite; a program needn't handle non-finite values.
Results may differ from the reference program's by a relative error of at most 0.001.
Values are sent between devices in bfloat16 or wider.
A program may use at most 1 GiB of HBM per device.

```python
import jax
import jax.numpy as jnp
from jax import lax

BATCH_SIZE = 32
GRID_ROWS = 96
GRID_COLS = 14
CHANNELS = 1024
HIDDEN_CHANNELS = 4 * CHANNELS
CONV_DIMS = ("NHWC", "HWIO", "NHWC")


def setup_inputs(seed: int = 0, part: int = 0) -> dict:
    base_key = jax.random.key(seed)
    key_x, key_one, key_two, key_bias = jax.random.split(base_key, 4)
    x_act = jax.random.normal(jax.random.fold_in(key_x, part), (BATCH_SIZE, GRID_ROWS, GRID_COLS, CHANNELS), jnp.float32)
    w_one = jax.random.normal(key_one, (3, 3, CHANNELS, HIDDEN_CHANNELS), jnp.float32) * (9 * CHANNELS) ** -0.5
    w_two = jax.random.normal(key_two, (3, 3, HIDDEN_CHANNELS, CHANNELS), jnp.float32) * (9 * HIDDEN_CHANNELS) ** -0.5
    bias_one = 0.7 * jax.random.normal(key_bias, (HIDDEN_CHANNELS,), jnp.float32)
    return {"x_act": x_act.astype(jnp.bfloat16), "w_one": w_one.astype(jnp.bfloat16), "w_two": w_two.astype(jnp.bfloat16), "bias_one": bias_one}


def reference(x_act, w_one, w_two, bias_one):
    w_first = w_one.astype(jnp.float32)
    w_second = w_two.astype(jnp.float32)

    def one_picture(picture):
        pic_f32 = picture.astype(jnp.float32)[None]
        pre_act = lax.conv_general_dilated(pic_f32, w_first, (1, 1), "SAME", dimension_numbers=CONV_DIMS)
        hidden = jax.nn.relu(pre_act + bias_one).astype(jnp.bfloat16)
        post_act = lax.conv_general_dilated(hidden.astype(jnp.float32), w_second, (1, 1), "SAME", dimension_numbers=CONV_DIMS)
        return (pic_f32 + post_act)[0].astype(jnp.bfloat16)

    return lax.map(one_picture, x_act)
```

```python
import functools

import jax
import jax.numpy as jnp
from jax import lax
from jax.experimental import pallas as pl
from jax.experimental.pallas import tpu as pltpu
from jax.sharding import PartitionSpec as P

MESH = pl.DeviceIdType.MESH
N_STEPS = 64


def fused_block(xt, w_one, w_two, bias):
    groups, h_loc, cols, ni, cb = xt.shape
    rows = h_loc // 2
    m_rows = rows * ni
    tile = 2 * cb

    def remote(src, dst, send_sem, recv_sem, sp, cp):
        return pltpu.make_async_remote_copy(src_ref=src, dst_ref=dst, send_sem=send_sem, recv_sem=recv_sem,
                                            device_id={"sp": sp, "cp": cp}, device_id_type=MESH)

    def kernel(xt, w1, w2, b1, yt, g1, g2, part, hid,
               xa, acc, wv, stage,
               wsem, asem, pst, pld, stl, zsem, xl, xs, xr, hs, hr,
               p1s, p1r, x1s, x1r, y1s, y1r, f1s, f1r,
               p2s, p2r, x2s, x2r, y2s, y2r, f2s, f2r,
               as_, ar, ys, yr, zs, zr, yl):
        sp = lax.axis_index("sp")
        k = lax.axis_index("cp")
        x = lax.div(k, 2)
        c = lax.rem(k, 2)
        blk = 2 * sp + c
        osp = 1 - sp
        k1 = 2 * x + (1 - c)
        k2 = 2 * (1 - x) + c
        k3 = 2 * (1 - x) + (1 - c)

        def tile_of(xx, j, par):
            return 4 * lax.rem(xx + lax.div(j, 2), 2) + 2 * lax.rem(j, 2) + par

        barrier = pltpu.get_barrier_semaphore()
        for d_sp in range(2):
            for d_cp in range(4):
                if d_sp or d_cp:
                    pl.semaphore_signal(barrier, inc=1, device_id={"sp": lax.rem(sp + d_sp, 2), "cp": lax.rem(k + d_cp, 4)},
                                        device_id_type=MESH)
        pl.semaphore_wait(barrier, 7)

        def x_copy(role):
            cc = c if role in (0, 2) else 1 - c
            xx = x if role < 2 else 1 - x
            src = xt.at[xx, pl.ds((rows - 1) * cc, rows + 1)]
            dst = xa.at[role, pl.ds(1 - cc, rows + 1)]
            if role == 0:
                return pltpu.make_async_copy(src, dst, xl.at[0])
            return remote(src, dst, xs.at[role - 1], xr.at[role - 1], sp, {1: k1, 2: k2, 3: k3}[role])

        def halo_copy(xx):
            role = 2 * lax.rem(x + xx, 2) + lax.rem(c + sp, 2)
            return remote(xt.at[xx, (h_loc - 1) * osp], xa.at[role, (rows + 1) * sp], hs.at[xx], hr.at[role], osp, 2 * xx + sp)

        half = cb // 2

        def w1_own(j, par, xx):
            return w1.at[:, :, :, pl.ds(pl.multiple_of(tile_of(xx, j, par) * tile, tile), tile)]

        def w1_part(j, par):
            return remote(w1_own(j, par, x), g1.at[0, j, par], p1s.at[j, par], p1r.at[j, par], sp, k1)

        def w1_x(j, hf):
            cut = pl.ds(pl.multiple_of(hf * half, half), half)
            src = w1.at[:, :, cut, pl.ds(pl.multiple_of(tile_of(1 - x, j, sp) * tile, tile), tile)]
            return remote(src, g1.at[1, j, sp, :, :, cut], x1s.at[j, hf], x1r.at[j, hf], sp, k2)

        def w1_y(j, hf):
            cut = pl.ds(pl.multiple_of(hf * half, half), half)
            ref = g1.at[1, j, sp, :, :, cut]
            return remote(ref, ref, y1s.at[j, hf], y1r.at[j, hf], osp, k)

        def w1_fwd(j, par, hf):
            cut = pl.ds(pl.multiple_of(hf * half, half), half)
            return remote(g1.at[1, j, par, :, :, cut], g1.at[2, j, par, :, :, cut], f1s.at[j, par, hf], f1r.at[j, par, hf], sp, k1)

        def w2_cut(n, par, h, xx):
            row = pl.multiple_of(par * tile + h * cb, cb)
            col = pl.multiple_of(tile * lax.rem(1 + xx + n, 2), tile)
            return w2.at[:, :, pl.ds(row, cb), pl.ds(col, tile)]

        def w2_part(n, par, h):
            return remote(w2_cut(n, par, h, x), g2.at[0, n, par, h], p2s.at[n, par, h], p2r.at[n, par, h], sp, k1)

        def w2_x(n, h):
            return remote(w2_cut(n, sp, h, 1 - x), g2.at[1, n, sp, h], x2s.at[n, h], x2r.at[n, h], sp, k2)

        def w2_y(n, h):
            ref = g2.at[1, n, sp, h]
            return remote(ref, ref, y2s.at[n, h], y2r.at[n, h], osp, k)

        def w2_fwd(n, par, h):
            return remote(g2.at[1, n, par, h], g2.at[2, n, par, h], f2s.at[n, par, h], f2r.at[n, par, h], sp, k1)

        up_blk = lax.max(blk - 1, 0)
        dn_blk = lax.min(blk + 1, 3)

        def hid_up(q, h):
            return remote(stage.at[h, 0], hid.at[q, rows + 1], as_.at[0, h], ar.at[1, q], lax.div(up_blk, 2), 2 * x + lax.rem(up_blk, 2))

        def hid_dn(q, h):
            return remote(stage.at[h, rows - 1], hid.at[q, 0], as_.at[1, h], ar.at[0, q], lax.div(dn_blk, 2), 2 * x + lax.rem(dn_blk, 2))

        def hid_store(q, h):
            return pltpu.make_async_copy(stage.at[h], hid.at[q, pl.ds(1, rows)], stl.at[h])

        y_rows = pl.ds(rows * c, rows)

        def y_far(h):
            return remote(stage.at[h], yt.at[x, y_rows], ys.at[h], yr.at[lax.rem(h + c, 2)], sp, 2 * (1 - x) + h)

        def y_near():
            return remote(stage.at[1 - c], yt.at[x, y_rows], zs.at[0], zr.at[0], sp, k1)

        def y_own():
            return pltpu.make_async_copy(stage.at[c], yt.at[x, y_rows], yl.at[0])

        def zero_rows(row):
            return pltpu.make_async_copy(stage.at[0, pl.ds(0, 16)], hid.at[:, row], zsem.at[0])

        x_copy(0).start()
        for xx in range(2):
            halo_copy(xx).start()
        x_copy(1).start()

        def p_of(m):
            return lax.rem(m + 2, 8)

        def jp(p):
            return lax.div(p, 2), lax.rem(sp + lax.rem(p, 2), 2)

        for m in range(3):
            w1_part(*jp(jnp.int32((m + 2) % 8))).start()
        for hf in range(2):
            w1_x(0, hf).start()

        stage[0, 0:16] = jnp.zeros((16, cols, ni, cb), jnp.bfloat16)

        @pl.when(blk == 0)
        def _():
            xa[0:4, 0] = jnp.zeros((4, cols, ni, cb), jnp.bfloat16)
            zero_rows(0).start()

        @pl.when(blk == 3)
        def _():
            xa[0:4, rows + 1] = jnp.zeros((4, cols, ni, cb), jnp.bfloat16)
            zero_rows(rows + 1).start()

        def w_load(src, t):
            return pltpu.make_async_copy(src, wv.at[lax.rem(t, 2)], wsem.at[lax.rem(t, 2)])

        def hid_load(a, q):
            slot = lax.rem(q, 2)
            return pltpu.make_async_copy(hid.at[a], xa.at[4 + slot], asem.at[slot])

        def issue(t):
            @pl.when(t < 16)
            def _():
                j, par = jp(p_of(lax.div(t, 2)))

                @pl.when(lax.rem(t, 2) == 0)
                def _():
                    w_load(w1_own(j, par, x), t).start()

                @pl.when(lax.rem(t, 2) == 1)
                def _():
                    w1_part(j, par).wait_recv()
                    w_load(g1.at[0, j, par], t).start()

            @pl.when((t >= 16) & (t < 32))
            def _():
                j, par = jp(lax.div(t - 16, 2))

                @pl.when(lax.rem(t, 2) == 1)
                def _():
                    for hf in range(2):
                        w1_fwd(j, par, hf).wait_recv()

                w_load(g1.at[1 + lax.rem(t, 2), j, par], t).start()

            @pl.when((t >= 32) & (t < N_STEPS))
            def _():
                n = lax.div(t - 32, 16)
                q = lax.rem(t - 32, 16)
                h = lax.rem(q, 2)
                p = lax.div(q, 2)
                j, par = jp(p)
                a = 4 * j + 2 * par + h
                same = lax.rem(j, 2) == c

                @pl.when((n == 0) & (blk > 0))
                def _():
                    hid_dn(a, h).wait_recv()

                @pl.when((n == 0) & (blk < 3))
                def _():
                    hid_up(a, h).wait_recv()

                hid_load(a, q).start()

                @pl.when((p < 4) & same)
                def _():
                    w_load(w2_cut(n, par, h, x), t).start()

                @pl.when((p < 4) & jnp.logical_not(same))
                def _():
                    w2_part(n, par, h).wait_recv()
                    w_load(g2.at[0, n, par, h], t).start()

                @pl.when((p >= 4) & same)
                def _():
                    w_load(g2.at[1, n, par, h], t).start()

                @pl.when((p >= 4) & jnp.logical_not(same))
                def _():
                    w2_fwd(n, par, h).wait_recv()
                    w_load(g2.at[2, n, par, h], t).start()

        issue(jnp.int32(0))
        x_copy(0).wait()

        @pl.when(c != sp)
        def _():
            for role in range(4):
                remote(xt.at[0, 0], xa.at[role, 0], hs.at[0], hr.at[role], osp, k).wait_recv()

        def events(i):
            @pl.when((lax.rem(i, 2) == 0) & (i < 10))
            def _():
                w1_part(*jp(p_of(lax.div(i, 2) + 3))).start()

            @pl.when(i == 1)
            def _():
                x_copy(1).wait_recv()

            @pl.when(i == 3)
            def _():
                x_copy(2).start()

            @pl.when(i == 7)
            def _():
                x_copy(3).start()

            @pl.when((i == 13) | (i == 17) | (i == 21))
            def _():
                j = lax.div(i - 8, 4)
                for hf in range(2):
                    w1_x(j, hf).start()

            @pl.when((i == 24) | (i == 28) | (i == 32) | (i == 36))
            def _():
                e = lax.div(i - 24, 4)
                w2_x(lax.div(e, 2), lax.rem(e, 2)).start()

            @pl.when((i >= 18) & (i < 26))
            def _():
                e = i - 18
                w2_part(lax.div(e, 4), lax.rem(lax.div(e, 2), 2), lax.rem(e, 2)).start()

            @pl.when(i == 6)
            def _():
                for hf in range(2):
                    w1_x(0, hf).wait_recv()
                    w1_y(0, hf).start()
                    w1_fwd(0, sp, hf).start()

            @pl.when((i >= 17) & (i < 28) & (lax.rem(i, 2) == 1))
            def _():
                e = lax.div(i - 13, 2)
                j = lax.div(e, 2)
                hf = lax.rem(e, 2)
                w1_x(j, hf).wait_recv()
                w1_y(j, hf).start()
                w1_fwd(j, sp, hf).start()

            @pl.when((i == 31) | (i == 35) | (i == 39) | (i == 44))
            def _():
                e = lax.div(i - 31, 4)
                w2_x(lax.div(e, 2), lax.rem(e, 2)).wait_recv()
                w2_y(lax.div(e, 2), lax.rem(e, 2)).start()
                w2_fwd(lax.div(e, 2), sp, lax.rem(e, 2)).start()

            @pl.when(i == 11)
            def _():
                for hf in range(2):
                    w1_y(0, hf).wait_recv()
                    w1_fwd(0, osp, hf).start()

            @pl.when((i == 20) | (i == 24) | (i == 28))
            def _():
                j = lax.div(i - 16, 4)
                w1_y(j, 0).wait_recv()
                w1_fwd(j, osp, 0).start()

            @pl.when((i == 21) | (i == 25) | (i == 29))
            def _():
                j = lax.div(i - 17, 4)
                w1_y(j, 1).wait_recv()
                w1_fwd(j, osp, 1).start()

            @pl.when((i == 36) | (i == 40) | (i == 45) | (i == 49))
            def _():
                e = lax.div(i - 36, 4)
                w2_y(lax.div(e, 2), lax.rem(e, 2)).wait_recv()
                w2_fwd(lax.div(e, 2), osp, lax.rem(e, 2)).start()

            stored = (i >= 19) & (i <= 33) & (lax.rem(i, 2) == 1)

            @pl.when(stored)
            def _():
                for h in range(2):
                    hid_store(0, h).wait()

            @pl.when(stored & (blk > 0))
            def _():
                for h in range(2):
                    hid_up(0, h).wait_send()

            @pl.when(stored & (blk < 3))
            def _():
                for h in range(2):
                    hid_dn(0, h).wait_send()

            @pl.when(i == 16)
            def _():
                x_copy(2).wait_recv()

            @pl.when(i == 17)
            def _():
                x_copy(3).wait_recv()

        def taps(xs_slot, ws_slot, col):
            total = None
            for dx in (-1, 0, 1):
                if not 0 <= col + dx < cols:
                    continue
                for dy in range(3):
                    lhs = xa[xs_slot, dy:dy + rows, col + dx].reshape(m_rows, cb)
                    prod = jnp.dot(lhs, wv[ws_slot, dy, dx + 1], preferred_element_type=jnp.float32)
                    total = prod if total is None else total + prod
            return total

        def step(i, carry):
            ph3 = i >= 32
            odd = lax.rem(i, 2) == 1
            n = jnp.where(ph3, lax.div(i - 32, 16), 0)
            q = jnp.where(ph3, lax.rem(i - 32, 16), 0)
            m = lax.div(i, 2)
            p = jnp.where(i < 16, p_of(m), lax.rem(m, 8))
            last = jnp.where(ph3, q == 15, (i >= 16) & odd)
            first = jnp.where(ph3, q == 0, (i < 16) & jnp.logical_not(odd))
            a_slot = jnp.where(ph3, n, lax.rem(p, 2))
            x_slot = jnp.where(ph3, 4 + lax.rem(q, 2), jnp.where(i < 16, 0, 2) + lax.rem(i, 2))
            w_slot = lax.rem(i, 2)

            events(i)
            issue(i + 1)
            w_load(g1.at[0, 0, 0], i).wait()

            @pl.when(ph3)
            def _():
                hid_load(0, q).wait()

            @pl.when((i >= 4) & (i < 16) & jnp.logical_not(odd))
            def _():
                pltpu.make_async_copy(acc.at[a_slot], part.at[0], pst.at[a_slot]).wait()

            @pl.when((i >= 20) & (i < 32) & jnp.logical_not(odd))
            def _():
                pltpu.make_async_copy(part.at[0], acc.at[a_slot], pld.at[a_slot]).wait()

            @pl.when(jnp.logical_not(last))
            def _():
                for col in range(cols):
                    total = taps(x_slot, w_slot, col)
                    acc[a_slot, col] = total + jnp.where(first, 0.0, acc[a_slot, col])

            @pl.when((i < 12) & odd)
            def _():
                pltpu.make_async_copy(acc.at[a_slot], part.at[p], pst.at[a_slot]).start()

            @pl.when(last)
            def _():
                @pl.when((i == 17) & ((blk == 0) | (blk == 3)))
                def _():
                    zero_rows(0).wait()

                @pl.when(i == 63)
                def _():
                    for h in range(2):
                        y_far(h).wait_send()

                keep = jnp.where(ph3, 1.0, 0.0)
                floor = jnp.where(ph3, -jnp.inf, 0.0)
                j, par = jp(p)
                shift = b1[tile_of(x, j, par)] * (1.0 - keep)
                role0 = jnp.where(n == 0, 2, 0)
                for col in range(cols):
                    total = taps(x_slot, w_slot, col) + acc[a_slot, col] + shift
                    for h in range(2):
                        role = role0 + lax.rem(c + h, 2)
                        res = xa[role, 1:rows + 1, col].reshape(m_rows, cb).astype(jnp.float32)
                        val = jnp.maximum(total[:, h * cb:(h + 1) * cb] + res * keep, floor)
                        stage[h, :, col] = val.astype(jnp.bfloat16).reshape(rows, ni, cb)

                @pl.when(i < 32)
                def _():
                    a = 4 * j + 2 * par
                    for h in range(2):
                        hid_store(a + h, h).start()

                    @pl.when(blk > 0)
                    def _():
                        for h in range(2):
                            hid_up(a + h, h).start()

                    @pl.when(blk < 3)
                    def _():
                        for h in range(2):
                            hid_dn(a + h, h).start()

                    @pl.when(p < 6)
                    def _():
                        pltpu.make_async_copy(part.at[p + 2], acc.at[a_slot], pld.at[a_slot]).start()

                @pl.when(i == 47)
                def _():
                    for h in range(2):
                        y_far(h).start()

                @pl.when(i == 63)
                def _():
                    y_near().start()
                    y_own().start()

            return carry

        lax.fori_loop(0, N_STEPS, step, 0)

        for role in range(1, 4):
            x_copy(role).wait_send()
        for xx in range(2):
            halo_copy(xx).wait_send()

        def drain(e, carry):
            hi, lo = lax.div(e, 2), lax.rem(e, 2)
            w1_part(hi, lo).wait_send()
            w1_x(hi, lo).wait_send()
            w1_y(hi, lo).wait_send()
            for hf in range(2):
                w1_fwd(hi, lo, hf).wait_send()
            n, par = lax.div(e, 4), lax.rem(lax.div(e, 2), 2)
            w2_part(n, par, lo).wait_send()
            w2_fwd(n, par, lo).wait_send()
            return carry

        lax.fori_loop(0, 8, drain, 0)

        def drain_two(e, carry):
            w2_x(lax.div(e, 2), lax.rem(e, 2)).wait_send()
            w2_y(lax.div(e, 2), lax.rem(e, 2)).wait_send()
            return carry

        lax.fori_loop(0, 4, drain_two, 0)
        for e in range(2):
            remote(stage.at[0], yt.at[0, pl.ds(0, rows)], ys.at[0], yr.at[e], sp, k).wait_recv()
        y_near().wait()
        y_own().wait()

    dma = pltpu.SemaphoreType.DMA
    bf16, f32 = jnp.bfloat16, jnp.float32
    any_space = pl.BlockSpec(memory_space=pl.ANY)
    outs = pl.pallas_call(
        kernel,
        out_shape=[
            jax.ShapeDtypeStruct(xt.shape, bf16),
            jax.ShapeDtypeStruct((3, 4, 2, 3, 3, cb, tile), bf16),
            jax.ShapeDtypeStruct((3, 2, 2, 2, 3, 3, cb, tile), bf16),
            jax.ShapeDtypeStruct((8, cols, m_rows, tile), f32),
            jax.ShapeDtypeStruct((16, rows + 2, cols, ni, cb), bf16),
        ],
        in_specs=[any_space, any_space, any_space, pl.BlockSpec(memory_space=pltpu.VMEM)],
        out_specs=[any_space] * 5,
        scratch_shapes=[
            pltpu.VMEM((6, rows + 2, cols, ni, cb), bf16),
            pltpu.VMEM((2, cols, m_rows, tile), f32),
            pltpu.VMEM((2, 3, 3, cb, tile), bf16),
            pltpu.VMEM((2, rows, cols, ni, cb), bf16),
            dma((2,)), dma((2,)), dma((2,)), dma((2,)), dma((2,)), dma((1,)), dma((1,)), dma((3,)), dma((3,)), dma((2,)), dma((4,)),
            dma((4, 2)), dma((4, 2)), dma((4, 2)), dma((4, 2)), dma((4, 2)), dma((4, 2)), dma((4, 2, 2)), dma((4, 2, 2)),
            dma((2, 2, 2)), dma((2, 2, 2)), dma((2, 2)), dma((2, 2)), dma((2, 2)), dma((2, 2)), dma((2, 2, 2)), dma((2, 2, 2)),
            dma((2, 2)), dma((2, 16)), dma((2,)), dma((2,)), dma((1,)), dma((1,)), dma((1,)),
        ],
        compiler_params=pltpu.CompilerParams(collective_id=0, has_side_effects=True, vmem_limit_bytes=60 * 1024 * 1024),
        name="fused_block",
    )(xt, w_one, w_two, bias)
    return outs[0]


def solution(mesh):
    act_spec = P("dp", "sp", None, "cp")
    kernel_spec = P(None, None, "cp", None)

    def local_block(x_tile, w_one_part, w_two_part, bias_one):
        images, h_loc, cols, cb = x_tile.shape
        ni = images // 2
        xt = x_tile.reshape(2, ni, h_loc, cols, cb).transpose(0, 2, 3, 1, 4)
        yt = fused_block(xt, w_one_part, w_two_part, bias_one.reshape(8, 1, 2 * cb))
        return yt.transpose(0, 3, 1, 2, 4).reshape(x_tile.shape)

    return jax.shard_map(local_block, mesh=mesh, in_specs=(act_spec, kernel_spec, kernel_spec, P()), out_specs=act_spec, check_vma=False)
```

```python
import functools

import jax
import jax.numpy as jnp
from jax import lax
from jax.experimental import pallas as pl
from jax.experimental.pallas import tpu as pltpu
from jax.sharding import PartitionSpec as P

MESH = pl.DeviceIdType.MESH
N_STEPS = 64


def fused_block(xt, w_one, w_two, bias):
    groups, h_loc, cols, ni, cb = xt.shape
    rows = h_loc // 2
    m_rows = rows * ni
    tile = 2 * cb

    def remote(src, dst, send_sem, recv_sem, sp, cp):
        return pltpu.make_async_remote_copy(src_ref=src, dst_ref=dst, send_sem=send_sem, recv_sem=recv_sem,
                                            device_id={"sp": sp, "cp": cp}, device_id_type=MESH)

    def kernel(xt, w1, w2, b1, yt, g1, g2, part, hid,
               xa, acc, wv, stage,
               wsem, asem, pst, pld, stl, zsem, xl, xs, xr, hs, hr,
               p1s, p1r, x1s, x1r, y1s, y1r, f1s, f1r,
               p2s, p2r, x2s, x2r, y2s, y2r, f2s, f2r,
               as_, ar, ys, yr, zs, zr, yl):
        sp = lax.axis_index("sp")
        k = lax.axis_index("cp")
        x = lax.div(k, 2)
        c = lax.rem(k, 2)
        blk = 2 * sp + c
        osp = 1 - sp
        k1 = 2 * x + (1 - c)
        k2 = 2 * (1 - x) + c
        k3 = 2 * (1 - x) + (1 - c)

        def tile_of(xx, j, par):
            return 4 * lax.rem(xx + lax.div(j, 2), 2) + 2 * lax.rem(j, 2) + par

        barrier = pltpu.get_barrier_semaphore()
        for d_sp in range(2):
            for d_cp in range(4):
                if d_sp or d_cp:
                    pl.semaphore_signal(barrier, inc=1, device_id={"sp": lax.rem(sp + d_sp, 2), "cp": lax.rem(k + d_cp, 4)},
                                        device_id_type=MESH)
        pl.semaphore_wait(barrier, 7)

        def x_copy(role):
            cc = c if role in (0, 2) else 1 - c
            xx = x if role < 2 else 1 - x
            src = xt.at[xx, pl.ds((rows - 1) * cc, rows + 1)]
            dst = xa.at[role, pl.ds(1 - cc, rows + 1)]
            if role == 0:
                return pltpu.make_async_copy(src, dst, xl.at[0])
            return remote(src, dst, xs.at[role - 1], xr.at[role - 1], sp, {1: k1, 2: k2, 3: k3}[role])

        def halo_copy(xx):
            role = 2 * lax.rem(x + xx, 2) + lax.rem(c + sp, 2)
            return remote(xt.at[xx, (h_loc - 1) * osp], xa.at[role, (rows + 1) * sp], hs.at[xx], hr.at[role], osp, 2 * xx + sp)

        half = cb // 2

        def w1_own(j, par, xx):
            return w1.at[:, :, :, pl.ds(pl.multiple_of(tile_of(xx, j, par) * tile, tile), tile)]

        def w1_part(j, par):
            return remote(w1_own(j, par, x), g1.at[0, j, par], p1s.at[j, par], p1r.at[j, par], sp, k1)

        def w1_x(j, hf):
            cut = pl.ds(pl.multiple_of(hf * half, half), half)
            src = w1.at[:, :, cut, pl.ds(pl.multiple_of(tile_of(1 - x, j, sp) * tile, tile), tile)]
            return remote(src, g1.at[1, j, sp, :, :, cut], x1s.at[j, hf], x1r.at[j, hf], sp, k2)

        def w1_y(j, hf):
            cut = pl.ds(pl.multiple_of(hf * half, half), half)
            ref = g1.at[1, j, sp, :, :, cut]
            return remote(ref, ref, y1s.at[j, hf], y1r.at[j, hf], osp, k)

        def w1_fwd(j, par, hf):
            cut = pl.ds(pl.multiple_of(hf * half, half), half)
            return remote(g1.at[1, j, par, :, :, cut], g1.at[2, j, par, :, :, cut], f1s.at[j, par, hf], f1r.at[j, par, hf], sp, k1)

        def w2_cut(n, par, h, xx):
            row = pl.multiple_of(par * tile + h * cb, cb)
            col = pl.multiple_of(tile * lax.rem(1 + xx + n, 2), tile)
            return w2.at[:, :, pl.ds(row, cb), pl.ds(col, tile)]

        def w2_part(n, par, h):
            return remote(w2_cut(n, par, h, x), g2.at[0, n, par, h], p2s.at[n, par, h], p2r.at[n, par, h], sp, k1)

        def w2_x(n, h):
            return remote(w2_cut(n, sp, h, 1 - x), g2.at[1, n, sp, h], x2s.at[n, h], x2r.at[n, h], sp, k2)

        def w2_y(n, h):
            ref = g2.at[1, n, sp, h]
            return remote(ref, ref, y2s.at[n, h], y2r.at[n, h], osp, k)

        def w2_fwd(n, par, h):
            return remote(g2.at[1, n, par, h], g2.at[2, n, par, h], f2s.at[n, par, h], f2r.at[n, par, h], sp, k1)

        up_blk = lax.max(blk - 1, 0)
        dn_blk = lax.min(blk + 1, 3)

        def hid_up(a):
            return remote(hid.at[a, 1], hid.at[a, rows + 1], as_.at[0, a], ar.at[1, a], lax.div(up_blk, 2), 2 * x + lax.rem(up_blk, 2))

        def hid_dn(a):
            return remote(hid.at[a, rows], hid.at[a, 0], as_.at[1, a], ar.at[0, a], lax.div(dn_blk, 2), 2 * x + lax.rem(dn_blk, 2))

        def hid_store(a, h):
            return pltpu.make_async_copy(stage.at[h], hid.at[a, pl.ds(1, rows)], stl.at[h])

        y_rows = pl.ds(rows * c, rows)

        def y_far(h):
            return remote(stage.at[h], yt.at[x, y_rows], ys.at[h], yr.at[lax.rem(h + c, 2)], sp, 2 * (1 - x) + h)

        def y_near():
            return remote(stage.at[1 - c], yt.at[x, y_rows], zs.at[0], zr.at[0], sp, k1)

        def y_own():
            return pltpu.make_async_copy(stage.at[c], yt.at[x, y_rows], yl.at[0])

        def zero_rows(row):
            return pltpu.make_async_copy(stage.at[0, pl.ds(0, 16)], hid.at[:, row], zsem.at[0])

        def p_of(m):
            return lax.rem(m + 2, 8)

        def jp(p):
            return lax.div(p, 2), lax.rem(sp + lax.rem(p, 2), 2)

        def near_step(i):
            e = lax.rem(i, 4)
            return 2 * lax.div(i, 4) + lax.rem(e, 2), lax.div(e, 2)

        def halo_wait(role):
            @pl.when(c != sp)
            def _():
                remote(xt.at[0, 0], xa.at[role, 0], hs.at[0], hr.at[role], osp, k).wait_recv()

        x_copy(0).start()
        for xx in (x, 1 - x):
            halo_copy(xx).start()
        x_copy(1).start()
        for m in range(2):
            w1_part(*jp(jnp.int32((m + 2) % 8))).start()
        for e in range(3):
            w1_x(e // 2, e % 2).start()

        stage[0, 0:16] = jnp.zeros((16, cols, ni, cb), jnp.bfloat16)

        @pl.when(blk == 0)
        def _():
            xa[0:4, 0] = jnp.zeros((4, cols, ni, cb), jnp.bfloat16)
            zero_rows(0).start()

        @pl.when(blk == 3)
        def _():
            xa[0:4, rows + 1] = jnp.zeros((4, cols, ni, cb), jnp.bfloat16)
            zero_rows(rows + 1).start()

        def w_load(src, t):
            return pltpu.make_async_copy(src, wv.at[lax.rem(t, 2)], wsem.at[lax.rem(t, 2)])

        def hid_load(a, q):
            slot = lax.rem(q, 2)
            return pltpu.make_async_copy(hid.at[a], xa.at[4 + slot], asem.at[slot])

        def issue(t):
            @pl.when(t < 16)
            def _():
                m, role = near_step(t)
                j, par = jp(p_of(m))

                @pl.when(role == 0)
                def _():
                    w_load(w1_own(j, par, x), t).start()

                @pl.when(role == 1)
                def _():
                    w1_part(j, par).wait_recv()
                    w_load(g1.at[0, j, par], t).start()

            @pl.when((t >= 16) & (t < 32))
            def _():
                j, par = jp(lax.div(t - 16, 2))

                @pl.when(lax.rem(t, 2) == 1)
                def _():
                    for hf in range(2):
                        w1_fwd(j, par, hf).wait_recv()

                w_load(g1.at[1 + lax.rem(t, 2), j, par], t).start()

            @pl.when((t >= 32) & (t < N_STEPS))
            def _():
                n = lax.div(t - 32, 16)
                q = lax.rem(t - 32, 16)
                h = lax.rem(q, 2)
                p = lax.div(q, 2)
                j, par = jp(p)
                a = 4 * j + 2 * par + h
                same = lax.rem(j, 2) == c

                @pl.when(n == 0)
                def _():
                    @pl.when(blk > 0)
                    def _():
                        hid_dn(a).wait_recv()

                    @pl.when(blk < 3)
                    def _():
                        hid_up(a).wait_recv()

                hid_load(a, q).start()

                @pl.when(p < 4)
                def _():
                    @pl.when(same)
                    def _():
                        w_load(w2_cut(n, par, h, x), t).start()

                    @pl.when(jnp.logical_not(same))
                    def _():
                        w2_part(n, par, h).wait_recv()
                        w_load(g2.at[0, n, par, h], t).start()

                @pl.when(p >= 4)
                def _():
                    @pl.when(jnp.logical_not(same))
                    def _():
                        w2_fwd(n, par, h).wait_recv()

                    w_load(g2.at[jnp.where(same, 1, 2), n, par, h], t).start()

        issue(jnp.int32(0))
        x_copy(0).wait()
        halo_wait(0)

        def pass_w1_x(e):
            j, hf = lax.div(e, 2), lax.rem(e, 2)
            w1_x(j, hf).wait_recv()
            w1_y(j, hf).start()
            w1_fwd(j, sp, hf).start()

        def pass_w1_y(e):
            j, hf = lax.div(e, 2), lax.rem(e, 2)
            w1_y(j, hf).wait_recv()
            w1_fwd(j, osp, hf).start()

        def pass_w2_x(e):
            n, h = lax.div(e, 2), lax.rem(e, 2)
            w2_x(n, h).wait_recv()
            w2_y(n, h).start()
            w2_fwd(n, sp, h).start()

        def pass_w2_y(e):
            n, h = lax.div(e, 2), lax.rem(e, 2)
            w2_y(n, h).wait_recv()
            w2_fwd(n, osp, h).start()

        def send_w1_x(e):
            w1_x(lax.div(e, 2), lax.rem(e, 2)).start()

        def send_w2_x(e):
            w2_x(lax.div(e, 2), lax.rem(e, 2)).start()

        def events(i):
            even = lax.rem(i, 2) == 0
            odd = jnp.logical_not(even)

            @pl.when(i < 16)
            def _():
                @pl.when(even)
                def _():
                    @pl.when(i < 12)
                    def _():
                        w1_part(*jp(p_of(lax.div(i, 2) + 2))).start()

                    @pl.when(i == 2)
                    def _():
                        x_copy(1).wait_recv()
                        halo_wait(1)

                    @pl.when(i == 4)
                    def _():
                        x_copy(2).start()

                    @pl.when(i == 10)
                    def _():
                        for e in range(2):
                            pass_w1_y(jnp.int32(e))

                    @pl.when(i == 12)
                    def _():
                        pass_w1_y(jnp.int32(2))

                @pl.when(odd)
                def _():
                    @pl.when(i == 5)
                    def _():
                        for e in range(2):
                            pass_w1_x(jnp.int32(e))

                    @pl.when(i == 7)
                    def _():
                        pass_w1_x(jnp.int32(2))

                    @pl.when(i == 9)
                    def _():
                        x_copy(3).start()

                    @pl.when(i >= 13)
                    def _():
                        send_w1_x(lax.div(i - 7, 2))

            @pl.when((i >= 16) & (i < 34))
            def _():
                @pl.when(i < 24)
                def _():
                    e = i - 16
                    w2_part(lax.div(e, 4), lax.rem(lax.div(e, 2), 2), lax.rem(e, 2)).start()

                @pl.when(even)
                def _():
                    @pl.when(i == 16)
                    def _():
                        x_copy(2).wait_recv()
                        halo_wait(2)

                    @pl.when((i >= 24) & (lax.rem(i, 4) == 0))
                    def _():
                        send_w2_x(lax.div(i - 24, 4))

                    @pl.when((i >= 18) & (i <= 26))
                    def _():
                        pass_w1_x(lax.div(i - 12, 2))

                @pl.when(odd)
                def _():
                    @pl.when(i == 17)
                    def _():
                        x_copy(3).wait_recv()
                        halo_wait(3)

                    @pl.when(i <= 21)
                    def _():
                        send_w1_x(lax.div(i - 7, 2))

                    @pl.when(i >= 19)
                    def _():
                        for h in range(2):
                            hid_store(0, h).wait()

                    @pl.when((i >= 21) & (i <= 29))
                    def _():
                        pass_w1_y(lax.div(i - 15, 2))

                    @pl.when(i >= 27)
                    def _():
                        for d in range(2):
                            j, par = jp(i - 27 + d)
                            for h in range(2):
                                a = 4 * j + 2 * par + h

                                @pl.when(blk > 0)
                                def _():
                                    hid_up(a).start()

                                @pl.when(blk < 3)
                                def _():
                                    hid_dn(a).start()

                    @pl.when(i == 31)
                    def _():
                        pass_w2_x(jnp.int32(0))

            @pl.when((i >= 34) & (i < 50))
            def _():
                @pl.when(i == 36)
                def _():
                    send_w2_x(jnp.int32(3))

                @pl.when((i < 44) & (lax.rem(i, 4) == 3))
                def _():
                    pass_w2_x(lax.div(i - 31, 4))

                @pl.when((i >= 37) & (lax.rem(i, 4) == 1))
                def _():
                    pass_w2_y(lax.div(i - 37, 4))

        def taps(xs_slot, ws_slot, col):
            total = None
            for dx in (-1, 0, 1):
                if not 0 <= col + dx < cols:
                    continue
                for dy in range(3):
                    lhs = xa[xs_slot, dy:dy + rows, col + dx].reshape(m_rows, cb)
                    prod = jnp.dot(lhs, wv[ws_slot, dy, dx + 1], preferred_element_type=jnp.float32)
                    total = prod if total is None else total + prod
            return total

        def step(i, carry):
            ph1 = i < 16
            ph3 = i >= 32
            n = jnp.where(ph3, lax.div(i - 32, 16), 0)
            q = jnp.where(ph3, lax.rem(i - 32, 16), 0)
            m, role = near_step(i)
            m = jnp.where(ph1, m, lax.div(i - 16, 2))
            role = jnp.where(ph1, role, 2 + lax.rem(i, 2))
            p = jnp.where(ph1, p_of(m), lax.rem(m, 8))
            p = jnp.where(ph3, 0, p)
            last = jnp.where(ph3, q == 15, role == 3)
            first = jnp.where(ph3, q == 0, role == 0)
            a_slot = jnp.where(ph3, n, lax.rem(p, 2))
            x_slot = jnp.where(ph3, 4 + lax.rem(q, 2), role)
            w_slot = lax.rem(i, 2)

            events(i)
            issue(i + 1)
            w_load(g1.at[0, 0, 0], i).wait()

            @pl.when(ph3)
            def _():
                hid_load(0, q).wait()

            @pl.when((i >= 4) & (i < 32))
            def _():
                @pl.when(ph1 & first)
                def _():
                    pltpu.make_async_copy(acc.at[a_slot], part.at[0], pst.at[a_slot]).wait()

                @pl.when((i >= 20) & (role == 2))
                def _():
                    pltpu.make_async_copy(part.at[0], acc.at[a_slot], pld.at[a_slot]).wait()

            @pl.when(jnp.logical_not(last))
            def _():
                for col in range(cols):
                    total = taps(x_slot, w_slot, col)
                    acc[a_slot, col] = total + jnp.where(first, 0.0, acc[a_slot, col])

            @pl.when((i < 12) & (role == 1))
            def _():
                pltpu.make_async_copy(acc.at[a_slot], part.at[p], pst.at[a_slot]).start()

            @pl.when(last)
            def _():
                @pl.when((i == 17) & ((blk == 0) | (blk == 3)))
                def _():
                    zero_rows(0).wait()

                @pl.when(i == 63)
                def _():
                    for h in range(2):
                        y_far(h).wait_send()

                keep = jnp.where(ph3, 1.0, 0.0)
                floor = jnp.where(ph3, -jnp.inf, 0.0)
                j, par = jp(p)
                shift = b1[tile_of(x, j, par)] * (1.0 - keep)
                role0 = jnp.where(n == 0, 2, 0)
                for col in range(cols):
                    total = taps(x_slot, w_slot, col) + acc[a_slot, col] + shift
                    for h in range(2):
                        role = role0 + lax.rem(c + h, 2)
                        res = xa[role, 1:rows + 1, col].reshape(m_rows, cb).astype(jnp.float32)
                        val = jnp.maximum(total[:, h * cb:(h + 1) * cb] + res * keep, floor)
                        stage[h, :, col] = val.astype(jnp.bfloat16).reshape(rows, ni, cb)

                @pl.when(i < 32)
                def _():
                    for h in range(2):
                        hid_store(4 * j + 2 * par + h, h).start()

                    @pl.when(p < 6)
                    def _():
                        pltpu.make_async_copy(part.at[p + 2], acc.at[a_slot], pld.at[a_slot]).start()

                @pl.when(i == 47)
                def _():
                    for h in range(2):
                        y_far(h).start()

                @pl.when(i == 63)
                def _():
                    y_near().start()
                    y_own().start()

            return carry

        lax.fori_loop(0, N_STEPS, step, 0)

        for role in range(1, 4):
            x_copy(role).wait_send()
        for xx in range(2):
            halo_copy(xx).wait_send()

        def drain(e, carry):
            hi, lo = lax.div(e, 2), lax.rem(e, 2)
            w1_part(hi, lo).wait_send()
            w1_x(hi, lo).wait_send()
            w1_y(hi, lo).wait_send()
            for hf in range(2):
                w1_fwd(hi, lo, hf).wait_send()
            n, par = lax.div(e, 4), lax.rem(lax.div(e, 2), 2)
            w2_part(n, par, lo).wait_send()
            w2_fwd(n, par, lo).wait_send()
            return carry

        lax.fori_loop(0, 8, drain, 0)

        def drain_rows(a, carry):
            @pl.when(blk > 0)
            def _():
                hid_up(a).wait_send()

            @pl.when(blk < 3)
            def _():
                hid_dn(a).wait_send()

            return carry

        lax.fori_loop(0, 16, drain_rows, 0)

        def drain_two(e, carry):
            w2_x(lax.div(e, 2), lax.rem(e, 2)).wait_send()
            w2_y(lax.div(e, 2), lax.rem(e, 2)).wait_send()
            return carry

        lax.fori_loop(0, 4, drain_two, 0)
        for e in range(2):
            remote(stage.at[0], yt.at[0, pl.ds(0, rows)], ys.at[0], yr.at[e], sp, k).wait_recv()
        y_near().wait()
        y_own().wait()

    dma = pltpu.SemaphoreType.DMA
    bf16, f32 = jnp.bfloat16, jnp.float32
    any_space = pl.BlockSpec(memory_space=pl.ANY)
    outs = pl.pallas_call(
        kernel,
        out_shape=[
            jax.ShapeDtypeStruct(xt.shape, bf16),
            jax.ShapeDtypeStruct((3, 4, 2, 3, 3, cb, tile), bf16),
            jax.ShapeDtypeStruct((3, 2, 2, 2, 3, 3, cb, tile), bf16),
            jax.ShapeDtypeStruct((8, cols, m_rows, tile), f32),
            jax.ShapeDtypeStruct((16, rows + 2, cols, ni, cb), bf16),
        ],
        in_specs=[any_space, any_space, any_space, pl.BlockSpec(memory_space=pltpu.VMEM)],
        out_specs=[any_space] * 5,
        scratch_shapes=[
            pltpu.VMEM((6, rows + 2, cols, ni, cb), bf16),
            pltpu.VMEM((2, cols, m_rows, tile), f32),
            pltpu.VMEM((2, 3, 3, cb, tile), bf16),
            pltpu.VMEM((2, rows, cols, ni, cb), bf16),
            dma((2,)), dma((2,)), dma((2,)), dma((2,)), dma((2,)), dma((1,)), dma((1,)), dma((3,)), dma((3,)), dma((2,)), dma((4,)),
            dma((4, 2)), dma((4, 2)), dma((4, 2)), dma((4, 2)), dma((4, 2)), dma((4, 2)), dma((4, 2, 2)), dma((4, 2, 2)),
            dma((2, 2, 2)), dma((2, 2, 2)), dma((2, 2)), dma((2, 2)), dma((2, 2)), dma((2, 2)), dma((2, 2, 2)), dma((2, 2, 2)),
            dma((2, 16)), dma((2, 16)), dma((2,)), dma((2,)), dma((1,)), dma((1,)), dma((1,)),
        ],
        compiler_params=pltpu.CompilerParams(collective_id=0, has_side_effects=True, vmem_limit_bytes=60 * 1024 * 1024),
        name="fused_block",
    )(xt, w_one, w_two, bias)
    return outs[0]


def solution(mesh):
    act_spec = P("dp", "sp", None, "cp")
    kernel_spec = P(None, None, "cp", None)

    def local_block(x_tile, w_one_part, w_two_part, bias_one):
        images, h_loc, cols, cb = x_tile.shape
        ni = images // 2
        xt = x_tile.reshape(2, ni, h_loc, cols, cb).transpose(0, 2, 3, 1, 4)
        yt = fused_block(xt, w_one_part, w_two_part, bias_one.reshape(8, 1, 2 * cb))
        return yt.transpose(0, 3, 1, 2, 4).reshape(x_tile.shape)

    return jax.shard_map(local_block, mesh=mesh, in_specs=(act_spec, kernel_spec, kernel_spec, P()), out_specs=act_spec, check_vma=False)
```

```python
import functools

import jax
import jax.numpy as jnp
from jax import lax
from jax.experimental import pallas as pl
from jax.experimental.pallas import tpu as pltpu
from jax.sharding import PartitionSpec as P

MESH = pl.DeviceIdType.MESH
N_STEPS = 64


def swap_matrix(n):
    to = lax.broadcasted_iota(jnp.int32, (n * n, n * n), 0)
    frm = lax.broadcasted_iota(jnp.int32, (n * n, n * n), 1)
    hit = (lax.div(to, n) == lax.rem(frm, n)) & (lax.rem(to, n) == lax.div(frm, n))
    return jnp.where(hit, 1.0, 0.0).astype(jnp.bfloat16)


def fused_block(xw, w_one, w_two, bias):
    images, cols, h_loc, cb = xw.shape
    ni = images // 2
    rows = h_loc // 2
    m_rows = rows * ni
    tile = 2 * cb
    assert ni == 16 and h_loc == 48

    def remote(src, dst, send_sem, recv_sem, sp, cp):
        return pltpu.make_async_remote_copy(src_ref=src, dst_ref=dst, send_sem=send_sem, recv_sem=recv_sem,
                                            device_id={"sp": sp, "cp": cp}, device_id_type=MESH)

    def kernel(xw, w1, w2, b1, yt, g1, g2, part, hid,
               xa, acc, wv, stage, raw, swap,
               wsem, asem, pst, pld, stl, zsem, rsem, xs, xr, hs, hr,
               p1s, p1r, x1s, x1r, y1s, y1r, f1s, f1r,
               p2s, p2r, x2s, x2r, y2s, y2r, f2s, f2r,
               as_, ar, ys, yr, zs, zr, yl):
        sp = lax.axis_index("sp")
        k = lax.axis_index("cp")
        x = lax.div(k, 2)
        c = lax.rem(k, 2)
        blk = 2 * sp + c
        osp = 1 - sp
        k1 = 2 * x + (1 - c)
        k2 = 2 * (1 - x) + c
        k3 = 2 * (1 - x) + (1 - c)

        def tile_of(xx, j, par):
            return 4 * lax.rem(xx + lax.div(j, 2), 2) + 2 * lax.rem(j, 2) + par

        barrier = pltpu.get_barrier_semaphore()
        for d_sp in range(2):
            for d_cp in range(4):
                if d_sp or d_cp:
                    pl.semaphore_signal(barrier, inc=1, device_id={"sp": lax.rem(sp + d_sp, 2), "cp": lax.rem(k + d_cp, 4)},
                                        device_id_type=MESH)

        def raw_load(xx, part):
            cut = pl.ds(part * (cols // 2), cols // 2 if part == 0 else cols - cols // 2)
            return pltpu.make_async_copy(xw.at[pl.ds(ni * xx, ni), cut], raw.at[:, cut], rsem.at[part])

        def swap_part(part, slot_same, slot_other):
            lo, hi = (0, cols // 2) if part == 0 else (cols // 2, cols)

            def block(col, h0):
                rows_in = raw[:, col, pl.ds(pl.multiple_of(h0, 16), 16), :].reshape(ni * 16, cb)
                out = jnp.dot(swap[...], rows_in, preferred_element_type=jnp.float32)
                return out.astype(jnp.bfloat16).reshape(16, ni, cb)

            for col in range(lo, hi):
                mid = block(col, 16)
                for cc, slot in ((c, slot_same), (1 - c, slot_other)):
                    xa[slot, pl.ds(1 + 8 * cc, 16), col] = block(col, 32 * cc)
                    xa[slot, pl.ds(17 * (1 - cc), 9), col] = jnp.where(cc == 0, mid[0:9], mid[7:16])

        def x_copy(role):
            cc = c if role == 2 else 1 - c
            cut = pl.ds(1 - cc, rows + 1)
            return remote(xa.at[5 if role == 2 else 4, cut], xa.at[role, cut], xs.at[role - 1], xr.at[role - 1], sp,
                          {1: k1, 2: k2, 3: k3}[role])

        def halo_copy(xx, slot_same):
            role = 2 * lax.rem(x + xx, 2) + lax.rem(c + sp, 2)
            src = xa.at[jnp.where(c == osp, slot_same, 4), jnp.where(sp == 0, rows, 1)]
            return remote(src, xa.at[role, (rows + 1) * sp], hs.at[xx], hr.at[role], osp, 2 * xx + sp)

        half = cb // 2

        def w1_own(j, par, xx):
            return w1.at[:, :, :, pl.ds(pl.multiple_of(tile_of(xx, j, par) * tile, tile), tile)]

        def w1_part(j, par):
            return remote(w1_own(j, par, x), g1.at[0, j, par], p1s.at[j, par], p1r.at[j, par], sp, k1)

        def w1_x(j, hf):
            cut = pl.ds(pl.multiple_of(hf * half, half), half)
            src = w1.at[:, :, cut, pl.ds(pl.multiple_of(tile_of(1 - x, j, sp) * tile, tile), tile)]
            return remote(src, g1.at[1, j, sp, :, :, cut], x1s.at[j, hf], x1r.at[j, hf], sp, k2)

        def w1_y(j, hf):
            cut = pl.ds(pl.multiple_of(hf * half, half), half)
            ref = g1.at[1, j, sp, :, :, cut]
            return remote(ref, ref, y1s.at[j, hf], y1r.at[j, hf], osp, k)

        def w1_fwd(j, par, hf):
            cut = pl.ds(pl.multiple_of(hf * half, half), half)
            return remote(g1.at[1, j, par, :, :, cut], g1.at[2, j, par, :, :, cut], f1s.at[j, par, hf], f1r.at[j, par, hf], sp, k1)

        def w2_cut(n, par, h, xx):
            row = pl.multiple_of(par * tile + h * cb, cb)
            col = pl.multiple_of(tile * lax.rem(1 + xx + n, 2), tile)
            return w2.at[:, :, pl.ds(row, cb), pl.ds(col, tile)]

        def w2_part(n, par, h):
            return remote(w2_cut(n, par, h, x), g2.at[0, n, par, h], p2s.at[n, par, h], p2r.at[n, par, h], sp, k1)

        def w2_x(n, h):
            return remote(w2_cut(n, sp, h, 1 - x), g2.at[1, n, sp, h], x2s.at[n, h], x2r.at[n, h], sp, k2)

        def w2_y(n, h):
            ref = g2.at[1, n, sp, h]
            return remote(ref, ref, y2s.at[n, h], y2r.at[n, h], osp, k)

        def w2_fwd(n, par, h):
            return remote(g2.at[1, n, par, h], g2.at[2, n, par, h], f2s.at[n, par, h], f2r.at[n, par, h], sp, k1)

        up_blk = lax.max(blk - 1, 0)
        dn_blk = lax.min(blk + 1, 3)

        def hid_up(a):
            return remote(hid.at[a, 1], hid.at[a, rows + 1], as_.at[0, a], ar.at[1, a], lax.div(up_blk, 2), 2 * x + lax.rem(up_blk, 2))

        def hid_dn(a):
            return remote(hid.at[a, rows], hid.at[a, 0], as_.at[1, a], ar.at[0, a], lax.div(dn_blk, 2), 2 * x + lax.rem(dn_blk, 2))

        def hid_store(a, h):
            return pltpu.make_async_copy(stage.at[h], hid.at[a, pl.ds(1, rows)], stl.at[h])

        y_rows = pl.ds(rows * c, rows)

        def y_far(h):
            return remote(stage.at[h], yt.at[x, y_rows], ys.at[h], yr.at[lax.rem(h + c, 2)], sp, 2 * (1 - x) + h)

        def y_near():
            return remote(stage.at[1 - c], yt.at[x, y_rows], zs.at[0], zr.at[0], sp, k1)

        def y_own():
            return pltpu.make_async_copy(stage.at[c], yt.at[x, y_rows], yl.at[0])

        def zero_rows(row):
            return pltpu.make_async_copy(stage.at[0, pl.ds(0, 16)], hid.at[:, row], zsem.at[0])

        def p_of(m):
            return lax.rem(m + 2, 8)

        def jp(p):
            return lax.div(p, 2), lax.rem(sp + lax.rem(p, 2), 2)

        def near_step(i):
            e = lax.rem(i, 4)
            return 2 * lax.div(i, 4) + lax.rem(e, 2), lax.div(e, 2)

        def halo_wait(role):
            @pl.when(c != sp)
            def _():
                remote(xa.at[0, 0], xa.at[role, 0], hs.at[0], hr.at[role], osp, k).wait_recv()

        for part_no in range(2):
            raw_load(x, part_no).start()
        swap[...] = swap_matrix(16)
        stage[0, 0:16] = jnp.zeros((16, cols, ni, cb), jnp.bfloat16)

        @pl.when(blk == 0)
        def _():
            xa[0:4, 0] = jnp.zeros((4, cols, ni, cb), jnp.bfloat16)
            zero_rows(0).start()

        @pl.when(blk == 3)
        def _():
            xa[0:4, rows + 1] = jnp.zeros((4, cols, ni, cb), jnp.bfloat16)
            zero_rows(rows + 1).start()

        def w_load(src, t):
            return pltpu.make_async_copy(src, wv.at[lax.rem(t, 2)], wsem.at[lax.rem(t, 2)])

        def hid_load(a, q):
            slot = lax.rem(q, 2)
            return pltpu.make_async_copy(hid.at[a], xa.at[4 + slot], asem.at[slot])

        def issue(t):
            @pl.when(t < 16)
            def _():
                m, role = near_step(t)
                j, par = jp(p_of(m))

                @pl.when(role == 0)
                def _():
                    w_load(w1_own(j, par, x), t).start()

                @pl.when(role == 1)
                def _():
                    w1_part(j, par).wait_recv()
                    w_load(g1.at[0, j, par], t).start()

            @pl.when((t >= 16) & (t < 32))
            def _():
                j, par = jp(lax.div(t - 16, 2))

                @pl.when(lax.rem(t, 2) == 1)
                def _():
                    for hf in range(2):
                        w1_fwd(j, par, hf).wait_recv()

                w_load(g1.at[1 + lax.rem(t, 2), j, par], t).start()

            @pl.when((t >= 32) & (t < N_STEPS))
            def _():
                n = lax.div(t - 32, 16)
                q = lax.rem(t - 32, 16)
                h = lax.rem(q, 2)
                p = lax.div(q, 2)
                j, par = jp(p)
                a = 4 * j + 2 * par + h
                same = lax.rem(j, 2) == c

                @pl.when(n == 0)
                def _():
                    @pl.when(blk > 0)
                    def _():
                        hid_dn(a).wait_recv()

                    @pl.when(blk < 3)
                    def _():
                        hid_up(a).wait_recv()

                hid_load(a, q).start()

                @pl.when(p < 4)
                def _():
                    @pl.when(same)
                    def _():
                        w_load(w2_cut(n, par, h, x), t).start()

                    @pl.when(jnp.logical_not(same))
                    def _():
                        w2_part(n, par, h).wait_recv()
                        w_load(g2.at[0, n, par, h], t).start()

                @pl.when(p >= 4)
                def _():
                    @pl.when(jnp.logical_not(same))
                    def _():
                        w2_fwd(n, par, h).wait_recv()

                    w_load(g2.at[jnp.where(same, 1, 2), n, par, h], t).start()

        issue(jnp.int32(0))
        with jax.named_scope("swap"):
            for part_no in range(2):
                raw_load(x, part_no).wait()
                swap_part(part_no, 0, 4)
        with jax.named_scope("bar"):
            pl.semaphore_wait(barrier, 7)
        halo_copy(x, 0).start()
        x_copy(1).start()
        for m in range(2):
            w1_part(*jp(jnp.int32((m + 2) % 8))).start()
        for e in range(3):
            w1_x(e // 2, e % 2).start()
        for part_no in range(2):
            raw_load(1 - x, part_no).start()
        with jax.named_scope("halo"):
            halo_wait(0)

        def pass_w1_x(e):
            j, hf = lax.div(e, 2), lax.rem(e, 2)
            w1_x(j, hf).wait_recv()
            w1_y(j, hf).start()
            w1_fwd(j, sp, hf).start()

        def pass_w1_y(e):
            j, hf = lax.div(e, 2), lax.rem(e, 2)
            w1_y(j, hf).wait_recv()
            w1_fwd(j, osp, hf).start()

        def pass_w2_x(e):
            n, h = lax.div(e, 2), lax.rem(e, 2)
            w2_x(n, h).wait_recv()
            w2_y(n, h).start()
            w2_fwd(n, sp, h).start()

        def pass_w2_y(e):
            n, h = lax.div(e, 2), lax.rem(e, 2)
            w2_y(n, h).wait_recv()
            w2_fwd(n, osp, h).start()

        def send_w1_x(e):
            w1_x(lax.div(e, 2), lax.rem(e, 2)).start()

        def send_w2_x(e):
            w2_x(lax.div(e, 2), lax.rem(e, 2)).start()

        def events(i):
            even = lax.rem(i, 2) == 0
            odd = jnp.logical_not(even)

            @pl.when(i < 16)
            def _():
                @pl.when(even)
                def _():
                    @pl.when(i < 12)
                    def _():
                        w1_part(*jp(p_of(lax.div(i, 2) + 2))).start()

                    @pl.when(i == 2)
                    def _():
                        x_copy(1).wait_recv()
                        halo_wait(1)

                    @pl.when(i == 10)
                    def _():
                        for e in range(2):
                            pass_w1_y(jnp.int32(e))

                    @pl.when(i == 12)
                    def _():
                        pass_w1_y(jnp.int32(2))

                @pl.when(odd)
                def _():
                    @pl.when(i == 3)
                    def _():
                        x_copy(1).wait_send()
                        halo_copy(x, 0).wait_send()
                        for part_no in range(2):
                            raw_load(1 - x, part_no).wait()
                            swap_part(part_no, 5, 4)
                        halo_copy(1 - x, 5).start()
                        x_copy(2).start()

                    @pl.when(i == 5)
                    def _():
                        for e in range(2):
                            pass_w1_x(jnp.int32(e))

                    @pl.when(i == 7)
                    def _():
                        pass_w1_x(jnp.int32(2))

                    @pl.when(i == 9)
                    def _():
                        x_copy(3).start()

                    @pl.when(i >= 13)
                    def _():
                        send_w1_x(lax.div(i - 7, 2))

            @pl.when((i >= 16) & (i < 34))
            def _():
                @pl.when(i < 24)
                def _():
                    e = i - 16
                    w2_part(lax.div(e, 4), lax.rem(lax.div(e, 2), 2), lax.rem(e, 2)).start()

                @pl.when(even)
                def _():
                    @pl.when(i == 16)
                    def _():
                        x_copy(2).wait_recv()
                        halo_wait(2)

                    @pl.when(i == 30)
                    def _():
                        x_copy(2).wait_send()
                        x_copy(3).wait_send()
                        halo_copy(1 - x, 5).wait_send()

                    @pl.when((i >= 24) & (lax.rem(i, 4) == 0))
                    def _():
                        send_w2_x(lax.div(i - 24, 4))

                    @pl.when((i >= 18) & (i <= 26))
                    def _():
                        pass_w1_x(lax.div(i - 12, 2))

                @pl.when(odd)
                def _():
                    @pl.when(i == 17)
                    def _():
                        x_copy(3).wait_recv()
                        halo_wait(3)

                    @pl.when(i <= 21)
                    def _():
                        send_w1_x(lax.div(i - 7, 2))

                    @pl.when(i >= 19)
                    def _():
                        for h in range(2):
                            hid_store(0, h).wait()

                    @pl.when((i >= 21) & (i <= 29))
                    def _():
                        pass_w1_y(lax.div(i - 15, 2))

                    @pl.when(i >= 27)
                    def _():
                        for d in range(2):
                            j, par = jp(i - 27 + d)
                            for h in range(2):
                                a = 4 * j + 2 * par + h

                                @pl.when(blk > 0)
                                def _():
                                    hid_up(a).start()

                                @pl.when(blk < 3)
                                def _():
                                    hid_dn(a).start()

                    @pl.when(i == 31)
                    def _():
                        pass_w2_x(jnp.int32(0))

            @pl.when((i >= 34) & (i < 50))
            def _():
                @pl.when(i == 36)
                def _():
                    send_w2_x(jnp.int32(3))

                @pl.when((i < 44) & (lax.rem(i, 4) == 3))
                def _():
                    pass_w2_x(lax.div(i - 31, 4))

                @pl.when((i >= 37) & (lax.rem(i, 4) == 1))
                def _():
                    pass_w2_y(lax.div(i - 37, 4))

        def taps(xs_slot, ws_slot, col):
            total = None
            for dx in (-1, 0, 1):
                if not 0 <= col + dx < cols:
                    continue
                for dy in range(3):
                    lhs = xa[xs_slot, dy:dy + rows, col + dx].reshape(m_rows, cb)
                    prod = jnp.dot(lhs, wv[ws_slot, dy, dx + 1], preferred_element_type=jnp.float32)
                    total = prod if total is None else total + prod
            return total

        def step(i, carry):
            ph1 = i < 16
            ph3 = i >= 32
            n = jnp.where(ph3, lax.div(i - 32, 16), 0)
            q = jnp.where(ph3, lax.rem(i - 32, 16), 0)
            m, role = near_step(i)
            m = jnp.where(ph1, m, lax.div(i - 16, 2))
            role = jnp.where(ph1, role, 2 + lax.rem(i, 2))
            p = jnp.where(ph1, p_of(m), lax.rem(m, 8))
            p = jnp.where(ph3, 0, p)
            last = jnp.where(ph3, q == 15, role == 3)
            first = jnp.where(ph3, q == 0, role == 0)
            a_slot = jnp.where(ph3, n, lax.rem(p, 2))
            x_slot = jnp.where(ph3, 4 + lax.rem(q, 2), role)
            w_slot = lax.rem(i, 2)

            with jax.named_scope("ev"):
                events(i)
            with jax.named_scope("iss"):
                issue(i + 1)
            w_load(g1.at[0, 0, 0], i).wait()

            @pl.when(ph3)
            def _():
                hid_load(0, q).wait()

            @pl.when((i >= 4) & (i < 32))
            def _():
                @pl.when(ph1 & first)
                def _():
                    pltpu.make_async_copy(acc.at[a_slot], part.at[0], pst.at[a_slot]).wait()

                @pl.when((i >= 20) & (role == 2))
                def _():
                    pltpu.make_async_copy(part.at[0], acc.at[a_slot], pld.at[a_slot]).wait()

            @pl.when(jnp.logical_not(last))
            def _():
                with jax.named_scope("mm"):
                    for col in range(cols):
                        total = taps(x_slot, w_slot, col)
                        acc[a_slot, col] = total + jnp.where(first, 0.0, acc[a_slot, col])

            @pl.when((i < 12) & (role == 1))
            def _():
                pltpu.make_async_copy(acc.at[a_slot], part.at[p], pst.at[a_slot]).start()

            @pl.when(last)
            def _():
                @pl.when((i == 17) & ((blk == 0) | (blk == 3)))
                def _():
                    zero_rows(0).wait()

                @pl.when(i == 63)
                def _():
                    for h in range(2):
                        y_far(h).wait_send()

                keep = jnp.where(ph3, 1.0, 0.0)
                floor = jnp.where(ph3, -jnp.inf, 0.0)
                j, par = jp(p)
                shift = b1[tile_of(x, j, par)] * (1.0 - keep)
                role0 = jnp.where(n == 0, 2, 0)
                with jax.named_scope("mmo"):
                    for col in range(cols):
                        total = taps(x_slot, w_slot, col) + acc[a_slot, col] + shift
                        for h in range(2):
                            role = role0 + lax.rem(c + h, 2)
                            res = xa[role, 1:rows + 1, col].reshape(m_rows, cb).astype(jnp.float32)
                            val = jnp.maximum(total[:, h * cb:(h + 1) * cb] + res * keep, floor)
                            stage[h, :, col] = val.astype(jnp.bfloat16).reshape(rows, ni, cb)

                @pl.when(i < 32)
                def _():
                    for h in range(2):
                        hid_store(4 * j + 2 * par + h, h).start()

                    @pl.when(p < 6)
                    def _():
                        pltpu.make_async_copy(part.at[p + 2], acc.at[a_slot], pld.at[a_slot]).start()

                @pl.when(i == 47)
                def _():
                    for h in range(2):
                        y_far(h).start()

                @pl.when(i == 63)
                def _():
                    y_near().start()
                    y_own().start()

            return carry

        lax.fori_loop(0, N_STEPS, step, 0)

        def drain(e, carry):
            hi, lo = lax.div(e, 2), lax.rem(e, 2)
            w1_part(hi, lo).wait_send()
            w1_x(hi, lo).wait_send()
            w1_y(hi, lo).wait_send()
            for hf in range(2):
                w1_fwd(hi, lo, hf).wait_send()
            n, par = lax.div(e, 4), lax.rem(lax.div(e, 2), 2)
            w2_part(n, par, lo).wait_send()
            w2_fwd(n, par, lo).wait_send()
            return carry

        lax.fori_loop(0, 8, drain, 0)

        def drain_rows(a, carry):
            @pl.when(blk > 0)
            def _():
                hid_up(a).wait_send()

            @pl.when(blk < 3)
            def _():
                hid_dn(a).wait_send()

            return carry

        lax.fori_loop(0, 16, drain_rows, 0)

        def drain_two(e, carry):
            w2_x(lax.div(e, 2), lax.rem(e, 2)).wait_send()
            w2_y(lax.div(e, 2), lax.rem(e, 2)).wait_send()
            return carry

        lax.fori_loop(0, 4, drain_two, 0)
        for e in range(2):
            remote(stage.at[0], yt.at[0, pl.ds(0, rows)], ys.at[0], yr.at[e], sp, k).wait_recv()
        y_near().wait()
        y_own().wait()

    dma = pltpu.SemaphoreType.DMA
    bf16, f32 = jnp.bfloat16, jnp.float32
    any_space = pl.BlockSpec(memory_space=pl.ANY)
    outs = pl.pallas_call(
        kernel,
        out_shape=[
            jax.ShapeDtypeStruct((2, h_loc, cols, ni, cb), bf16),
            jax.ShapeDtypeStruct((3, 4, 2, 3, 3, cb, tile), bf16),
            jax.ShapeDtypeStruct((3, 2, 2, 2, 3, 3, cb, tile), bf16),
            jax.ShapeDtypeStruct((8, cols, m_rows, tile), f32),
            jax.ShapeDtypeStruct((16, rows + 2, cols, ni, cb), bf16),
        ],
        in_specs=[any_space, any_space, any_space, pl.BlockSpec(memory_space=pltpu.VMEM)],
        out_specs=[any_space] * 5,
        scratch_shapes=[
            pltpu.VMEM((6, rows + 2, cols, ni, cb), bf16),
            pltpu.VMEM((2, cols, m_rows, tile), f32),
            pltpu.VMEM((2, 3, 3, cb, tile), bf16),
            pltpu.VMEM((2, rows, cols, ni, cb), bf16),
            pltpu.VMEM((ni, cols, h_loc, cb), bf16),
            pltpu.VMEM((16 * ni, 16 * ni), bf16),
            dma((2,)), dma((2,)), dma((2,)), dma((2,)), dma((2,)), dma((1,)), dma((2,)), dma((3,)), dma((3,)), dma((2,)), dma((4,)),
            dma((4, 2)), dma((4, 2)), dma((4, 2)), dma((4, 2)), dma((4, 2)), dma((4, 2)), dma((4, 2, 2)), dma((4, 2, 2)),
            dma((2, 2, 2)), dma((2, 2, 2)), dma((2, 2)), dma((2, 2)), dma((2, 2)), dma((2, 2)), dma((2, 2, 2)), dma((2, 2, 2)),
            dma((2, 16)), dma((2, 16)), dma((2,)), dma((2,)), dma((1,)), dma((1,)), dma((1,)),
        ],
        compiler_params=pltpu.CompilerParams(collective_id=0, has_side_effects=True, vmem_limit_bytes=60 * 1024 * 1024),
        name="fused_block",
    )(xw, w_one, w_two, bias)
    return outs[0]


def images_major(yt):
    groups, h_loc, cols, ni, cb = yt.shape
    assert ni == 16 and h_loc % 16 == 0
    width = 2 if cols % 2 == 0 else 1

    def kernel(y_ref, out_ref, swap):
        @pl.when((pl.program_id(0) == 0) & (pl.program_id(1) == 0))
        def _():
            swap[...] = swap_matrix(16)

        for col in range(width):
            for h0 in range(0, h_loc, 16):
                rows_in = y_ref[0, h0:h0 + 16, col].reshape(16 * ni, cb)
                out = jnp.dot(swap[...], rows_in, preferred_element_type=jnp.float32)
                out_ref[:, col, h0:h0 + 16] = out.astype(jnp.bfloat16).reshape(ni, 16, cb)

    return pl.pallas_call(
        kernel,
        grid=(groups, cols // width),
        out_shape=jax.ShapeDtypeStruct((groups * ni, cols, h_loc, cb), jnp.bfloat16),
        in_specs=[pl.BlockSpec((1, h_loc, width, ni, cb), lambda g, w: (g, 0, w, 0, 0))],
        out_specs=pl.BlockSpec((ni, width, h_loc, cb), lambda g, w: (g, w, 0, 0)),
        scratch_shapes=[pltpu.VMEM((16 * ni, 16 * ni), jnp.bfloat16)],
        compiler_params=pltpu.CompilerParams(vmem_limit_bytes=60 * 1024 * 1024),
        name="images_major",
    )(yt)


def solution(mesh):
    act_spec = P("dp", "sp", None, "cp")
    kernel_spec = P(None, None, "cp", None)

    def local_block(x_tile, w_one_part, w_two_part, bias_one):
        xw = x_tile.transpose(0, 2, 1, 3)
        yt = fused_block(xw, w_one_part, w_two_part, bias_one.reshape(8, 1, 2 * x_tile.shape[3]))
        return images_major(yt).transpose(0, 2, 1, 3)

    return jax.shard_map(local_block, mesh=mesh, in_specs=(act_spec, kernel_spec, kernel_spec, P()), out_specs=act_spec, check_vma=False)
```

```python
import functools

import jax
import jax.numpy as jnp
from jax import lax
from jax.experimental import pallas as pl
from jax.experimental.pallas import tpu as pltpu
from jax.sharding import PartitionSpec as P

MESH = pl.DeviceIdType.MESH
N_STEPS = 64
MIB = 1024 * 1024
ONE, TWO, THREE, FOUR, ALL = (1,), (2,), (3,), (4,), (2, 16)
GRID, CUBE, HALVES = (2, 2), (2, 2, 2), (4, 2)
THIRDS = (4, 2, 2)
SEMS = (
    TWO, TWO, TWO, TWO, TWO, ONE, THREE, THREE, THREE, TWO, FOUR,
    HALVES, HALVES, HALVES, HALVES, HALVES, HALVES, THIRDS, THIRDS,
    CUBE, CUBE, GRID, GRID, GRID, GRID, CUBE, CUBE,
    ALL, ALL, TWO, TWO, ONE, ONE, ONE,
)


def pair(e):
    return lax.div(e, 2), lax.rem(e, 2)


def odd(i):
    return lax.rem(i, 2) == 1


def swap_matrix(n):
    to = lax.broadcasted_iota(jnp.int32, (n * n, n * n), 0)
    frm = lax.broadcasted_iota(jnp.int32, (n * n, n * n), 1)
    hit = (lax.div(to, n) == lax.rem(frm, n)) & (lax.rem(to, n) == lax.div(frm, n))
    return jnp.where(hit, 1.0, 0.0).astype(jnp.bfloat16)


def fused_block(xw, w_one, w_two, bias):
    images, cols, h_loc, cb = xw.shape
    ni = images // 2
    rows = h_loc // 2
    m_rows = rows * ni
    tile = 2 * cb
    assert ni == 16 and h_loc == 48

    def remote(src, dst, send_sem, recv_sem, sp, cp):
        return pltpu.make_async_remote_copy(src_ref=src, dst_ref=dst, send_sem=send_sem, recv_sem=recv_sem,
                                            device_id={"sp": sp, "cp": cp}, device_id_type=MESH)

    def kernel(xw, w1, w2, b1, yt, g1, g2, part, hid,
               xa, acc, wv, stage, raw, swap,
               wsem, asem, pst, pld, stl, zsem, rsem, xs, xr, hs, hr,
               p1s, p1r, x1s, x1r, y1s, y1r, f1s, f1r,
               p2s, p2r, x2s, x2r, y2s, y2r, f2s, f2r,
               as_, ar, ys, yr, zs, zr, yl):
        sp = lax.axis_index("sp")
        k = lax.axis_index("cp")
        x = lax.div(k, 2)
        c = lax.rem(k, 2)
        blk = 2 * sp + c
        osp = 1 - sp
        k1 = 2 * x + (1 - c)
        k2 = 2 * (1 - x) + c
        k3 = 2 * (1 - x) + (1 - c)

        def tile_of(xx, j, par):
            return 4 * lax.rem(xx + lax.div(j, 2), 2) + 2 * lax.rem(j, 2) + par

        barrier = pltpu.get_barrier_semaphore()
        for d_sp in range(2):
            for d_cp in range(4):
                if d_sp or d_cp:
                    pl.semaphore_signal(barrier, inc=1, device_id={"sp": lax.rem(sp + d_sp, 2), "cp": lax.rem(k + d_cp, 4)},
                                        device_id_type=MESH)

        def raw_load(xx, part):
            cut = pl.ds(pl.multiple_of(ni * part, ni), ni)
            return pltpu.make_async_copy(xw.at[pl.ds(ni * xx, ni), :, cut], raw.at[:, :, cut], rsem.at[part])

        def block(col, part):
            rows_in = raw[:, col, pl.ds(pl.multiple_of(ni * part, ni), ni), :].reshape(ni * ni, cb)
            out = jnp.dot(swap[...], rows_in, preferred_element_type=jnp.float32)
            return out.astype(jnp.bfloat16).reshape(ni, ni, cb)

        def slot_of(cc, slot_same):
            return jnp.where(cc == c, slot_same, 4)

        def swap_end(xx, cc, slot_same):
            raw_load(xx, 2 * cc).wait()
            for col in range(cols):
                xa[slot_of(cc, slot_same), pl.ds(1 + 8 * cc, ni), col] = block(col, 2 * cc)

        def swap_mid(xx, slot_same):
            raw_load(xx, 1).wait()
            for col in range(cols):
                mid = block(col, 1)
                xa[slot_of(0, slot_same), 17:26, col] = mid[0:9]
                xa[slot_of(1, slot_same), 0:9, col] = mid[7:16]

        def x_copy(role):
            cc = c if role == 2 else 1 - c
            cut = pl.ds(1 - cc, rows + 1)
            return remote(xa.at[5 if role == 2 else 4, cut], xa.at[role, cut], xs.at[role - 1], xr.at[role - 1], sp,
                          {1: k1, 2: k2, 3: k3}[role])

        def halo_copy(xx, slot_same):
            role = 2 * lax.rem(x + xx, 2) + lax.rem(c + sp, 2)
            src = xa.at[slot_of(osp, slot_same), jnp.where(sp == 0, rows, 1)]
            return remote(src, xa.at[role, (rows + 1) * sp], hs.at[xx], hr.at[role], osp, 2 * xx + sp)

        half = cb // 2

        def w1_own(j, par, xx):
            return w1.at[:, :, :, pl.ds(pl.multiple_of(tile_of(xx, j, par) * tile, tile), tile)]

        def w1_part(j, par):
            return remote(w1_own(j, par, x), g1.at[0, j, par], p1s.at[j, par], p1r.at[j, par], sp, k1)

        def w1_x(j, hf):
            cut = pl.ds(pl.multiple_of(hf * half, half), half)
            src = w1.at[:, :, cut, pl.ds(pl.multiple_of(tile_of(1 - x, j, sp) * tile, tile), tile)]
            return remote(src, g1.at[1, j, sp, :, :, cut], x1s.at[j, hf], x1r.at[j, hf], sp, k2)

        def w1_y(j, hf):
            cut = pl.ds(pl.multiple_of(hf * half, half), half)
            ref = g1.at[1, j, sp, :, :, cut]
            return remote(ref, ref, y1s.at[j, hf], y1r.at[j, hf], osp, k)

        def w1_fwd(j, par, hf):
            cut = pl.ds(pl.multiple_of(hf * half, half), half)
            return remote(g1.at[1, j, par, :, :, cut], g1.at[2, j, par, :, :, cut], f1s.at[j, par, hf], f1r.at[j, par, hf], sp, k1)

        def w2_cut(n, par, h, xx):
            row = pl.multiple_of(par * tile + h * cb, cb)
            col = pl.multiple_of(tile * lax.rem(1 + xx + n, 2), tile)
            return w2.at[:, :, pl.ds(row, cb), pl.ds(col, tile)]

        def w2_part(n, par, h):
            return remote(w2_cut(n, par, h, x), g2.at[0, n, par, h], p2s.at[n, par, h], p2r.at[n, par, h], sp, k1)

        def w2_x(n, h):
            return remote(w2_cut(n, sp, h, 1 - x), g2.at[1, n, sp, h], x2s.at[n, h], x2r.at[n, h], sp, k2)

        def w2_y(n, h):
            ref = g2.at[1, n, sp, h]
            return remote(ref, ref, y2s.at[n, h], y2r.at[n, h], osp, k)

        def w2_fwd(n, par, h):
            return remote(g2.at[1, n, par, h], g2.at[2, n, par, h], f2s.at[n, par, h], f2r.at[n, par, h], sp, k1)

        up_blk = lax.max(blk - 1, 0)
        dn_blk = lax.min(blk + 1, 3)

        def hid_up(a):
            return remote(hid.at[a, 1], hid.at[a, rows + 1], as_.at[0, a], ar.at[1, a], lax.div(up_blk, 2), 2 * x + lax.rem(up_blk, 2))

        def hid_dn(a):
            return remote(hid.at[a, rows], hid.at[a, 0], as_.at[1, a], ar.at[0, a], lax.div(dn_blk, 2), 2 * x + lax.rem(dn_blk, 2))

        def hid_store(a, h):
            return pltpu.make_async_copy(stage.at[h], hid.at[a, pl.ds(1, rows)], stl.at[h])

        y_rows = pl.ds(rows * c, rows)

        def y_far(h):
            return remote(stage.at[h], yt.at[x, y_rows], ys.at[h], yr.at[lax.rem(h + c, 2)], sp, 2 * (1 - x) + h)

        def y_near():
            return remote(stage.at[1 - c], yt.at[x, y_rows], zs.at[0], zr.at[0], sp, k1)

        def y_own():
            return pltpu.make_async_copy(stage.at[c], yt.at[x, y_rows], yl.at[0])

        def zero_rows(row):
            return pltpu.make_async_copy(stage.at[0, pl.ds(0, 16)], hid.at[:, row], zsem.at[0])

        def p_of(m):
            return lax.rem(m + 2, 8)

        def jp(p):
            return lax.div(p, 2), lax.rem(sp + lax.rem(p, 2), 2)

        def near_step(i):
            e = lax.rem(i, 4)
            return 2 * lax.div(i, 4) + lax.rem(e, 2), lax.div(e, 2)

        def halo_wait(role):
            @pl.when(c != sp)
            def _():
                remote(xa.at[0, 0], xa.at[role, 0], hs.at[0], hr.at[role], osp, k).wait_recv()

        for part_no in (2 * osp, 1, 2 * sp):
            raw_load(x, part_no).start()
        swap[...] = swap_matrix(ni)
        stage[0, 0:16] = jnp.zeros((16, cols, ni, cb), jnp.bfloat16)

        @pl.when(blk == 0)
        def _():
            xa[0:4, 0] = jnp.zeros((4, cols, ni, cb), jnp.bfloat16)
            zero_rows(0).start()

        @pl.when(blk == 3)
        def _():
            xa[0:4, rows + 1] = jnp.zeros((4, cols, ni, cb), jnp.bfloat16)
            zero_rows(rows + 1).start()

        def w_load(src, t):
            return pltpu.make_async_copy(src, wv.at[lax.rem(t, 2)], wsem.at[lax.rem(t, 2)])

        def hid_load(a, q):
            slot = lax.rem(q, 2)
            return pltpu.make_async_copy(hid.at[a], xa.at[4 + slot], asem.at[slot])

        def issue(t):
            @pl.when(t < 16)
            def _():
                m, role = near_step(t)
                j, par = jp(p_of(m))

                @pl.when(role == 0)
                def _():
                    w_load(w1_own(j, par, x), t).start()

                @pl.when(role == 1)
                def _():
                    w1_part(j, par).wait_recv()
                    w_load(g1.at[0, j, par], t).start()

            @pl.when((t >= 16) & (t < 32))
            def _():
                j, par = jp(lax.div(t - 16, 2))

                @pl.when(lax.rem(t, 2) == 1)
                def _():
                    for hf in range(2):
                        w1_fwd(j, par, hf).wait_recv()

                w_load(g1.at[1 + lax.rem(t, 2), j, par], t).start()

            @pl.when((t >= 32) & (t < N_STEPS))
            def _():
                n = lax.div(t - 32, 16)
                q = lax.rem(t - 32, 16)
                h = lax.rem(q, 2)
                p = lax.div(q, 2)
                j, par = jp(p)
                a = 4 * j + 2 * par + h
                same = lax.rem(j, 2) == c

                @pl.when(n == 0)
                def _():
                    @pl.when(blk > 0)
                    def _():
                        hid_dn(a).wait_recv()

                    @pl.when(blk < 3)
                    def _():
                        hid_up(a).wait_recv()

                hid_load(a, q).start()

                @pl.when(p < 4)
                def _():
                    @pl.when(same)
                    def _():
                        w_load(w2_cut(n, par, h, x), t).start()

                    @pl.when(jnp.logical_not(same))
                    def _():
                        w2_part(n, par, h).wait_recv()
                        w_load(g2.at[0, n, par, h], t).start()

                @pl.when(p >= 4)
                def _():
                    @pl.when(jnp.logical_not(same))
                    def _():
                        w2_fwd(n, par, h).wait_recv()

                    w_load(g2.at[jnp.where(same, 1, 2), n, par, h], t).start()

        issue(jnp.int32(0))
        with jax.named_scope("swap"):
            swap_end(x, osp, 0)
        with jax.named_scope("bar"):
            pl.semaphore_wait(barrier, 7)

        @pl.when(c == sp)
        def _():
            halo_copy(x, 0).start()

        for e in range(3):
            w1_x(*divmod(e, 2)).start()
        with jax.named_scope("swap2"):
            swap_end(x, sp, 0)
            swap_mid(x, 0)
        x_copy(1).start()
        for m in range(2):
            w1_part(*jp(jnp.int32(m + 2))).start()

        @pl.when(c != sp)
        def _():
            halo_copy(x, 0).start()

        for part_no in range(3):
            raw_load(1 - x, part_no).start()
        with jax.named_scope("halo"):
            halo_wait(0)

        def pass_w1_x(e):
            j, hf = pair(e)
            w1_x(j, hf).wait_recv()
            w1_y(j, hf).start()
            w1_fwd(j, sp, hf).start()

        def pass_w1_y(e):
            j, hf = pair(e)
            w1_y(j, hf).wait_recv()
            w1_fwd(j, osp, hf).start()

        def pass_w2_x(e):
            n, h = pair(e)
            w2_x(n, h).wait_recv()
            w2_y(n, h).start()
            w2_fwd(n, sp, h).start()

        def pass_w2_y(e):
            n, h = pair(e)
            w2_y(n, h).wait_recv()
            w2_fwd(n, osp, h).start()

        def send_w1_x(e):
            w1_x(*pair(e)).start()

        def send_w2_x(e):
            w2_x(*pair(e)).start()

        def events(i):
            is_odd = odd(i)
            even = jnp.logical_not(is_odd)

            @pl.when(i < 16)
            def _():
                @pl.when(even)
                def _():
                    @pl.when(i < 12)
                    def _():
                        w1_part(*jp(p_of(lax.div(i, 2) + 2))).start()

                    @pl.when(i == 2)
                    def _():
                        x_copy(1).wait_recv()
                        halo_wait(1)

                    @pl.when(i == 10)
                    def _():
                        for e in range(2):
                            pass_w1_y(jnp.int32(e))

                    @pl.when(i == 12)
                    def _():
                        pass_w1_y(jnp.int32(2))

                @pl.when(is_odd)
                def _():
                    @pl.when(i == 3)
                    def _():
                        x_copy(1).wait_send()
                        halo_copy(x, 0).wait_send()
                        for cc in range(2):
                            swap_end(1 - x, cc, 5)
                        swap_mid(1 - x, 5)
                        halo_copy(1 - x, 5).start()
                        x_copy(2).start()

                    @pl.when(i == 5)
                    def _():
                        for e in range(2):
                            pass_w1_x(jnp.int32(e))

                    @pl.when(i == 7)
                    def _():
                        pass_w1_x(jnp.int32(2))

                    @pl.when(i == 9)
                    def _():
                        x_copy(3).start()

                    @pl.when(i >= 13)
                    def _():
                        send_w1_x(lax.div(i - 7, 2))

            @pl.when((i >= 16) & (i < 34))
            def _():
                @pl.when(i < 24)
                def _():
                    e = i - 16
                    w2_part(lax.div(e, 4), lax.rem(lax.div(e, 2), 2), lax.rem(e, 2)).start()

                @pl.when(even)
                def _():
                    @pl.when(i == 16)
                    def _():
                        x_copy(2).wait_recv()
                        halo_wait(2)

                    @pl.when(i == 30)
                    def _():
                        x_copy(2).wait_send()
                        x_copy(3).wait_send()
                        halo_copy(1 - x, 5).wait_send()

                    @pl.when((i >= 24) & (lax.rem(i, 4) == 0))
                    def _():
                        send_w2_x(lax.div(i - 24, 4))

                    @pl.when((i >= 18) & (i <= 26))
                    def _():
                        pass_w1_x(lax.div(i - 12, 2))

                @pl.when(is_odd)
                def _():
                    @pl.when(i == 17)
                    def _():
                        x_copy(3).wait_recv()
                        halo_wait(3)

                    @pl.when(i <= 21)
                    def _():
                        send_w1_x(lax.div(i - 7, 2))

                    @pl.when(i >= 19)
                    def _():
                        for h in range(2):
                            hid_store(0, h).wait()

                    @pl.when((i >= 21) & (i <= 29))
                    def _():
                        pass_w1_y(lax.div(i - 15, 2))

                    @pl.when(i >= 27)
                    def _():
                        for d in range(2):
                            j, par = jp(i - 27 + d)
                            for h in range(2):
                                a = 4 * j + 2 * par + h

                                @pl.when(blk > 0)
                                def _():
                                    hid_up(a).start()

                                @pl.when(blk < 3)
                                def _():
                                    hid_dn(a).start()

                    @pl.when(i == 31)
                    def _():
                        pass_w2_x(jnp.int32(0))

            @pl.when((i >= 34) & (i < 50))
            def _():
                @pl.when(i == 36)
                def _():
                    send_w2_x(jnp.int32(3))

                @pl.when((i < 44) & (lax.rem(i, 4) == 3))
                def _():
                    pass_w2_x(lax.div(i - 31, 4))

                @pl.when((i >= 37) & (lax.rem(i, 4) == 1))
                def _():
                    pass_w2_y(lax.div(i - 37, 4))

        def taps(xs_slot, ws_slot, col):
            total = None
            for dx in (-1, 0, 1):
                if not 0 <= col + dx < cols:
                    continue
                for dy in range(3):
                    lhs = xa[xs_slot, dy:dy + rows, col + dx].reshape(m_rows, cb)
                    prod = jnp.dot(lhs, wv[ws_slot, dy, dx + 1], preferred_element_type=jnp.float32)
                    total = prod if total is None else total + prod
            return total

        def step(i, carry):
            ph1 = i < 16
            ph3 = i >= 32
            n = jnp.where(ph3, lax.div(i - 32, 16), 0)
            q = jnp.where(ph3, lax.rem(i - 32, 16), 0)
            m, role = near_step(i)
            m = jnp.where(ph1, m, lax.div(i - 16, 2))
            role = jnp.where(ph1, role, 2 + lax.rem(i, 2))
            p = jnp.where(ph1, p_of(m), lax.rem(m, 8))
            p = jnp.where(ph3, 0, p)
            last = jnp.where(ph3, q == 15, role == 3)
            first = jnp.where(ph3, q == 0, role == 0)
            a_slot = jnp.where(ph3, n, lax.rem(p, 2))
            x_slot = jnp.where(ph3, 4 + lax.rem(q, 2), role)
            w_slot = lax.rem(i, 2)

            with jax.named_scope("ev"):
                events(i)
            with jax.named_scope("iss"):
                issue(i + 1)
            w_load(g1.at[0, 0, 0], i).wait()

            @pl.when(ph3)
            def _():
                hid_load(0, q).wait()

            @pl.when((i >= 4) & (i < 32))
            def _():
                @pl.when(ph1 & first)
                def _():
                    pltpu.make_async_copy(acc.at[a_slot], part.at[0], pst.at[a_slot]).wait()

                @pl.when((i >= 20) & (role == 2))
                def _():
                    pltpu.make_async_copy(part.at[0], acc.at[a_slot], pld.at[a_slot]).wait()

            @pl.when(jnp.logical_not(last))
            def _():
                with jax.named_scope("mm"):
                    for col in range(cols):
                        total = taps(x_slot, w_slot, col)
                        acc[a_slot, col] = total + jnp.where(first, 0.0, acc[a_slot, col])

            @pl.when((i < 12) & (role == 1))
            def _():
                pltpu.make_async_copy(acc.at[a_slot], part.at[p], pst.at[a_slot]).start()

            @pl.when(last)
            def _():
                @pl.when((i == 17) & ((blk == 0) | (blk == 3)))
                def _():
                    zero_rows(0).wait()

                @pl.when(i == 63)
                def _():
                    for h in range(2):
                        y_far(h).wait_send()

                keep = jnp.where(ph3, 1.0, 0.0)
                floor = jnp.where(ph3, -jnp.inf, 0.0)
                j, par = jp(p)
                shift = b1[tile_of(x, j, par)] * (1.0 - keep)
                role0 = jnp.where(n == 0, 2, 0)
                with jax.named_scope("mmo"):
                    for col in range(cols):
                        total = taps(x_slot, w_slot, col) + acc[a_slot, col] + shift
                        for h in range(2):
                            role = role0 + lax.rem(c + h, 2)
                            res = xa[role, 1:rows + 1, col].reshape(m_rows, cb).astype(jnp.float32)
                            val = jnp.maximum(total[:, h * cb:(h + 1) * cb] + res * keep, floor)
                            stage[h, :, col] = val.astype(jnp.bfloat16).reshape(rows, ni, cb)

                @pl.when(i < 32)
                def _():
                    for h in range(2):
                        hid_store(4 * j + 2 * par + h, h).start()

                    @pl.when(p < 6)
                    def _():
                        pltpu.make_async_copy(part.at[p + 2], acc.at[a_slot], pld.at[a_slot]).start()

                @pl.when(i == 47)
                def _():
                    for h in range(2):
                        y_far(h).start()

                @pl.when(i == 63)
                def _():
                    y_near().start()
                    y_own().start()

            return carry

        lax.fori_loop(0, N_STEPS, step, 0)

        def drain(e, carry):
            hi, lo = pair(e)
            w1_part(hi, lo).wait_send()
            w1_x(hi, lo).wait_send()
            w1_y(hi, lo).wait_send()
            for hf in range(2):
                w1_fwd(hi, lo, hf).wait_send()
            n, par = lax.div(e, 4), lax.rem(lax.div(e, 2), 2)
            w2_part(n, par, lo).wait_send()
            w2_fwd(n, par, lo).wait_send()
            return carry

        lax.fori_loop(0, 8, drain, 0)

        def drain_rows(a, carry):
            @pl.when(blk > 0)
            def _():
                hid_up(a).wait_send()

            @pl.when(blk < 3)
            def _():
                hid_dn(a).wait_send()

            return carry

        lax.fori_loop(0, 16, drain_rows, 0)

        def drain_two(e, carry):
            w2_x(*pair(e)).wait_send()
            w2_y(*pair(e)).wait_send()
            return carry

        lax.fori_loop(0, 4, drain_two, 0)
        for e in range(2):
            remote(stage.at[0], yt.at[0, pl.ds(0, rows)], ys.at[0], yr.at[e], sp, k).wait_recv()
        y_near().wait()
        y_own().wait()

    dma = pltpu.SemaphoreType.DMA
    bf16, f32 = jnp.bfloat16, jnp.float32
    any_space = pl.BlockSpec(memory_space=pl.ANY)
    outs = pl.pallas_call(
        kernel,
        out_shape=[
            jax.ShapeDtypeStruct((2, h_loc, cols, ni, cb), bf16),
            jax.ShapeDtypeStruct((3, 4, 2, 3, 3, cb, tile), bf16),
            jax.ShapeDtypeStruct((3, 2, 2, 2, 3, 3, cb, tile), bf16),
            jax.ShapeDtypeStruct((8, cols, m_rows, tile), f32),
            jax.ShapeDtypeStruct((16, rows + 2, cols, ni, cb), bf16),
        ],
        in_specs=[any_space, any_space, any_space, pl.BlockSpec(memory_space=pltpu.VMEM)],
        out_specs=[any_space] * 5,
        scratch_shapes=[
            pltpu.VMEM((6, rows + 2, cols, ni, cb), bf16),
            pltpu.VMEM((2, cols, m_rows, tile), f32),
            pltpu.VMEM((2, 3, 3, cb, tile), bf16),
            pltpu.VMEM((2, rows, cols, ni, cb), bf16),
            pltpu.VMEM((ni, cols, h_loc, cb), bf16),
            pltpu.VMEM((ni * ni, ni * ni), bf16),
            *map(dma, SEMS),
        ],
        compiler_params=pltpu.CompilerParams(collective_id=0, has_side_effects=True, vmem_limit_bytes=60 * MIB),
        name="fused_block",
    )(xw, w_one, w_two, bias)
    return outs[0]


def images_major(yt):
    groups, h_loc, cols, ni, cb = yt.shape
    parts = h_loc // ni
    chunks = groups * parts
    assert ni == 16

    def kernel(y, out, y_in, y_out, swap, in_sem, out_sem):
        def load(e):
            cut = (lax.div(e, parts), pl.ds(pl.multiple_of(ni * lax.rem(e, parts), ni), ni))
            return pltpu.make_async_copy(y.at[cut], y_in.at[cut], in_sem.at[e])

        def store(e):
            cut = (pl.ds(pl.multiple_of(ni * lax.div(e, parts), ni), ni), slice(None), pl.ds(pl.multiple_of(ni * lax.rem(e, parts), ni), ni))
            return pltpu.make_async_copy(y_out.at[cut], out.at[cut], out_sem.at[e])

        for e in range(chunks):
            load(jnp.int32(e)).start()
        swap[...] = swap_matrix(ni)

        def chunk(e, carry):
            load(e).wait()
            group, part = lax.div(e, parts), lax.rem(e, parts)
            h0 = pl.multiple_of(ni * part, ni)
            n0 = pl.multiple_of(ni * group, ni)
            for col in range(cols):
                rows_in = y_in[group, pl.ds(h0, ni), col].reshape(ni * ni, cb)
                res = jnp.dot(swap[...], rows_in, preferred_element_type=jnp.float32)
                y_out[pl.ds(n0, ni), col, pl.ds(h0, ni)] = res.astype(jnp.bfloat16).reshape(ni, ni, cb)
            store(e).start()
            return carry

        lax.fori_loop(0, chunks, chunk, 0)
        for e in range(chunks):
            store(jnp.int32(e)).wait()

    dma = pltpu.SemaphoreType.DMA
    out_shape = (groups * ni, cols, h_loc, cb)
    return pl.pallas_call(
        kernel,
        out_shape=jax.ShapeDtypeStruct(out_shape, jnp.bfloat16),
        in_specs=[pl.BlockSpec(memory_space=pl.ANY)],
        out_specs=pl.BlockSpec(memory_space=pl.ANY),
        scratch_shapes=[pltpu.VMEM(yt.shape, jnp.bfloat16), pltpu.VMEM(out_shape, jnp.bfloat16), pltpu.VMEM((ni * ni, ni * ni), jnp.bfloat16),
                        dma((chunks,)), dma((chunks,))],
        compiler_params=pltpu.CompilerParams(vmem_limit_bytes=60 * MIB),
        name="images_major",
    )(yt)


def solution(mesh):
    act_spec = P("dp", "sp", None, "cp")
    kernel_spec = P(None, None, "cp", None)

    def local_block(x_tile, w_one_part, w_two_part, bias_one):
        xw = x_tile.transpose(0, 2, 1, 3)
        yt = fused_block(xw, w_one_part, w_two_part, bias_one.reshape(8, 1, 2 * x_tile.shape[3]))
        return images_major(yt).transpose(0, 2, 1, 3)

    return jax.shard_map(local_block, mesh=mesh, in_specs=(act_spec, kernel_spec, kernel_spec, P()), out_specs=act_spec, check_vma=False)
```

```python
import functools

import jax
import jax.numpy as jnp
from jax import lax
from jax.experimental import pallas as pl
from jax.experimental.pallas import tpu as pltpu
from jax.sharding import PartitionSpec as P

MESH = pl.DeviceIdType.MESH
N_STEPS = 64
MIB = 1024 * 1024
ONE, TWO, THREE, FOUR, ALL = (1,), (2,), (3,), (4,), (2, 16)
GRID, CUBE, HALVES = (2, 2), (2, 2, 2), (4, 2)
THIRDS = (4, 2, 2)
SEMS = (
    TWO, TWO, TWO, TWO, TWO, ONE, THREE, THREE, THREE, TWO, FOUR,
    HALVES, HALVES, HALVES, HALVES, HALVES, HALVES, THIRDS, THIRDS,
    CUBE, CUBE, GRID, GRID, GRID, GRID, CUBE, CUBE,
    ALL, ALL, TWO, TWO, ONE, ONE, ONE,
)


def pair(e):
    return e >> 1, e & 1


def odd(i):
    return (i & 1) == 1


def swap_matrix(n):
    to = lax.broadcasted_iota(jnp.int32, (n * n, n * n), 0)
    frm = lax.broadcasted_iota(jnp.int32, (n * n, n * n), 1)
    hit = (lax.div(to, n) == lax.rem(frm, n)) & (lax.rem(to, n) == lax.div(frm, n))
    return jnp.where(hit, 1.0, 0.0).astype(jnp.bfloat16)


def fused_block(xw, w_one, w_two, bias):
    images, cols, h_loc, cb = xw.shape
    ni = images // 2
    rows = h_loc // 2
    m_rows = rows * ni
    tile = 2 * cb
    assert ni == 16 and h_loc == 48

    def remote(src, dst, send_sem, recv_sem, sp, cp):
        return pltpu.make_async_remote_copy(src_ref=src, dst_ref=dst, send_sem=send_sem, recv_sem=recv_sem,
                                            device_id={"sp": sp, "cp": cp}, device_id_type=MESH)

    def kernel(xw, w1, w2, b1, yt, g1, g2, part, hid,
               xa, acc, wv, stage, raw, swap,
               wsem, asem, pst, pld, stl, zsem, rsem, xs, xr, hs, hr,
               p1s, p1r, x1s, x1r, y1s, y1r, f1s, f1r,
               p2s, p2r, x2s, x2r, y2s, y2r, f2s, f2r,
               as_, ar, ys, yr, zs, zr, yl):
        sp = lax.axis_index("sp")
        k = lax.axis_index("cp")
        x = (k >> 1)
        c = (k & 1)
        blk = 2 * sp + c
        osp = 1 - sp
        k1 = 2 * x + (1 - c)
        k2 = 2 * (1 - x) + c
        k3 = 2 * (1 - x) + (1 - c)

        def tile_of(xx, j, par):
            return 4 * ((xx + (j >> 1)) & 1) + 2 * (j & 1) + par

        barrier = pltpu.get_barrier_semaphore()
        for d_sp in range(2):
            for d_cp in range(4):
                if d_sp or d_cp:
                    pl.semaphore_signal(barrier, inc=1, device_id={"sp": ((sp + d_sp) & 1), "cp": ((k + d_cp) & 3)},
                                        device_id_type=MESH)

        def raw_load(xx, part):
            cut = pl.ds(pl.multiple_of(ni * part, ni), ni)
            return pltpu.make_async_copy(xw.at[pl.ds(ni * xx, ni), :, cut], raw.at[:, :, cut], rsem.at[part])

        def block(col, part):
            rows_in = raw[:, col, pl.ds(pl.multiple_of(ni * part, ni), ni), :].reshape(ni * ni, cb)
            out = jnp.dot(swap[...], rows_in, preferred_element_type=jnp.float32)
            return out.astype(jnp.bfloat16).reshape(ni, ni, cb)

        def slot_of(cc, slot_same):
            return jnp.where(cc == c, slot_same, 4)

        def swap_end(xx, cc, slot_same):
            raw_load(xx, 2 * cc).wait()
            for col in range(cols):
                xa[slot_of(cc, slot_same), pl.ds(1 + 8 * cc, ni), col] = block(col, 2 * cc)

        def swap_mid(xx, slot_same):
            raw_load(xx, 1).wait()
            for col in range(cols):
                mid = block(col, 1)
                xa[slot_of(0, slot_same), 17:26, col] = mid[0:9]
                xa[slot_of(1, slot_same), 0:9, col] = mid[7:16]

        def x_copy(role):
            cc = c if role == 2 else 1 - c
            cut = pl.ds(1 - cc, rows + 1)
            return remote(xa.at[5 if role == 2 else 4, cut], xa.at[role, cut], xs.at[role - 1], xr.at[role - 1], sp,
                          {1: k1, 2: k2, 3: k3}[role])

        def halo_copy(xx, slot_same):
            role = 2 * ((x + xx) & 1) + ((c + sp) & 1)
            src = xa.at[slot_of(osp, slot_same), jnp.where(sp == 0, rows, 1)]
            return remote(src, xa.at[role, (rows + 1) * sp], hs.at[xx], hr.at[role], osp, 2 * xx + sp)

        half = cb // 2

        def w1_own(j, par, xx):
            return w1.at[:, :, :, pl.ds(pl.multiple_of(tile_of(xx, j, par) * tile, tile), tile)]

        def w1_part(j, par):
            return remote(w1_own(j, par, x), g1.at[0, j, par], p1s.at[j, par], p1r.at[j, par], sp, k1)

        def w1_x(j, hf):
            cut = pl.ds(pl.multiple_of(hf * half, half), half)
            src = w1.at[:, :, cut, pl.ds(pl.multiple_of(tile_of(1 - x, j, sp) * tile, tile), tile)]
            return remote(src, g1.at[1, j, sp, :, :, cut], x1s.at[j, hf], x1r.at[j, hf], sp, k2)

        def w1_y(j, hf):
            cut = pl.ds(pl.multiple_of(hf * half, half), half)
            ref = g1.at[1, j, sp, :, :, cut]
            return remote(ref, ref, y1s.at[j, hf], y1r.at[j, hf], osp, k)

        def w1_fwd(j, par, hf):
            cut = pl.ds(pl.multiple_of(hf * half, half), half)
            return remote(g1.at[1, j, par, :, :, cut], g1.at[2, j, par, :, :, cut], f1s.at[j, par, hf], f1r.at[j, par, hf], sp, k1)

        def w2_cut(n, par, h, xx):
            row = pl.multiple_of(par * tile + h * cb, cb)
            col = pl.multiple_of(tile * ((1 + xx + n) & 1), tile)
            return w2.at[:, :, pl.ds(row, cb), pl.ds(col, tile)]

        def w2_part(n, par, h):
            return remote(w2_cut(n, par, h, x), g2.at[0, n, par, h], p2s.at[n, par, h], p2r.at[n, par, h], sp, k1)

        def w2_x(n, h):
            return remote(w2_cut(n, sp, h, 1 - x), g2.at[1, n, sp, h], x2s.at[n, h], x2r.at[n, h], sp, k2)

        def w2_y(n, h):
            ref = g2.at[1, n, sp, h]
            return remote(ref, ref, y2s.at[n, h], y2r.at[n, h], osp, k)

        def w2_fwd(n, par, h):
            return remote(g2.at[1, n, par, h], g2.at[2, n, par, h], f2s.at[n, par, h], f2r.at[n, par, h], sp, k1)

        up_blk = lax.max(blk - 1, 0)
        dn_blk = lax.min(blk + 1, 3)

        def hid_up(a):
            return remote(hid.at[a, 1], hid.at[a, rows + 1], as_.at[0, a], ar.at[1, a], (up_blk >> 1), 2 * x + (up_blk & 1))

        def hid_dn(a):
            return remote(hid.at[a, rows], hid.at[a, 0], as_.at[1, a], ar.at[0, a], (dn_blk >> 1), 2 * x + (dn_blk & 1))

        def hid_store(a, h):
            return pltpu.make_async_copy(stage.at[h], hid.at[a, pl.ds(1, rows)], stl.at[h])

        y_rows = pl.ds(rows * c, rows)

        def y_far(h):
            return remote(stage.at[h], yt.at[x, y_rows], ys.at[h], yr.at[((h + c) & 1)], sp, 2 * (1 - x) + h)

        def y_near():
            return remote(stage.at[1 - c], yt.at[x, y_rows], zs.at[0], zr.at[0], sp, k1)

        def y_own():
            return pltpu.make_async_copy(stage.at[c], yt.at[x, y_rows], yl.at[0])

        def zero_rows(row):
            return pltpu.make_async_copy(stage.at[0, pl.ds(0, 16)], hid.at[:, row], zsem.at[0])

        def p_of(m):
            return (m + 2) & 7

        def jp(p):
            return p >> 1, (sp + p) & 1

        def near_step(i):
            return 2 * (i >> 2) + (i & 1), (i & 2) >> 1

        def halo_wait(role):
            @pl.when(c != sp)
            def _():
                remote(xa.at[0, 0], xa.at[role, 0], hs.at[0], hr.at[role], osp, k).wait_recv()

        for part_no in (2 * osp, 1, 2 * sp):
            raw_load(x, part_no).start()
        swap[...] = swap_matrix(ni)
        stage[0, 0:16] = jnp.zeros((16, cols, ni, cb), jnp.bfloat16)

        @pl.when(blk == 0)
        def _():
            xa[0:4, 0] = jnp.zeros((4, cols, ni, cb), jnp.bfloat16)
            zero_rows(0).start()

        @pl.when(blk == 3)
        def _():
            xa[0:4, rows + 1] = jnp.zeros((4, cols, ni, cb), jnp.bfloat16)
            zero_rows(rows + 1).start()

        def w_load(src, t):
            return pltpu.make_async_copy(src, wv.at[(t & 1)], wsem.at[(t & 1)])

        def hid_load(a, q):
            slot = (q & 1)
            return pltpu.make_async_copy(hid.at[a], xa.at[4 + slot], asem.at[slot])

        def issue(t):
            @pl.when(t < 16)
            def _():
                m, role = near_step(t)
                j, par = jp(p_of(m))

                @pl.when(role == 0)
                def _():
                    w_load(w1_own(j, par, x), t).start()

                @pl.when(role == 1)
                def _():
                    w1_part(j, par).wait_recv()
                    w_load(g1.at[0, j, par], t).start()

            @pl.when((t >= 16) & (t < 32))
            def _():
                j, par = jp(((t - 16) >> 1))

                @pl.when((t & 1) == 1)
                def _():
                    for hf in range(2):
                        w1_fwd(j, par, hf).wait_recv()

                w_load(g1.at[1 + (t & 1), j, par], t).start()

            @pl.when((t >= 32) & (t < N_STEPS))
            def _():
                n = ((t - 32) >> 4)
                q = ((t - 32) & 15)
                h = (q & 1)
                p = (q >> 1)
                j, par = jp(p)
                a = 4 * j + 2 * par + h
                same = (j & 1) == c

                @pl.when(n == 0)
                def _():
                    @pl.when(blk > 0)
                    def _():
                        hid_dn(a).wait_recv()

                    @pl.when(blk < 3)
                    def _():
                        hid_up(a).wait_recv()

                hid_load(a, q).start()

                @pl.when(p < 4)
                def _():
                    @pl.when(same)
                    def _():
                        w_load(w2_cut(n, par, h, x), t).start()

                    @pl.when(jnp.logical_not(same))
                    def _():
                        w2_part(n, par, h).wait_recv()
                        w_load(g2.at[0, n, par, h], t).start()

                @pl.when(p >= 4)
                def _():
                    @pl.when(jnp.logical_not(same))
                    def _():
                        w2_fwd(n, par, h).wait_recv()

                    w_load(g2.at[jnp.where(same, 1, 2), n, par, h], t).start()

        issue(jnp.int32(0))
        with jax.named_scope("swap"):
            swap_end(x, osp, 0)
        with jax.named_scope("bar"):
            pl.semaphore_wait(barrier, 7)

        @pl.when(c == sp)
        def _():
            halo_copy(x, 0).start()

        for e in range(3):
            w1_x(*divmod(e, 2)).start()
        with jax.named_scope("swap2"):
            swap_end(x, sp, 0)
            swap_mid(x, 0)
        x_copy(1).start()
        for m in range(2):
            w1_part(*jp(jnp.int32(m + 2))).start()

        for part_no in range(3):
            raw_load(1 - x, part_no).start()
        with jax.named_scope("halo"):
            halo_wait(0)

        def pass_w1_x(e):
            j, hf = pair(e)
            w1_x(j, hf).wait_recv()
            w1_y(j, hf).start()
            w1_fwd(j, sp, hf).start()

        def pass_w1_y(e):
            j, hf = pair(e)
            w1_y(j, hf).wait_recv()
            w1_fwd(j, osp, hf).start()

        def pass_w2_x(e):
            n, h = pair(e)
            w2_x(n, h).wait_recv()
            w2_y(n, h).start()
            w2_fwd(n, sp, h).start()

        def pass_w2_y(e):
            n, h = pair(e)
            w2_y(n, h).wait_recv()
            w2_fwd(n, osp, h).start()

        def send_w1_x(e):
            w1_x(*pair(e)).start()

        def send_w2_x(e):
            w2_x(*pair(e)).start()

        def events(i):
            is_odd = odd(i)
            even = jnp.logical_not(is_odd)

            @pl.when(i < 16)
            def _():
                @pl.when(even)
                def _():
                    @pl.when(i < 12)
                    def _():
                        w1_part(*jp(p_of((i >> 1) + 2))).start()

                    @pl.when(i == 2)
                    def _():
                        x_copy(1).wait_recv()
                        halo_wait(1)

                    @pl.when(i == 10)
                    def _():
                        for e in range(2):
                            pass_w1_y(jnp.int32(e))

                    @pl.when(i == 12)
                    def _():
                        pass_w1_y(jnp.int32(2))

                @pl.when(is_odd)
                def _():
                    @pl.when((i == 1) & (c != sp))
                    def _():
                        halo_copy(x, 0).start()

                    @pl.when(i == 3)
                    def _():
                        x_copy(1).wait_send()
                        halo_copy(x, 0).wait_send()
                        for cc in range(2):
                            swap_end(1 - x, cc, 5)
                        swap_mid(1 - x, 5)
                        halo_copy(1 - x, 5).start()
                        x_copy(2).start()

                    @pl.when(i == 5)
                    def _():
                        for e in range(2):
                            pass_w1_x(jnp.int32(e))

                    @pl.when(i == 7)
                    def _():
                        pass_w1_x(jnp.int32(2))

                    @pl.when(i == 9)
                    def _():
                        x_copy(3).start()

                    @pl.when(i >= 13)
                    def _():
                        send_w1_x(((i - 7) >> 1))

            @pl.when((i >= 16) & (i < 34))
            def _():
                @pl.when(i < 24)
                def _():
                    e = i - 16
                    w2_part((e >> 2), ((e >> 1) & 1), (e & 1)).start()

                @pl.when(even)
                def _():
                    @pl.when(i == 16)
                    def _():
                        x_copy(2).wait_recv()
                        halo_wait(2)

                    @pl.when(i == 30)
                    def _():
                        x_copy(2).wait_send()
                        x_copy(3).wait_send()
                        halo_copy(1 - x, 5).wait_send()

                    @pl.when((i >= 24) & ((i & 3) == 0))
                    def _():
                        send_w2_x(((i - 24) >> 2))

                    @pl.when((i >= 18) & (i <= 26))
                    def _():
                        pass_w1_x(((i - 12) >> 1))

                @pl.when(is_odd)
                def _():
                    @pl.when(i == 17)
                    def _():
                        x_copy(3).wait_recv()
                        halo_wait(3)

                    @pl.when(i <= 21)
                    def _():
                        send_w1_x(((i - 7) >> 1))

                    @pl.when(i >= 19)
                    def _():
                        for h in range(2):
                            hid_store(0, h).wait()

                    @pl.when((i >= 21) & (i <= 29))
                    def _():
                        pass_w1_y(((i - 15) >> 1))

                    @pl.when(i >= 27)
                    def _():
                        for d in range(2):
                            j, par = jp(i - 27 + d)
                            for h in range(2):
                                a = 4 * j + 2 * par + h

                                @pl.when(blk > 0)
                                def _():
                                    hid_up(a).start()

                                @pl.when(blk < 3)
                                def _():
                                    hid_dn(a).start()

                    @pl.when(i == 31)
                    def _():
                        pass_w2_x(jnp.int32(0))

            @pl.when((i >= 34) & (i < 50))
            def _():
                @pl.when(i == 36)
                def _():
                    send_w2_x(jnp.int32(3))

                @pl.when((i < 44) & ((i & 3) == 3))
                def _():
                    pass_w2_x(((i - 31) >> 2))

                @pl.when((i >= 37) & ((i & 3) == 1))
                def _():
                    pass_w2_y(((i - 37) >> 2))

        def taps(xs_slot, ws_slot, col, lanes=slice(None)):
            total = None
            for dx in (-1, 0, 1):
                if not 0 <= col + dx < cols:
                    continue
                for dy in range(3):
                    lhs = xa[xs_slot, dy:dy + rows, col + dx].reshape(m_rows, cb)
                    prod = jnp.dot(lhs, wv[ws_slot, dy, dx + 1, :, lanes], preferred_element_type=jnp.float32)
                    total = prod if total is None else total + prod
            return total

        def step(i, carry):
            ph1 = i < 16
            ph3 = i >= 32
            n = jnp.where(ph3, ((i - 32) >> 4), 0)
            q = jnp.where(ph3, ((i - 32) & 15), 0)
            m, role = near_step(i)
            m = jnp.where(ph1, m, ((i - 16) >> 1))
            role = jnp.where(ph1, role, 2 + (i & 1))
            p = jnp.where(ph1, p_of(m), (m & 7))
            p = jnp.where(ph3, 0, p)
            last = jnp.where(ph3, q == 15, role == 3)
            first = jnp.where(ph3, q == 0, role == 0)
            a_slot = jnp.where(ph3, n, (p & 1))
            x_slot = jnp.where(ph3, 4 + (q & 1), role)
            w_slot = (i & 1)

            with jax.named_scope("ev"):
                events(i)
            with jax.named_scope("iss"):
                issue(i + 1)
            w_load(g1.at[0, 0, 0], i).wait()

            @pl.when(ph3)
            def _():
                hid_load(0, q).wait()

            @pl.when((i >= 4) & (i < 32))
            def _():
                @pl.when(ph1 & first)
                def _():
                    pltpu.make_async_copy(acc.at[a_slot], part.at[0], pst.at[a_slot]).wait()

                @pl.when((i >= 20) & (role == 2))
                def _():
                    pltpu.make_async_copy(part.at[0], acc.at[a_slot], pld.at[a_slot]).wait()

            @pl.when(jnp.logical_not(last))
            def _():
                with jax.named_scope("mm"):
                    for col in range(cols):
                        total = taps(x_slot, w_slot, col)
                        acc[a_slot, col] = total + jnp.where(first, 0.0, acc[a_slot, col])

            @pl.when((i < 12) & (role == 1))
            def _():
                pltpu.make_async_copy(acc.at[a_slot], part.at[p], pst.at[a_slot]).start()

            @pl.when(last & (i < N_STEPS - 1))
            def _():
                @pl.when((i == 17) & ((blk == 0) | (blk == 3)))
                def _():
                    zero_rows(0).wait()

                keep = jnp.where(ph3, 1.0, 0.0)
                floor = jnp.where(ph3, -jnp.inf, 0.0)
                j, par = jp(p)
                shift = b1[tile_of(x, j, par)] * (1.0 - keep)
                with jax.named_scope("mmo"):
                    for col in range(cols):
                        total = taps(x_slot, w_slot, col) + acc[a_slot, col] + shift
                        for h in range(2):
                            role = 2 + ((c + h) & 1)
                            res = xa[role, 1:rows + 1, col].reshape(m_rows, cb).astype(jnp.float32)
                            val = jnp.maximum(total[:, h * cb:(h + 1) * cb] + res * keep, floor)
                            stage[h, :, col] = val.astype(jnp.bfloat16).reshape(rows, ni, cb)

                @pl.when(i < 32)
                def _():
                    for h in range(2):
                        hid_store(4 * j + 2 * par + h, h).start()

                    @pl.when(p < 6)
                    def _():
                        pltpu.make_async_copy(part.at[p + 2], acc.at[a_slot], pld.at[a_slot]).start()

                @pl.when(i == 47)
                def _():
                    for h in range(2):
                        y_far(h).start()

            @pl.when(i == N_STEPS - 1)
            def _():
                for h in range(2):
                    y_far(h).wait_send()

                def half_step(own, carry):
                    h = jnp.where(own == 1, c, 1 - c)
                    lanes = pl.ds(pl.multiple_of(h * cb, cb), cb)
                    with jax.named_scope("half"):
                        for col in range(cols):
                            total = taps(x_slot, w_slot, col, lanes) + acc[a_slot, col, :, lanes]
                            res = xa[1 - own, 1:rows + 1, col].reshape(m_rows, cb).astype(jnp.float32)
                            stage[h, :, col] = (total + res).astype(jnp.bfloat16).reshape(rows, ni, cb)

                    @pl.when(own == 0)
                    def _():
                        y_near().start()

                    return carry

                lax.fori_loop(0, 2, half_step, 0)
                y_own().start()

            return carry

        lax.fori_loop(0, N_STEPS, step, 0)

        def drain(e, carry):
            hi, lo = pair(e)
            w1_part(hi, lo).wait_send()
            w1_x(hi, lo).wait_send()
            w1_y(hi, lo).wait_send()
            for hf in range(2):
                w1_fwd(hi, lo, hf).wait_send()
            n, par = (e >> 2), ((e >> 1) & 1)
            w2_part(n, par, lo).wait_send()
            w2_fwd(n, par, lo).wait_send()
            return carry

        lax.fori_loop(0, 8, drain, 0)

        def drain_rows(a, carry):
            @pl.when(blk > 0)
            def _():
                hid_up(a).wait_send()

            @pl.when(blk < 3)
            def _():
                hid_dn(a).wait_send()

            return carry

        lax.fori_loop(0, 16, drain_rows, 0)

        def drain_two(e, carry):
            w2_x(*pair(e)).wait_send()
            w2_y(*pair(e)).wait_send()
            return carry

        lax.fori_loop(0, 4, drain_two, 0)
        for e in range(2):
            remote(stage.at[0], yt.at[0, pl.ds(0, rows)], ys.at[0], yr.at[e], sp, k).wait_recv()
        y_near().wait()
        y_own().wait()

    dma = pltpu.SemaphoreType.DMA
    bf16, f32 = jnp.bfloat16, jnp.float32
    any_space = pl.BlockSpec(memory_space=pl.ANY)
    outs = pl.pallas_call(
        kernel,
        out_shape=[
            jax.ShapeDtypeStruct((2, h_loc, cols, ni, cb), bf16),
            jax.ShapeDtypeStruct((3, 4, 2, 3, 3, cb, tile), bf16),
            jax.ShapeDtypeStruct((3, 2, 2, 2, 3, 3, cb, tile), bf16),
            jax.ShapeDtypeStruct((8, cols, m_rows, tile), f32),
            jax.ShapeDtypeStruct((16, rows + 2, cols, ni, cb), bf16),
        ],
        in_specs=[any_space, any_space, any_space, pl.BlockSpec(memory_space=pltpu.VMEM)],
        out_specs=[any_space] * 5,
        scratch_shapes=[
            pltpu.VMEM((6, rows + 2, cols, ni, cb), bf16),
            pltpu.VMEM((2, cols, m_rows, tile), f32),
            pltpu.VMEM((2, 3, 3, cb, tile), bf16),
            pltpu.VMEM((2, rows, cols, ni, cb), bf16),
            pltpu.VMEM((ni, cols, h_loc, cb), bf16),
            pltpu.VMEM((ni * ni, ni * ni), bf16),
            *map(dma, SEMS),
        ],
        compiler_params=pltpu.CompilerParams(collective_id=0, has_side_effects=True, vmem_limit_bytes=60 * MIB),
        name="fused_block",
    )(xw, w_one, w_two, bias)
    return outs[0]


def images_major(yt):
    groups, h_loc, cols, ni, cb = yt.shape
    parts = h_loc // ni
    chunks = groups * parts
    assert ni == 16

    def kernel(y, out, y_in, y_out, swap, in_sem, out_sem):
        def load(e):
            cut = (lax.div(e, parts), pl.ds(pl.multiple_of(ni * lax.rem(e, parts), ni), ni))
            return pltpu.make_async_copy(y.at[cut], y_in.at[cut], in_sem.at[e])

        def store(e):
            cut = (pl.ds(pl.multiple_of(ni * lax.div(e, parts), ni), ni), slice(None), pl.ds(pl.multiple_of(ni * lax.rem(e, parts), ni), ni))
            return pltpu.make_async_copy(y_out.at[cut], out.at[cut], out_sem.at[e])

        for e in range(chunks):
            load(jnp.int32(e)).start()
        swap[...] = swap_matrix(ni)

        def chunk(e, carry):
            load(e).wait()
            group, part = lax.div(e, parts), lax.rem(e, parts)
            h0 = pl.multiple_of(ni * part, ni)
            n0 = pl.multiple_of(ni * group, ni)
            for col in range(cols):
                rows_in = y_in[group, pl.ds(h0, ni), col].reshape(ni * ni, cb)
                res = jnp.dot(swap[...], rows_in, preferred_element_type=jnp.float32)
                y_out[pl.ds(n0, ni), col, pl.ds(h0, ni)] = res.astype(jnp.bfloat16).reshape(ni, ni, cb)
            store(e).start()
            return carry

        lax.fori_loop(0, chunks, chunk, 0)
        for e in range(chunks):
            store(jnp.int32(e)).wait()

    dma = pltpu.SemaphoreType.DMA
    out_shape = (groups * ni, cols, h_loc, cb)
    return pl.pallas_call(
        kernel,
        out_shape=jax.ShapeDtypeStruct(out_shape, jnp.bfloat16),
        in_specs=[pl.BlockSpec(memory_space=pl.ANY)],
        out_specs=pl.BlockSpec(memory_space=pl.ANY),
        scratch_shapes=[pltpu.VMEM(yt.shape, jnp.bfloat16), pltpu.VMEM(out_shape, jnp.bfloat16), pltpu.VMEM((ni * ni, ni * ni), jnp.bfloat16),
                        dma((chunks,)), dma((chunks,))],
        compiler_params=pltpu.CompilerParams(vmem_limit_bytes=60 * MIB),
        name="images_major",
    )(yt)


def solution(mesh):
    act_spec = P("dp", "sp", None, "cp")
    kernel_spec = P(None, None, "cp", None)

    def local_block(x_tile, w_one_part, w_two_part, bias_one):
        xw = x_tile.transpose(0, 2, 1, 3)
        yt = fused_block(xw, w_one_part, w_two_part, bias_one.reshape(8, 1, 2 * x_tile.shape[3]))
        return images_major(yt).transpose(0, 2, 1, 3)

    return jax.shard_map(local_block, mesh=mesh, in_specs=(act_spec, kernel_spec, kernel_spec, P()), out_specs=act_spec, check_vma=False)
```

```python
import functools

import jax
import jax.numpy as jnp
from jax import lax
from jax.experimental import pallas as pl
from jax.experimental.pallas import tpu as pltpu
from jax.sharding import PartitionSpec as P

MESH = pl.DeviceIdType.MESH
N_STEPS = 64
MIB = 1024 * 1024
ONE, TWO, THREE, FOUR, ALL = (1,), (2,), (3,), (4,), (2, 16)
GRID, CUBE, HALVES = (2, 2), (2, 2, 2), (4, 2)
THIRDS = (4, 2, 2)
SEMS = (
    TWO, TWO, TWO, TWO, TWO, ONE, (2, 3), THREE, THREE, TWO, FOUR,
    HALVES, HALVES, HALVES, HALVES, HALVES, HALVES, THIRDS, THIRDS,
    CUBE, CUBE, GRID, GRID, GRID, GRID, CUBE, CUBE,
    ALL, ALL, TWO, TWO, ONE, ONE, ONE,
)


def pair(e):
    return e >> 1, e & 1


def odd(i):
    return (i & 1) == 1


def swap_matrix(n):
    to = lax.broadcasted_iota(jnp.int32, (n * n, n * n), 0)
    frm = lax.broadcasted_iota(jnp.int32, (n * n, n * n), 1)
    hit = (lax.div(to, n) == lax.rem(frm, n)) & (lax.rem(to, n) == lax.div(frm, n))
    return jnp.where(hit, 1.0, 0.0).astype(jnp.bfloat16)


def fused_block(xw, w_one, w_two, bias):
    images, cols, h_loc, cb = xw.shape
    ni = images // 2
    rows = h_loc // 2
    m_rows = rows * ni
    tile = 2 * cb
    assert ni == 16 and h_loc == 48

    def remote(src, dst, send_sem, recv_sem, sp, cp):
        return pltpu.make_async_remote_copy(src_ref=src, dst_ref=dst, send_sem=send_sem, recv_sem=recv_sem,
                                            device_id={"sp": sp, "cp": cp}, device_id_type=MESH)

    def kernel(xw, w1, w2, b1, yt, g1, g2, part, hid,
               xa, acc, wv, stage, raw, swap,
               wsem, asem, pst, pld, stl, zsem, rsem, xs, xr, hs, hr,
               p1s, p1r, x1s, x1r, y1s, y1r, f1s, f1r,
               p2s, p2r, x2s, x2r, y2s, y2r, f2s, f2r,
               as_, ar, ys, yr, zs, zr, yl):
        sp = lax.axis_index("sp")
        k = lax.axis_index("cp")
        x = (k >> 1)
        c = (k & 1)
        blk = 2 * sp + c
        osp = 1 - sp
        k1 = 2 * x + (1 - c)
        k2 = 2 * (1 - x) + c
        k3 = 2 * (1 - x) + (1 - c)

        def tile_of(xx, j, par):
            return 4 * ((xx + (j >> 1)) & 1) + 2 * (j & 1) + par

        barrier = pltpu.get_barrier_semaphore()
        for d_sp in range(2):
            for d_cp in range(4):
                if d_sp or d_cp:
                    pl.semaphore_signal(barrier, inc=1, device_id={"sp": ((sp + d_sp) & 1), "cp": ((k + d_cp) & 3)},
                                        device_id_type=MESH)

        def raw_load(far, part):
            cut = pl.ds(pl.multiple_of(ni * part, ni), ni)
            group = pl.ds(ni * (1 - x if far else x), ni)
            return pltpu.make_async_copy(xw.at[group, :, cut], raw.at[far, :, :, cut], rsem.at[far, part])

        def block(far, col, part):
            rows_in = raw[far, :, col, pl.ds(pl.multiple_of(ni * part, ni), ni), :].reshape(ni * ni, cb)
            out = jnp.dot(swap[...], rows_in, preferred_element_type=jnp.float32)
            return out.astype(jnp.bfloat16).reshape(ni, ni, cb)

        def slot_of(far, cc):
            return jnp.where(cc == c, 5 if far else 0, 6 if far else 4)

        def swap_end(far, cc):
            raw_load(far, 2 * cc).wait()
            for col in range(cols):
                xa[slot_of(far, cc), pl.ds(1 + 8 * cc, ni), col] = block(far, col, 2 * cc)

        def swap_mid(far):
            raw_load(far, 1).wait()
            for col in range(cols):
                mid = block(far, col, 1)
                xa[slot_of(far, 0), 17:26, col] = mid[0:9]
                xa[slot_of(far, 1), 0:9, col] = mid[7:16]

        def x_copy(role):
            cc = c if role == 2 else 1 - c
            cut = pl.ds(1 - cc, rows + 1)
            return remote(xa.at[3 + role, cut], xa.at[role, cut], xs.at[role - 1], xr.at[role - 1], sp,
                          {1: k1, 2: k2, 3: k3}[role])

        def halo_copy(far):
            xx = 1 - x if far else x
            role = 2 * ((x + xx) & 1) + ((c + sp) & 1)
            src = xa.at[slot_of(far, osp), jnp.where(sp == 0, rows, 1)]
            return remote(src, xa.at[role, (rows + 1) * sp], hs.at[far], hr.at[role], osp, 2 * xx + sp)

        half = cb // 2

        def w1_own(j, par, xx):
            return w1.at[:, :, :, pl.ds(pl.multiple_of(tile_of(xx, j, par) * tile, tile), tile)]

        def w1_part(j, par):
            return remote(w1_own(j, par, x), g1.at[0, j, par], p1s.at[j, par], p1r.at[j, par], sp, k1)

        def w1_x(j, hf):
            cut = pl.ds(pl.multiple_of(hf * half, half), half)
            src = w1.at[:, :, cut, pl.ds(pl.multiple_of(tile_of(1 - x, j, sp) * tile, tile), tile)]
            return remote(src, g1.at[1, j, sp, :, :, cut], x1s.at[j, hf], x1r.at[j, hf], sp, k2)

        def w1_y(j, hf):
            cut = pl.ds(pl.multiple_of(hf * half, half), half)
            ref = g1.at[1, j, sp, :, :, cut]
            return remote(ref, ref, y1s.at[j, hf], y1r.at[j, hf], osp, k)

        def w1_fwd(j, par, hf):
            cut = pl.ds(pl.multiple_of(hf * half, half), half)
            return remote(g1.at[1, j, par, :, :, cut], g1.at[2, j, par, :, :, cut], f1s.at[j, par, hf], f1r.at[j, par, hf], sp, k1)

        def w2_cut(n, par, h, xx):
            row = pl.multiple_of(par * tile + h * cb, cb)
            col = pl.multiple_of(tile * ((1 + xx + n) & 1), tile)
            return w2.at[:, :, pl.ds(row, cb), pl.ds(col, tile)]

        def w2_part(n, par, h):
            return remote(w2_cut(n, par, h, x), g2.at[0, n, par, h], p2s.at[n, par, h], p2r.at[n, par, h], sp, k1)

        def w2_x(n, h):
            return remote(w2_cut(n, sp, h, 1 - x), g2.at[1, n, sp, h], x2s.at[n, h], x2r.at[n, h], sp, k2)

        def w2_y(n, h):
            ref = g2.at[1, n, sp, h]
            return remote(ref, ref, y2s.at[n, h], y2r.at[n, h], osp, k)

        def w2_fwd(n, par, h):
            return remote(g2.at[1, n, par, h], g2.at[2, n, par, h], f2s.at[n, par, h], f2r.at[n, par, h], sp, k1)

        up_blk = lax.max(blk - 1, 0)
        dn_blk = lax.min(blk + 1, 3)

        def hid_up(a):
            return remote(hid.at[a, 1], hid.at[a, rows + 1], as_.at[0, a], ar.at[1, a], (up_blk >> 1), 2 * x + (up_blk & 1))

        def hid_dn(a):
            return remote(hid.at[a, rows], hid.at[a, 0], as_.at[1, a], ar.at[0, a], (dn_blk >> 1), 2 * x + (dn_blk & 1))

        def hid_store(a, h):
            return pltpu.make_async_copy(stage.at[h], hid.at[a, pl.ds(1, rows)], stl.at[h])

        y_rows = pl.ds(rows * c, rows)

        def y_far(h):
            return remote(stage.at[h], yt.at[x, y_rows], ys.at[h], yr.at[((h + c) & 1)], sp, 2 * (1 - x) + h)

        def y_near():
            return remote(stage.at[1 - c], yt.at[x, y_rows], zs.at[0], zr.at[0], sp, k1)

        def y_own():
            return pltpu.make_async_copy(stage.at[c], yt.at[x, y_rows], yl.at[0])

        def zero_rows(row):
            return pltpu.make_async_copy(stage.at[0, pl.ds(0, 16)], hid.at[:, row], zsem.at[0])

        def p_of(m):
            return (m + 2) & 7

        def jp(p):
            return p >> 1, (sp + p) & 1

        def near_step(i):
            return 2 * (i >> 2) + (i & 1), (i & 2) >> 1

        def halo_wait(role):
            @pl.when(c != sp)
            def _():
                remote(xa.at[0, 0], xa.at[role, 0], hs.at[0], hr.at[role], osp, k).wait_recv()

        for part_no in (2 * osp, 2 * sp, 1):
            raw_load(0, part_no).start()
        for part_no in range(3):
            raw_load(1, part_no).start()
        swap[...] = swap_matrix(ni)
        stage[0, 0:16] = jnp.zeros((16, cols, ni, cb), jnp.bfloat16)

        @pl.when(blk == 0)
        def _():
            xa[0:4, 0] = jnp.zeros((4, cols, ni, cb), jnp.bfloat16)
            zero_rows(0).start()

        @pl.when(blk == 3)
        def _():
            xa[0:4, rows + 1] = jnp.zeros((4, cols, ni, cb), jnp.bfloat16)
            zero_rows(rows + 1).start()

        def w_load(src, t):
            return pltpu.make_async_copy(src, wv.at[(t & 1)], wsem.at[(t & 1)])

        def hid_load(a, q):
            slot = (q & 1)
            return pltpu.make_async_copy(hid.at[a], xa.at[4 + slot], asem.at[slot])

        def issue(t):
            @pl.when(t < 16)
            def _():
                m, role = near_step(t)
                j, par = jp(p_of(m))

                @pl.when(role == 0)
                def _():
                    w_load(w1_own(j, par, x), t).start()

                @pl.when(role == 1)
                def _():
                    w1_part(j, par).wait_recv()
                    w_load(g1.at[0, j, par], t).start()

            @pl.when((t >= 16) & (t < 32))
            def _():
                j, par = jp(((t - 16) >> 1))

                @pl.when((t & 1) == 1)
                def _():
                    for hf in range(2):
                        w1_fwd(j, par, hf).wait_recv()

                w_load(g1.at[1 + (t & 1), j, par], t).start()

            @pl.when((t >= 32) & (t < N_STEPS))
            def _():
                n = ((t - 32) >> 4)
                q = ((t - 32) & 15)
                h = (q & 1)
                p = (q >> 1)
                j, par = jp(p)
                a = 4 * j + 2 * par + h
                same = (j & 1) == c

                @pl.when(n == 0)
                def _():
                    @pl.when(blk > 0)
                    def _():
                        hid_dn(a).wait_recv()

                    @pl.when(blk < 3)
                    def _():
                        hid_up(a).wait_recv()

                hid_load(a, q).start()

                @pl.when(p < 4)
                def _():
                    @pl.when(same)
                    def _():
                        w_load(w2_cut(n, par, h, x), t).start()

                    @pl.when(jnp.logical_not(same))
                    def _():
                        w2_part(n, par, h).wait_recv()
                        w_load(g2.at[0, n, par, h], t).start()

                @pl.when(p >= 4)
                def _():
                    @pl.when(jnp.logical_not(same))
                    def _():
                        w2_fwd(n, par, h).wait_recv()

                    w_load(g2.at[jnp.where(same, 1, 2), n, par, h], t).start()

        issue(jnp.int32(0))
        with jax.named_scope("swap"):
            swap_end(0, osp)
        with jax.named_scope("bar"):
            pl.semaphore_wait(barrier, 7)

        @pl.when(c == sp)
        def _():
            halo_copy(0).start()

        for e in range(3):
            w1_x(*divmod(e, 2)).start()
        with jax.named_scope("swap2"):
            swap_end(0, sp)
            swap_mid(0)
        x_copy(1).start()
        for m in range(2):
            w1_part(*jp(jnp.int32(m + 2))).start()
        with jax.named_scope("swap3"):
            for cc in range(2):
                swap_end(1, cc)
            swap_mid(1)
        with jax.named_scope("halo"):
            halo_wait(0)

        def pass_w1_x(e):
            j, hf = pair(e)
            w1_x(j, hf).wait_recv()
            w1_y(j, hf).start()
            w1_fwd(j, sp, hf).start()

        def pass_w1_y(e):
            j, hf = pair(e)
            w1_y(j, hf).wait_recv()
            w1_fwd(j, osp, hf).start()

        def pass_w2_x(e):
            n, h = pair(e)
            w2_x(n, h).wait_recv()
            w2_y(n, h).start()
            w2_fwd(n, sp, h).start()

        def pass_w2_y(e):
            n, h = pair(e)
            w2_y(n, h).wait_recv()
            w2_fwd(n, osp, h).start()

        def send_w1_x(e):
            w1_x(*pair(e)).start()

        def send_w2_x(e):
            w2_x(*pair(e)).start()

        def events(i):
            is_odd = odd(i)
            even = jnp.logical_not(is_odd)

            @pl.when(i < 16)
            def _():
                @pl.when(even)
                def _():
                    @pl.when(i < 12)
                    def _():
                        w1_part(*jp(p_of((i >> 1) + 2))).start()

                    @pl.when(i == 2)
                    def _():
                        x_copy(1).wait_recv()
                        halo_wait(1)

                    @pl.when(i == 10)
                    def _():
                        for e in range(2):
                            pass_w1_y(jnp.int32(e))

                    @pl.when(i == 12)
                    def _():
                        pass_w1_y(jnp.int32(2))

                @pl.when(is_odd)
                def _():
                    @pl.when(i == 1)
                    def _():
                        @pl.when(c != sp)
                        def _():
                            halo_copy(0).start()

                        halo_copy(1).start()

                    @pl.when(i == 3)
                    def _():
                        x_copy(2).start()

                    @pl.when(i == 5)
                    def _():
                        for e in range(2):
                            pass_w1_x(jnp.int32(e))

                    @pl.when(i == 7)
                    def _():
                        pass_w1_x(jnp.int32(2))

                    @pl.when(i == 9)
                    def _():
                        x_copy(3).start()

                    @pl.when(i >= 13)
                    def _():
                        send_w1_x(((i - 7) >> 1))

            @pl.when((i >= 16) & (i < 34))
            def _():
                @pl.when(i < 24)
                def _():
                    e = i - 16
                    w2_part((e >> 2), ((e >> 1) & 1), (e & 1)).start()

                @pl.when(even)
                def _():
                    @pl.when(i == 16)
                    def _():
                        x_copy(2).wait_recv()
                        halo_wait(2)

                    @pl.when(i == 30)
                    def _():
                        x_copy(1).wait_send()
                        x_copy(2).wait_send()
                        x_copy(3).wait_send()
                        for far in range(2):
                            halo_copy(far).wait_send()

                    @pl.when((i >= 24) & ((i & 3) == 0))
                    def _():
                        send_w2_x(((i - 24) >> 2))

                    @pl.when((i >= 18) & (i <= 26))
                    def _():
                        pass_w1_x(((i - 12) >> 1))

                @pl.when(is_odd)
                def _():
                    @pl.when(i == 17)
                    def _():
                        x_copy(3).wait_recv()
                        halo_wait(3)

                    @pl.when(i <= 21)
                    def _():
                        send_w1_x(((i - 7) >> 1))

                    @pl.when(i >= 19)
                    def _():
                        for h in range(2):
                            hid_store(0, h).wait()

                    @pl.when((i >= 21) & (i <= 29))
                    def _():
                        pass_w1_y(((i - 15) >> 1))

                    @pl.when(i >= 27)
                    def _():
                        for d in range(2):
                            j, par = jp(i - 27 + d)
                            for h in range(2):
                                a = 4 * j + 2 * par + h

                                @pl.when(blk > 0)
                                def _():
                                    hid_up(a).start()

                                @pl.when(blk < 3)
                                def _():
                                    hid_dn(a).start()

                    @pl.when(i == 31)
                    def _():
                        pass_w2_x(jnp.int32(0))

            @pl.when((i >= 34) & (i < 50))
            def _():
                @pl.when(i == 36)
                def _():
                    send_w2_x(jnp.int32(3))

                @pl.when((i < 44) & ((i & 3) == 3))
                def _():
                    pass_w2_x(((i - 31) >> 2))

                @pl.when((i >= 37) & ((i & 3) == 1))
                def _():
                    pass_w2_y(((i - 37) >> 2))

        def taps(xs_slot, ws_slot, col, lanes=slice(None)):
            total = None
            for dx in (-1, 0, 1):
                if not 0 <= col + dx < cols:
                    continue
                for dy in range(3):
                    lhs = xa[xs_slot, dy:dy + rows, col + dx].reshape(m_rows, cb)
                    prod = jnp.dot(lhs, wv[ws_slot, dy, dx + 1, :, lanes], preferred_element_type=jnp.float32)
                    total = prod if total is None else total + prod
            return total

        def step(i, carry):
            ph1 = i < 16
            ph3 = i >= 32
            n = jnp.where(ph3, ((i - 32) >> 4), 0)
            q = jnp.where(ph3, ((i - 32) & 15), 0)
            m, role = near_step(i)
            m = jnp.where(ph1, m, ((i - 16) >> 1))
            role = jnp.where(ph1, role, 2 + (i & 1))
            p = jnp.where(ph1, p_of(m), (m & 7))
            p = jnp.where(ph3, 0, p)
            last = jnp.where(ph3, q == 15, role == 3)
            first = jnp.where(ph3, q == 0, role == 0)
            a_slot = jnp.where(ph3, n, (p & 1))
            x_slot = jnp.where(ph3, 4 + (q & 1), role)
            w_slot = (i & 1)

            with jax.named_scope("ev"):
                events(i)
            with jax.named_scope("iss"):
                issue(i + 1)
            w_load(g1.at[0, 0, 0], i).wait()

            @pl.when(ph3)
            def _():
                hid_load(0, q).wait()

            @pl.when((i >= 4) & (i < 32))
            def _():
                @pl.when(ph1 & first)
                def _():
                    pltpu.make_async_copy(acc.at[a_slot], part.at[0], pst.at[a_slot]).wait()

                @pl.when((i >= 20) & (role == 2))
                def _():
                    pltpu.make_async_copy(part.at[0], acc.at[a_slot], pld.at[a_slot]).wait()

            @pl.when(jnp.logical_not(last))
            def _():
                with jax.named_scope("mm"):
                    for col in range(cols):
                        total = taps(x_slot, w_slot, col)
                        acc[a_slot, col] = total + jnp.where(first, 0.0, acc[a_slot, col])

            @pl.when((i < 12) & (role == 1))
            def _():
                pltpu.make_async_copy(acc.at[a_slot], part.at[p], pst.at[a_slot]).start()

            @pl.when(last & (i < N_STEPS - 1))
            def _():
                @pl.when((i == 17) & ((blk == 0) | (blk == 3)))
                def _():
                    zero_rows(0).wait()

                keep = jnp.where(ph3, 1.0, 0.0)
                floor = jnp.where(ph3, -jnp.inf, 0.0)
                j, par = jp(p)
                shift = b1[tile_of(x, j, par)] * (1.0 - keep)
                with jax.named_scope("mmo"):
                    for col in range(cols):
                        total = taps(x_slot, w_slot, col) + acc[a_slot, col] + shift
                        for h in range(2):
                            role = 2 + ((c + h) & 1)
                            res = xa[role, 1:rows + 1, col].reshape(m_rows, cb).astype(jnp.float32)
                            val = jnp.maximum(total[:, h * cb:(h + 1) * cb] + res * keep, floor)
                            stage[h, :, col] = val.astype(jnp.bfloat16).reshape(rows, ni, cb)

                @pl.when(i < 32)
                def _():
                    for h in range(2):
                        hid_store(4 * j + 2 * par + h, h).start()

                    @pl.when(p < 6)
                    def _():
                        pltpu.make_async_copy(part.at[p + 2], acc.at[a_slot], pld.at[a_slot]).start()

                @pl.when(i == 47)
                def _():
                    for h in range(2):
                        y_far(h).start()

            @pl.when(i == N_STEPS - 1)
            def _():
                for h in range(2):
                    y_far(h).wait_send()

                def half_step(own, carry):
                    h = jnp.where(own == 1, c, 1 - c)
                    lanes = pl.ds(pl.multiple_of(h * cb, cb), cb)
                    with jax.named_scope("half"):
                        for col in range(cols):
                            total = taps(x_slot, w_slot, col, lanes) + acc[a_slot, col, :, lanes]
                            res = xa[1 - own, 1:rows + 1, col].reshape(m_rows, cb).astype(jnp.float32)
                            stage[h, :, col] = (total + res).astype(jnp.bfloat16).reshape(rows, ni, cb)

                    @pl.when(own == 0)
                    def _():
                        y_near().start()

                    return carry

                lax.fori_loop(0, 2, half_step, 0)
                y_own().start()

            return carry

        lax.fori_loop(0, N_STEPS, step, 0)

        def drain(e, carry):
            hi, lo = pair(e)
            w1_part(hi, lo).wait_send()
            w1_x(hi, lo).wait_send()
            w1_y(hi, lo).wait_send()
            for hf in range(2):
                w1_fwd(hi, lo, hf).wait_send()
            n, par = (e >> 2), ((e >> 1) & 1)
            w2_part(n, par, lo).wait_send()
            w2_fwd(n, par, lo).wait_send()
            return carry

        lax.fori_loop(0, 8, drain, 0)

        def drain_rows(a, carry):
            @pl.when(blk > 0)
            def _():
                hid_up(a).wait_send()

            @pl.when(blk < 3)
            def _():
                hid_dn(a).wait_send()

            return carry

        lax.fori_loop(0, 16, drain_rows, 0)

        def drain_two(e, carry):
            w2_x(*pair(e)).wait_send()
            w2_y(*pair(e)).wait_send()
            return carry

        lax.fori_loop(0, 4, drain_two, 0)
        for e in range(2):
            remote(stage.at[0], yt.at[0, pl.ds(0, rows)], ys.at[0], yr.at[e], sp, k).wait_recv()
        y_near().wait()
        y_own().wait()

    dma = pltpu.SemaphoreType.DMA
    bf16, f32 = jnp.bfloat16, jnp.float32
    any_space = pl.BlockSpec(memory_space=pl.ANY)
    outs = pl.pallas_call(
        kernel,
        out_shape=[
            jax.ShapeDtypeStruct((2, h_loc, cols, ni, cb), bf16),
            jax.ShapeDtypeStruct((3, 4, 2, 3, 3, cb, tile), bf16),
            jax.ShapeDtypeStruct((3, 2, 2, 2, 3, 3, cb, tile), bf16),
            jax.ShapeDtypeStruct((8, cols, m_rows, tile), f32),
            jax.ShapeDtypeStruct((16, rows + 2, cols, ni, cb), bf16),
        ],
        in_specs=[any_space, any_space, any_space, pl.BlockSpec(memory_space=pltpu.VMEM)],
        out_specs=[any_space] * 5,
        scratch_shapes=[
            pltpu.VMEM((7, rows + 2, cols, ni, cb), bf16),
            pltpu.VMEM((2, cols, m_rows, tile), f32),
            pltpu.VMEM((2, 3, 3, cb, tile), bf16),
            pltpu.VMEM((2, rows, cols, ni, cb), bf16),
            pltpu.VMEM((2, ni, cols, h_loc, cb), bf16),
            pltpu.VMEM((ni * ni, ni * ni), bf16),
            *map(dma, SEMS),
        ],
        compiler_params=pltpu.CompilerParams(collective_id=0, has_side_effects=True, vmem_limit_bytes=63 * MIB),
        name="fused_block",
    )(xw, w_one, w_two, bias)
    return outs[0]


def images_major(yt):
    groups, h_loc, cols, ni, cb = yt.shape
    parts = h_loc // ni
    width = cols // 2
    chunks = groups * parts * 2
    assert ni == 16

    def kernel(y, out, y_in, y_out, swap, in_sem, out_sem):
        def place(e):
            block, side = pair(e)
            group, part = lax.div(block, parts), lax.rem(block, parts)
            n0, h0 = pl.multiple_of(ni * group, ni), pl.multiple_of(ni * part, ni)
            return group, n0, h0, width * side

        def load(e):
            group, _, h0, col = place(e)
            cut = (group, pl.ds(h0, ni), pl.ds(col, width))
            return pltpu.make_async_copy(y.at[cut], y_in.at[cut], in_sem.at[e])

        def store(e):
            _, n0, h0, col = place(e)
            cut = (pl.ds(n0, ni), pl.ds(col, width), pl.ds(h0, ni))
            return pltpu.make_async_copy(y_out.at[cut], out.at[cut], out_sem.at[e])

        for e in range(chunks):
            load(jnp.int32(e)).start()
        swap[...] = swap_matrix(ni)

        def chunk(e, carry):
            load(e).wait()
            group, n0, h0, base = place(e)
            for col in range(width):
                rows_in = y_in[group, pl.ds(h0, ni), base + col].reshape(ni * ni, cb)
                res = jnp.dot(swap[...], rows_in, preferred_element_type=jnp.float32)
                y_out[pl.ds(n0, ni), base + col, pl.ds(h0, ni)] = res.astype(jnp.bfloat16).reshape(ni, ni, cb)
            store(e).start()
            return carry

        lax.fori_loop(0, chunks, chunk, 0)
        for e in range(chunks):
            store(jnp.int32(e)).wait()

    dma = pltpu.SemaphoreType.DMA
    out_shape = (groups * ni, cols, h_loc, cb)
    return pl.pallas_call(
        kernel,
        out_shape=jax.ShapeDtypeStruct(out_shape, jnp.bfloat16),
        in_specs=[pl.BlockSpec(memory_space=pl.ANY)],
        out_specs=pl.BlockSpec(memory_space=pl.ANY),
        scratch_shapes=[pltpu.VMEM(yt.shape, jnp.bfloat16), pltpu.VMEM(out_shape, jnp.bfloat16), pltpu.VMEM((ni * ni, ni * ni), jnp.bfloat16),
                        dma((chunks,)), dma((chunks,))],
        compiler_params=pltpu.CompilerParams(vmem_limit_bytes=63 * MIB),
        name="images_major",
    )(yt)


def solution(mesh):
    act_spec = P("dp", "sp", None, "cp")
    kernel_spec = P(None, None, "cp", None)

    def local_block(x_tile, w_one_part, w_two_part, bias_one):
        xw = x_tile.transpose(0, 2, 1, 3)
        yt = fused_block(xw, w_one_part, w_two_part, bias_one.reshape(8, 1, 2 * x_tile.shape[3]))
        return images_major(yt).transpose(0, 2, 1, 3)

    return jax.shard_map(local_block, mesh=mesh, in_specs=(act_spec, kernel_spec, kernel_spec, P()), out_specs=act_spec, check_vma=False)
```

```python
import functools

import jax
import jax.numpy as jnp
from jax import lax
from jax.experimental import pallas as pl
from jax.experimental.pallas import tpu as pltpu
from jax.sharding import PartitionSpec as P

MESH = pl.DeviceIdType.MESH
N_STEPS = 64
MIB = 1024 * 1024
ONE, TWO, THREE, FOUR, ALL = (1,), (2,), (3,), (4,), (2, 16)
GRID, CUBE, HALVES = (2, 2), (2, 2, 2), (4, 2)
QUARTERS, ROWS = (4, 4), (4, 2, 4)
SEMS = (
    TWO, TWO, TWO, TWO, TWO, ONE, (2, 3), THREE, THREE, TWO, FOUR,
    HALVES, HALVES, QUARTERS, QUARTERS, QUARTERS, QUARTERS, ROWS, ROWS,
    CUBE, CUBE, GRID, GRID, GRID, GRID, CUBE, CUBE,
    ALL, ALL, TWO, TWO, ONE, ONE, ONE,
)


def pair(e):
    return e >> 1, e & 1


def odd(i):
    return (i & 1) == 1


def swap_matrix(n):
    to = lax.broadcasted_iota(jnp.int32, (n * n, n * n), 0)
    frm = lax.broadcasted_iota(jnp.int32, (n * n, n * n), 1)
    hit = (lax.div(to, n) == lax.rem(frm, n)) & (lax.rem(to, n) == lax.div(frm, n))
    return jnp.where(hit, 1.0, 0.0).astype(jnp.bfloat16)


def fused_block(xw, w_one, w_two, bias):
    images, cols, h_loc, cb = xw.shape
    ni = images // 2
    rows = h_loc // 2
    m_rows = rows * ni
    tile = 2 * cb
    assert ni == 16 and h_loc == 48

    def remote(src, dst, send_sem, recv_sem, sp, cp):
        return pltpu.make_async_remote_copy(src_ref=src, dst_ref=dst, send_sem=send_sem, recv_sem=recv_sem,
                                            device_id={"sp": sp, "cp": cp}, device_id_type=MESH)

    def kernel(xw, w1, w2, b1, yt, g1, g2, part, hid,
               xa, acc, wv, stage, raw, swap,
               wsem, asem, pst, pld, stl, zsem, rsem, xs, xr, hs, hr,
               p1s, p1r, x1s, x1r, y1s, y1r, f1s, f1r,
               p2s, p2r, x2s, x2r, y2s, y2r, f2s, f2r,
               as_, ar, ys, yr, zs, zr, yl):
        sp = lax.axis_index("sp")
        k = lax.axis_index("cp")
        x = (k >> 1)
        c = (k & 1)
        blk = 2 * sp + c
        osp = 1 - sp
        k1 = 2 * x + (1 - c)
        k2 = 2 * (1 - x) + c
        k3 = 2 * (1 - x) + (1 - c)

        def tile_of(xx, j, par):
            return 4 * ((xx + (j >> 1)) & 1) + 2 * (j & 1) + par

        barrier = pltpu.get_barrier_semaphore()
        for d_sp in range(2):
            for d_cp in range(4):
                if d_sp or d_cp:
                    pl.semaphore_signal(barrier, inc=1, device_id={"sp": ((sp + d_sp) & 1), "cp": ((k + d_cp) & 3)},
                                        device_id_type=MESH)

        def raw_load(far, part):
            cut = pl.ds(pl.multiple_of(ni * part, ni), ni)
            group = pl.ds(ni * (1 - x if far else x), ni)
            return pltpu.make_async_copy(xw.at[group, :, cut], raw.at[far, :, :, cut], rsem.at[far, part])

        def block(far, col, part):
            rows_in = raw[far, :, col, pl.ds(pl.multiple_of(ni * part, ni), ni), :].reshape(ni * ni, cb)
            out = jnp.dot(swap[...], rows_in, preferred_element_type=jnp.float32)
            return out.astype(jnp.bfloat16).reshape(ni, ni, cb)

        def slot_of(far, cc):
            return jnp.where(cc == c, 5 if far else 0, 6 if far else 4)

        def swap_end(far, cc):
            raw_load(far, 2 * cc).wait()
            for col in range(cols):
                xa[slot_of(far, cc), pl.ds(1 + 8 * cc, ni), col] = block(far, col, 2 * cc)

        def swap_mid(far):
            raw_load(far, 1).wait()
            for col in range(cols):
                mid = block(far, col, 1)
                xa[slot_of(far, 0), 17:26, col] = mid[0:9]
                xa[slot_of(far, 1), 0:9, col] = mid[7:16]

        def x_copy(role):
            cc = c if role == 2 else 1 - c
            cut = pl.ds(1 - cc, rows + 1)
            return remote(xa.at[3 + role, cut], xa.at[role, cut], xs.at[role - 1], xr.at[role - 1], sp,
                          {1: k1, 2: k2, 3: k3}[role])

        def halo_copy(far):
            xx = 1 - x if far else x
            role = 2 * ((x + xx) & 1) + ((c + sp) & 1)
            src = xa.at[slot_of(far, osp), jnp.where(sp == 0, rows, 1)]
            return remote(src, xa.at[role, (rows + 1) * sp], hs.at[far], hr.at[role], osp, 2 * xx + sp)

        piece = cb // 4

        def w1_own(j, par, xx):
            return w1.at[:, :, :, pl.ds(pl.multiple_of(tile_of(xx, j, par) * tile, tile), tile)]

        def w1_part(j, par):
            return remote(w1_own(j, par, x), g1.at[0, j, par], p1s.at[j, par], p1r.at[j, par], sp, k1)

        def w1_x(j, hf):
            cut = pl.ds(pl.multiple_of(hf * piece, piece), piece)
            src = w1.at[:, :, cut, pl.ds(pl.multiple_of(tile_of(1 - x, j, sp) * tile, tile), tile)]
            return remote(src, g1.at[1, j, sp, :, :, cut], x1s.at[j, hf], x1r.at[j, hf], sp, k2)

        def w1_y(j, hf):
            cut = pl.ds(pl.multiple_of(hf * piece, piece), piece)
            ref = g1.at[1, j, sp, :, :, cut]
            return remote(ref, ref, y1s.at[j, hf], y1r.at[j, hf], osp, k)

        def w1_fwd(j, par, hf):
            cut = pl.ds(pl.multiple_of(hf * piece, piece), piece)
            return remote(g1.at[1, j, par, :, :, cut], g1.at[2, j, par, :, :, cut], f1s.at[j, par, hf], f1r.at[j, par, hf], sp, k1)

        def w2_cut(n, par, h, xx):
            row = pl.multiple_of(par * tile + h * cb, cb)
            col = pl.multiple_of(tile * ((1 + xx + n) & 1), tile)
            return w2.at[:, :, pl.ds(row, cb), pl.ds(col, tile)]

        def w2_part(n, par, h):
            return remote(w2_cut(n, par, h, x), g2.at[0, n, par, h], p2s.at[n, par, h], p2r.at[n, par, h], sp, k1)

        def w2_x(n, h):
            return remote(w2_cut(n, sp, h, 1 - x), g2.at[1, n, sp, h], x2s.at[n, h], x2r.at[n, h], sp, k2)

        def w2_y(n, h):
            ref = g2.at[1, n, sp, h]
            return remote(ref, ref, y2s.at[n, h], y2r.at[n, h], osp, k)

        def w2_fwd(n, par, h):
            return remote(g2.at[1, n, par, h], g2.at[2, n, par, h], f2s.at[n, par, h], f2r.at[n, par, h], sp, k1)

        up_blk = lax.max(blk - 1, 0)
        dn_blk = lax.min(blk + 1, 3)

        def hid_up(a):
            return remote(hid.at[a, 1], hid.at[a, rows + 1], as_.at[0, a], ar.at[1, a], (up_blk >> 1), 2 * x + (up_blk & 1))

        def hid_dn(a):
            return remote(hid.at[a, rows], hid.at[a, 0], as_.at[1, a], ar.at[0, a], (dn_blk >> 1), 2 * x + (dn_blk & 1))

        def hid_store(a, h):
            return pltpu.make_async_copy(stage.at[h], hid.at[a, pl.ds(1, rows)], stl.at[h])

        y_rows = pl.ds(rows * c, rows)

        def y_far(h):
            return remote(stage.at[h], yt.at[x, y_rows], ys.at[h], yr.at[((h + c) & 1)], sp, 2 * (1 - x) + h)

        def y_near():
            return remote(stage.at[1 - c], yt.at[x, y_rows], zs.at[0], zr.at[0], sp, k1)

        def y_own():
            return pltpu.make_async_copy(stage.at[c], yt.at[x, y_rows], yl.at[0])

        def zero_rows(row):
            return pltpu.make_async_copy(stage.at[0, pl.ds(0, 16)], hid.at[:, row], zsem.at[0])

        def p_of(m):
            return (m + 2) & 7

        def jp(p):
            return p >> 1, (sp + p) & 1

        def near_step(i):
            return 2 * (i >> 2) + (i & 1), (i & 2) >> 1

        def halo_wait(role):
            @pl.when(c != sp)
            def _():
                remote(xa.at[0, 0], xa.at[role, 0], hs.at[0], hr.at[role], osp, k).wait_recv()

        for part_no in (2 * osp, 2 * sp, 1):
            raw_load(0, part_no).start()
        for part_no in range(3):
            raw_load(1, part_no).start()
        swap[...] = swap_matrix(ni)
        edge = c == sp

        @pl.when(edge)
        def _():
            xa[0:4, (rows + 1) * sp] = jnp.zeros((4, cols, ni, cb), jnp.bfloat16)

        def w_load(src, t):
            return pltpu.make_async_copy(src, wv.at[(t & 1)], wsem.at[(t & 1)])

        def hid_load(a, q):
            slot = (q & 1)
            return pltpu.make_async_copy(hid.at[a], xa.at[4 + slot], asem.at[slot])

        def issue(t):
            @pl.when(t < 16)
            def _():
                m, role = near_step(t)
                j, par = jp(p_of(m))

                @pl.when(role == 0)
                def _():
                    w_load(w1_own(j, par, x), t).start()

                @pl.when(role == 1)
                def _():
                    w1_part(j, par).wait_recv()
                    w_load(g1.at[0, j, par], t).start()

            @pl.when((t >= 16) & (t < 32))
            def _():
                j, par = jp(((t - 16) >> 1))

                @pl.when((t & 1) == 1)
                def _():
                    for hf in range(4):
                        w1_fwd(j, par, hf).wait_recv()

                w_load(g1.at[1 + (t & 1), j, par], t).start()

            @pl.when((t >= 32) & (t < N_STEPS))
            def _():
                n = ((t - 32) >> 4)
                q = ((t - 32) & 15)
                h = (q & 1)
                p = (q >> 1)
                j, par = jp(p)
                a = 4 * j + 2 * par + h
                same = (j & 1) == c

                @pl.when(n == 0)
                def _():
                    @pl.when(blk > 0)
                    def _():
                        hid_dn(a).wait_recv()

                    @pl.when(blk < 3)
                    def _():
                        hid_up(a).wait_recv()

                hid_load(a, q).start()

                @pl.when(p < 4)
                def _():
                    @pl.when(same)
                    def _():
                        w_load(w2_cut(n, par, h, x), t).start()

                    @pl.when(jnp.logical_not(same))
                    def _():
                        w2_part(n, par, h).wait_recv()
                        w_load(g2.at[0, n, par, h], t).start()

                @pl.when(p >= 4)
                def _():
                    @pl.when(jnp.logical_not(same))
                    def _():
                        w2_fwd(n, par, h).wait_recv()

                    w_load(g2.at[jnp.where(same, 1, 2), n, par, h], t).start()

        issue(jnp.int32(0))
        with jax.named_scope("swap"):
            swap_end(0, osp)
        with jax.named_scope("bar"):
            pl.semaphore_wait(barrier, 7)

        @pl.when(edge)
        def _():
            halo_copy(0).start()

        for e in range(6):
            w1_x(*divmod(e, 4)).start()
        with jax.named_scope("swap2"):
            swap_end(0, sp)
            swap_mid(0)
        x_copy(1).start()
        for m in range(2):
            w1_part(*jp(jnp.int32(m + 2))).start()
        with jax.named_scope("swap3"):
            for cc in range(2):
                swap_end(1, cc)
            swap_mid(1)
        with jax.named_scope("halo"):
            halo_wait(0)

        def pass_w1_x(e):
            j, hf = e >> 2, e & 3
            w1_x(j, hf).wait_recv()
            w1_y(j, hf).start()
            w1_fwd(j, sp, hf).start()

        def pass_w1_y(e):
            j, hf = e >> 2, e & 3
            w1_y(j, hf).wait_recv()
            w1_fwd(j, osp, hf).start()

        def pass_w2_x(e):
            n, h = pair(e)
            w2_x(n, h).wait_recv()
            w2_y(n, h).start()
            w2_fwd(n, sp, h).start()

        def pass_w2_y(e):
            n, h = pair(e)
            w2_y(n, h).wait_recv()
            w2_fwd(n, osp, h).start()

        def send_w1_x(e):
            w1_x(e >> 2, e & 3).start()

        def send_w2_x(e):
            w2_x(*pair(e)).start()

        def events(i):
            is_odd = odd(i)
            even = jnp.logical_not(is_odd)

            @pl.when(i < 16)
            def _():
                @pl.when(even)
                def _():
                    @pl.when(i < 12)
                    def _():
                        w1_part(*jp(p_of((i >> 1) + 2))).start()

                    @pl.when(i == 2)
                    def _():
                        x_copy(1).wait_recv()
                        halo_wait(1)

                    @pl.when(i == 10)
                    def _():
                        lax.fori_loop(0, 4, lambda e, carry: (pass_w1_y(e), carry)[1], 0)

                    @pl.when(i == 12)
                    def _():
                        lax.fori_loop(4, 6, lambda e, carry: (pass_w1_y(e), carry)[1], 0)

                @pl.when(is_odd)
                def _():
                    @pl.when(i == 1)
                    def _():
                        @pl.when(c != sp)
                        def _():
                            halo_copy(0).start()

                        halo_copy(1).start()

                        @pl.when(edge)
                        def _():
                            stage[0, 0:16] = jnp.zeros((16, cols, ni, cb), jnp.bfloat16)
                            zero_rows((rows + 1) * sp).start()

                    @pl.when(i == 3)
                    def _():
                        x_copy(2).start()

                    @pl.when(i == 5)
                    def _():
                        lax.fori_loop(0, 4, lambda e, carry: (pass_w1_x(e), carry)[1], 0)

                    @pl.when(i == 7)
                    def _():
                        lax.fori_loop(4, 6, lambda e, carry: (pass_w1_x(e), carry)[1], 0)

                    @pl.when(i == 9)
                    def _():
                        x_copy(3).start()

            @pl.when((i >= 13) & (i < 23))
            def _():
                send_w1_x(i - 7)

            @pl.when((i >= 16) & (i < 34))
            def _():
                @pl.when((i >= 18) & (i < 28))
                def _():
                    pass_w1_x(i - 12)

                @pl.when((i >= 20) & (i < 30))
                def _():
                    pass_w1_y(i - 14)

                @pl.when(i < 24)
                def _():
                    e = i - 16
                    w2_part((e >> 2), ((e >> 1) & 1), (e & 1)).start()

                @pl.when(even)
                def _():
                    @pl.when(i == 16)
                    def _():
                        x_copy(2).wait_recv()
                        halo_wait(2)

                    @pl.when(i == 30)
                    def _():
                        x_copy(1).wait_send()
                        x_copy(2).wait_send()
                        x_copy(3).wait_send()
                        for far in range(2):
                            halo_copy(far).wait_send()

                    @pl.when((i >= 24) & ((i & 3) == 0))
                    def _():
                        send_w2_x(((i - 24) >> 2))

                @pl.when(is_odd)
                def _():
                    @pl.when(i == 17)
                    def _():
                        x_copy(3).wait_recv()
                        halo_wait(3)

                    @pl.when(i >= 19)
                    def _():
                        for h in range(2):
                            hid_store(0, h).wait()

                    @pl.when(i >= 27)
                    def _():
                        for d in range(2):
                            j, par = jp(i - 27 + d)
                            for h in range(2):
                                a = 4 * j + 2 * par + h

                                @pl.when(blk > 0)
                                def _():
                                    hid_up(a).start()

                                @pl.when(blk < 3)
                                def _():
                                    hid_dn(a).start()

                    @pl.when(i == 31)
                    def _():
                        pass_w2_x(jnp.int32(0))

            @pl.when((i >= 34) & (i < 50))
            def _():
                @pl.when(i == 36)
                def _():
                    send_w2_x(jnp.int32(3))

                @pl.when((i < 44) & ((i & 3) == 3))
                def _():
                    pass_w2_x(((i - 31) >> 2))

                @pl.when((i >= 37) & ((i & 3) == 1))
                def _():
                    pass_w2_y(((i - 37) >> 2))

        def taps(xs_slot, ws_slot, col, lanes=slice(None)):
            total = None
            for dx in (-1, 0, 1):
                if not 0 <= col + dx < cols:
                    continue
                for dy in range(3):
                    lhs = xa[xs_slot, dy:dy + rows, col + dx].reshape(m_rows, cb)
                    prod = jnp.dot(lhs, wv[ws_slot, dy, dx + 1, :, lanes], preferred_element_type=jnp.float32)
                    total = prod if total is None else total + prod
            return total

        def step(i, carry):
            ph1 = i < 16
            ph3 = i >= 32
            n = jnp.where(ph3, ((i - 32) >> 4), 0)
            q = jnp.where(ph3, ((i - 32) & 15), 0)
            m, role = near_step(i)
            m = jnp.where(ph1, m, ((i - 16) >> 1))
            role = jnp.where(ph1, role, 2 + (i & 1))
            p = jnp.where(ph1, p_of(m), (m & 7))
            p = jnp.where(ph3, 0, p)
            last = jnp.where(ph3, q == 15, role == 3)
            first = jnp.where(ph3, q == 0, role == 0)
            a_slot = jnp.where(ph3, n, (p & 1))
            x_slot = jnp.where(ph3, 4 + (q & 1), role)
            w_slot = (i & 1)

            with jax.named_scope("ev"):
                events(i)
            with jax.named_scope("iss"):
                issue(i + 1)
            w_load(g1.at[0, 0, 0], i).wait()

            @pl.when(ph3)
            def _():
                hid_load(0, q).wait()

            @pl.when((i >= 4) & (i < 32))
            def _():
                @pl.when(ph1 & first)
                def _():
                    pltpu.make_async_copy(acc.at[a_slot], part.at[0], pst.at[a_slot]).wait()

                @pl.when((i >= 20) & (role == 2))
                def _():
                    pltpu.make_async_copy(part.at[0], acc.at[a_slot], pld.at[a_slot]).wait()

            @pl.when(jnp.logical_not(last))
            def _():
                with jax.named_scope("mm"):
                    for col in range(cols):
                        total = taps(x_slot, w_slot, col)
                        acc[a_slot, col] = total + jnp.where(first, 0.0, acc[a_slot, col])

            @pl.when((i < 12) & (role == 1))
            def _():
                pltpu.make_async_copy(acc.at[a_slot], part.at[p], pst.at[a_slot]).start()

            @pl.when(last & (i < N_STEPS - 1))
            def _():
                @pl.when((i == 17) & edge)
                def _():
                    zero_rows(0).wait()

                keep = jnp.where(ph3, 1.0, 0.0)
                floor = jnp.where(ph3, -jnp.inf, 0.0)
                j, par = jp(p)
                shift = b1[tile_of(x, j, par)] * (1.0 - keep)
                with jax.named_scope("mmo"):
                    for col in range(cols):
                        total = taps(x_slot, w_slot, col) + acc[a_slot, col] + shift
                        for h in range(2):
                            role = 2 + ((c + h) & 1)
                            res = xa[role, 1:rows + 1, col].reshape(m_rows, cb).astype(jnp.float32)
                            val = jnp.maximum(total[:, h * cb:(h + 1) * cb] + res * keep, floor)
                            stage[h, :, col] = val.astype(jnp.bfloat16).reshape(rows, ni, cb)

                @pl.when(i < 32)
                def _():
                    for h in range(2):
                        hid_store(4 * j + 2 * par + h, h).start()

                    @pl.when(p < 6)
                    def _():
                        pltpu.make_async_copy(part.at[p + 2], acc.at[a_slot], pld.at[a_slot]).start()

                @pl.when(i == 47)
                def _():
                    for h in range(2):
                        y_far(h).start()

            @pl.when(i == N_STEPS - 1)
            def _():
                for h in range(2):
                    y_far(h).wait_send()

                def half_step(own, carry):
                    h = jnp.where(own == 1, c, 1 - c)
                    lanes = pl.ds(pl.multiple_of(h * cb, cb), cb)
                    with jax.named_scope("half"):
                        for col in range(cols):
                            total = taps(x_slot, w_slot, col, lanes) + acc[a_slot, col, :, lanes]
                            res = xa[1 - own, 1:rows + 1, col].reshape(m_rows, cb).astype(jnp.float32)
                            stage[h, :, col] = (total + res).astype(jnp.bfloat16).reshape(rows, ni, cb)

                    @pl.when(own == 0)
                    def _():
                        y_near().start()

                    return carry

                lax.fori_loop(0, 2, half_step, 0)
                y_own().start()

            return carry

        lax.fori_loop(0, N_STEPS, step, 0)

        def drain(e, carry):
            hi, lo = pair(e)
            w1_part(hi, lo).wait_send()
            for hf in (lo, lo + 2):
                w1_x(hi, hf).wait_send()
                w1_y(hi, hf).wait_send()
            for hf in range(4):
                w1_fwd(hi, lo, hf).wait_send()
            n, par = e >> 2, (e >> 1) & 1
            w2_part(n, par, lo).wait_send()
            w2_fwd(n, par, lo).wait_send()
            return carry

        lax.fori_loop(0, 8, drain, 0)

        def drain_rows(a, carry):
            @pl.when(blk > 0)
            def _():
                hid_up(a).wait_send()

            @pl.when(blk < 3)
            def _():
                hid_dn(a).wait_send()

            return carry

        lax.fori_loop(0, 16, drain_rows, 0)

        def drain_two(e, carry):
            w2_x(*pair(e)).wait_send()
            w2_y(*pair(e)).wait_send()
            return carry

        lax.fori_loop(0, 4, drain_two, 0)
        for e in range(2):
            remote(stage.at[0], yt.at[0, pl.ds(0, rows)], ys.at[0], yr.at[e], sp, k).wait_recv()
        y_near().wait()
        y_own().wait()

    dma = pltpu.SemaphoreType.DMA
    bf16, f32 = jnp.bfloat16, jnp.float32
    any_space = pl.BlockSpec(memory_space=pl.ANY)
    outs = pl.pallas_call(
        kernel,
        out_shape=[
            jax.ShapeDtypeStruct((2, h_loc, cols, ni, cb), bf16),
            jax.ShapeDtypeStruct((3, 4, 2, 3, 3, cb, tile), bf16),
            jax.ShapeDtypeStruct((3, 2, 2, 2, 3, 3, cb, tile), bf16),
            jax.ShapeDtypeStruct((8, cols, m_rows, tile), f32),
            jax.ShapeDtypeStruct((16, rows + 2, cols, ni, cb), bf16),
        ],
        in_specs=[any_space, any_space, any_space, pl.BlockSpec(memory_space=pltpu.VMEM)],
        out_specs=[any_space] * 5,
        scratch_shapes=[
            pltpu.VMEM((7, rows + 2, cols, ni, cb), bf16),
            pltpu.VMEM((2, cols, m_rows, tile), f32),
            pltpu.VMEM((2, 3, 3, cb, tile), bf16),
            pltpu.VMEM((2, rows, cols, ni, cb), bf16),
            pltpu.VMEM((2, ni, cols, h_loc, cb), bf16),
            pltpu.VMEM((ni * ni, ni * ni), bf16),
            *map(dma, SEMS),
        ],
        compiler_params=pltpu.CompilerParams(collective_id=0, has_side_effects=True, vmem_limit_bytes=63 * MIB),
        name="fused_block",
    )(xw, w_one, w_two, bias)
    return outs[0]


def images_major(yt):
    groups, h_loc, cols, ni, cb = yt.shape
    parts = h_loc // ni
    width = cols // 2
    chunks = groups * parts * 2
    assert ni == 16

    def kernel(y, out, y_in, y_out, swap, in_sem, out_sem):
        def place(e):
            block, side = pair(e)
            group, part = lax.div(block, parts), lax.rem(block, parts)
            n0, h0 = pl.multiple_of(ni * group, ni), pl.multiple_of(ni * part, ni)
            return group, n0, h0, width * side

        def load(e):
            group, _, h0, col = place(e)
            cut = (group, pl.ds(h0, ni), pl.ds(col, width))
            return pltpu.make_async_copy(y.at[cut], y_in.at[cut], in_sem.at[e])

        def store(e):
            _, n0, h0, col = place(e)
            cut = (pl.ds(n0, ni), pl.ds(col, width), pl.ds(h0, ni))
            return pltpu.make_async_copy(y_out.at[cut], out.at[cut], out_sem.at[e])

        for e in range(chunks):
            load(jnp.int32(e)).start()
        swap[...] = swap_matrix(ni)

        def chunk(e, carry):
            load(e).wait()
            group, n0, h0, base = place(e)
            for col in range(width):
                rows_in = y_in[group, pl.ds(h0, ni), base + col].reshape(ni * ni, cb)
                res = jnp.dot(swap[...], rows_in, preferred_element_type=jnp.float32)
                y_out[pl.ds(n0, ni), base + col, pl.ds(h0, ni)] = res.astype(jnp.bfloat16).reshape(ni, ni, cb)
            store(e).start()
            return carry

        lax.fori_loop(0, chunks, chunk, 0)
        for e in range(chunks):
            store(jnp.int32(e)).wait()

    dma = pltpu.SemaphoreType.DMA
    out_shape = (groups * ni, cols, h_loc, cb)
    return pl.pallas_call(
        kernel,
        out_shape=jax.ShapeDtypeStruct(out_shape, jnp.bfloat16),
        in_specs=[pl.BlockSpec(memory_space=pl.ANY)],
        out_specs=pl.BlockSpec(memory_space=pl.ANY),
        scratch_shapes=[pltpu.VMEM(yt.shape, jnp.bfloat16), pltpu.VMEM(out_shape, jnp.bfloat16), pltpu.VMEM((ni * ni, ni * ni), jnp.bfloat16),
                        dma((chunks,)), dma((chunks,))],
        compiler_params=pltpu.CompilerParams(vmem_limit_bytes=63 * MIB),
        name="images_major",
    )(yt)


def solution(mesh):
    act_spec = P("dp", "sp", None, "cp")
    kernel_spec = P(None, None, "cp", None)

    def local_block(x_tile, w_one_part, w_two_part, bias_one):
        xw = x_tile.transpose(0, 2, 1, 3)
        yt = fused_block(xw, w_one_part, w_two_part, bias_one.reshape(8, 1, 2 * x_tile.shape[3]))
        return images_major(yt).transpose(0, 2, 1, 3)

    return jax.shard_map(local_block, mesh=mesh, in_specs=(act_spec, kernel_spec, kernel_spec, P()), out_specs=act_spec, check_vma=False)
```

```python
import functools

import jax
import jax.numpy as jnp
from jax import lax
from jax.experimental import pallas as pl
from jax.experimental.pallas import tpu as pltpu
from jax.sharding import PartitionSpec as P

MESH = pl.DeviceIdType.MESH
N_STEPS = 64
MIB = 1024 * 1024
ONE, TWO, THREE, FOUR, ALL = (1,), (2,), (3,), (4,), (2, 16)
GRID, CUBE, HALVES = (2, 2), (2, 2, 2), (4, 2)
QUARTERS, ROWS = (4, 4), (4, 2, 4)
SEMS = (
    TWO, TWO, TWO, TWO, TWO, ONE, (2, 3), THREE, THREE, TWO, FOUR,
    HALVES, HALVES, QUARTERS, QUARTERS, QUARTERS, QUARTERS, ROWS, ROWS,
    CUBE, CUBE, GRID, GRID, GRID, GRID, CUBE, CUBE,
    ALL, ALL, TWO, TWO, ONE, ONE, ONE,
)


def pair(e):
    return e >> 1, e & 1


def odd(i):
    return (i & 1) == 1


def swap_matrix(n):
    to = lax.broadcasted_iota(jnp.int32, (n * n, n * n), 0)
    frm = lax.broadcasted_iota(jnp.int32, (n * n, n * n), 1)
    hit = (lax.div(to, n) == lax.rem(frm, n)) & (lax.rem(to, n) == lax.div(frm, n))
    return jnp.where(hit, 1.0, 0.0).astype(jnp.bfloat16)


def fused_block(xw, w_one, w_two, bias):
    images, cols, h_loc, cb = xw.shape
    ni = images // 2
    rows = h_loc // 2
    m_rows = rows * ni
    tile = 2 * cb
    assert ni == 16 and h_loc == 48

    def remote(src, dst, send_sem, recv_sem, sp, cp):
        return pltpu.make_async_remote_copy(src_ref=src, dst_ref=dst, send_sem=send_sem, recv_sem=recv_sem,
                                            device_id={"sp": sp, "cp": cp}, device_id_type=MESH)

    def kernel(xw, w1, w2, b1, yt, g1, g2, part, hid,
               xa, acc, wv, stage, raw, swap, mark,
               wsem, asem, pst, pld, stl, zsem, rsem, xs, xr, hs, hr,
               p1s, p1r, x1s, x1r, y1s, y1r, f1s, f1r,
               p2s, p2r, x2s, x2r, y2s, y2r, f2s, f2r,
               as_, ar, ys, yr, zs, zr, yl):
        sp = lax.axis_index("sp")
        k = lax.axis_index("cp")
        x = (k >> 1)
        c = (k & 1)
        blk = 2 * sp + c
        osp = 1 - sp
        k1 = 2 * x + (1 - c)
        k2 = 2 * (1 - x) + c
        k3 = 2 * (1 - x) + (1 - c)

        def rarely(cond):
            def wrap(body):
                @pl.when(cond)
                def _():
                    mark[...] = jnp.zeros(mark.shape, jnp.float32)
                    body()

            return wrap

        def tile_of(xx, j, par):
            return 4 * ((xx + (j >> 1)) & 1) + 2 * (j & 1) + par

        barrier = pltpu.get_barrier_semaphore()
        for d_sp in range(2):
            for d_cp in range(4):
                if d_sp or d_cp:
                    pl.semaphore_signal(barrier, inc=1, device_id={"sp": ((sp + d_sp) & 1), "cp": ((k + d_cp) & 3)},
                                        device_id_type=MESH)

        def raw_load(far, part):
            cut = pl.ds(pl.multiple_of(ni * part, ni), ni)
            group = pl.ds(ni * (1 - x if far else x), ni)
            return pltpu.make_async_copy(xw.at[group, :, cut], raw.at[far, :, :, cut], rsem.at[far, part])

        def block(far, col, part):
            rows_in = raw[far, :, col, pl.ds(pl.multiple_of(ni * part, ni), ni), :].reshape(ni * ni, cb)
            out = jnp.dot(swap[...], rows_in, preferred_element_type=jnp.float32)
            return out.astype(jnp.bfloat16).reshape(ni, ni, cb)

        def slot_of(far, cc):
            return jnp.where(cc == c, 5 if far else 0, 6 if far else 4)

        def swap_end(far, cc):
            raw_load(far, 2 * cc).wait()
            for col in range(cols):
                xa[slot_of(far, cc), pl.ds(1 + 8 * cc, ni), col] = block(far, col, 2 * cc)

        def swap_mid(far):
            raw_load(far, 1).wait()
            for col in range(cols):
                mid = block(far, col, 1)
                xa[slot_of(far, 0), 17:26, col] = mid[0:9]
                xa[slot_of(far, 1), 0:9, col] = mid[7:16]

        def x_copy(role):
            cc = c if role == 2 else 1 - c
            cut = pl.ds(1 - cc, rows + 1)
            return remote(xa.at[3 + role, cut], xa.at[role, cut], xs.at[role - 1], xr.at[role - 1], sp,
                          {1: k1, 2: k2, 3: k3}[role])

        def halo_copy(far):
            xx = 1 - x if far else x
            role = 2 * ((x + xx) & 1) + ((c + sp) & 1)
            src = xa.at[slot_of(far, osp), jnp.where(sp == 0, rows, 1)]
            return remote(src, xa.at[role, (rows + 1) * sp], hs.at[far], hr.at[role], osp, 2 * xx + sp)

        piece = cb // 4

        def w1_own(j, par, xx):
            return w1.at[:, :, :, pl.ds(pl.multiple_of(tile_of(xx, j, par) * tile, tile), tile)]

        def w1_part(j, par):
            return remote(w1_own(j, par, x), g1.at[0, j, par], p1s.at[j, par], p1r.at[j, par], sp, k1)

        def w1_x(j, hf):
            cut = pl.ds(pl.multiple_of(hf * piece, piece), piece)
            src = w1.at[:, :, cut, pl.ds(pl.multiple_of(tile_of(1 - x, j, sp) * tile, tile), tile)]
            return remote(src, g1.at[1, j, sp, :, :, cut], x1s.at[j, hf], x1r.at[j, hf], sp, k2)

        def w1_y(j, hf):
            cut = pl.ds(pl.multiple_of(hf * piece, piece), piece)
            ref = g1.at[1, j, sp, :, :, cut]
            return remote(ref, ref, y1s.at[j, hf], y1r.at[j, hf], osp, k)

        def w1_fwd(j, par, hf):
            cut = pl.ds(pl.multiple_of(hf * piece, piece), piece)
            return remote(g1.at[1, j, par, :, :, cut], g1.at[2, j, par, :, :, cut], f1s.at[j, par, hf], f1r.at[j, par, hf], sp, k1)

        def w2_cut(n, par, h, xx):
            row = pl.multiple_of(par * tile + h * cb, cb)
            col = pl.multiple_of(tile * ((1 + xx + n) & 1), tile)
            return w2.at[:, :, pl.ds(row, cb), pl.ds(col, tile)]

        def w2_part(n, par, h):
            return remote(w2_cut(n, par, h, x), g2.at[0, n, par, h], p2s.at[n, par, h], p2r.at[n, par, h], sp, k1)

        def w2_x(n, h):
            return remote(w2_cut(n, sp, h, 1 - x), g2.at[1, n, sp, h], x2s.at[n, h], x2r.at[n, h], sp, k2)

        def w2_y(n, h):
            ref = g2.at[1, n, sp, h]
            return remote(ref, ref, y2s.at[n, h], y2r.at[n, h], osp, k)

        def w2_fwd(n, par, h):
            return remote(g2.at[1, n, par, h], g2.at[2, n, par, h], f2s.at[n, par, h], f2r.at[n, par, h], sp, k1)

        up_blk = lax.max(blk - 1, 0)
        dn_blk = lax.min(blk + 1, 3)

        def hid_up(a):
            return remote(hid.at[a, 1], hid.at[a, rows + 1], as_.at[0, a], ar.at[1, a], (up_blk >> 1), 2 * x + (up_blk & 1))

        def hid_dn(a):
            return remote(hid.at[a, rows], hid.at[a, 0], as_.at[1, a], ar.at[0, a], (dn_blk >> 1), 2 * x + (dn_blk & 1))

        def hid_store(a, h):
            return pltpu.make_async_copy(stage.at[h], hid.at[a, pl.ds(1, rows)], stl.at[h])

        y_rows = pl.ds(rows * c, rows)

        def y_far(h):
            return remote(stage.at[h], yt.at[x, y_rows], ys.at[h], yr.at[((h + c) & 1)], sp, 2 * (1 - x) + h)

        def y_near():
            return remote(stage.at[1 - c], yt.at[x, y_rows], zs.at[0], zr.at[0], sp, k1)

        def y_own():
            return pltpu.make_async_copy(stage.at[c], yt.at[x, y_rows], yl.at[0])

        def zero_rows(row):
            return pltpu.make_async_copy(stage.at[0, pl.ds(0, 16)], hid.at[:, row], zsem.at[0])

        def p_of(m):
            return (m + 2) & 7

        def jp(p):
            return p >> 1, (sp + p) & 1

        def near_step(i):
            return 2 * (i >> 2) + (i & 1), (i & 2) >> 1

        def halo_wait(role):
            @pl.when(c != sp)
            def _():
                remote(xa.at[0, 0], xa.at[role, 0], hs.at[0], hr.at[role], osp, k).wait_recv()

        for part_no in (2 * osp, 2 * sp, 1):
            raw_load(0, part_no).start()
        for part_no in range(3):
            raw_load(1, part_no).start()
        swap[...] = swap_matrix(ni)
        edge = c == sp

        @pl.when(edge)
        def _():
            xa[0:4, (rows + 1) * sp] = jnp.zeros((4, cols, ni, cb), jnp.bfloat16)

        def w_load(src, t):
            return pltpu.make_async_copy(src, wv.at[(t & 1)], wsem.at[(t & 1)])

        def hid_load(a, q):
            slot = (q & 1)
            return pltpu.make_async_copy(hid.at[a], xa.at[4 + slot], asem.at[slot])

        def issue(t):
            @rarely(t < 16)
            def _():
                m, role = near_step(t)
                j, par = jp(p_of(m))

                @rarely(role == 0)
                def _():
                    w_load(w1_own(j, par, x), t).start()

                @rarely(role == 1)
                def _():
                    w1_part(j, par).wait_recv()
                    w_load(g1.at[0, j, par], t).start()

            @rarely((t >= 16) & (t < 32))
            def _():
                j, par = jp(((t - 16) >> 1))

                @rarely((t & 1) == 1)
                def _():
                    for hf in range(4):
                        w1_fwd(j, par, hf).wait_recv()

                w_load(g1.at[1 + (t & 1), j, par], t).start()

            @rarely((t >= 32) & (t < N_STEPS))
            def _():
                n = ((t - 32) >> 4)
                q = ((t - 32) & 15)
                h = (q & 1)
                p = (q >> 1)
                j, par = jp(p)
                a = 4 * j + 2 * par + h
                same = (j & 1) == c

                @rarely(n == 0)
                def _():
                    @pl.when(blk > 0)
                    def _():
                        hid_dn(a).wait_recv()

                    @pl.when(blk < 3)
                    def _():
                        hid_up(a).wait_recv()

                hid_load(a, q).start()

                @rarely(p < 4)
                def _():
                    @rarely(same)
                    def _():
                        w_load(w2_cut(n, par, h, x), t).start()

                    @rarely(jnp.logical_not(same))
                    def _():
                        w2_part(n, par, h).wait_recv()
                        w_load(g2.at[0, n, par, h], t).start()

                @rarely(p >= 4)
                def _():
                    @pl.when(jnp.logical_not(same))
                    def _():
                        w2_fwd(n, par, h).wait_recv()

                    w_load(g2.at[jnp.where(same, 1, 2), n, par, h], t).start()

        issue(jnp.int32(0))
        with jax.named_scope("swap"):
            swap_end(0, osp)
        with jax.named_scope("bar"):
            pl.semaphore_wait(barrier, 7)

        @pl.when(edge)
        def _():
            halo_copy(0).start()

        for e in range(6):
            w1_x(*divmod(e, 4)).start()
        with jax.named_scope("swap2"):
            swap_end(0, sp)
            swap_mid(0)
        x_copy(1).start()
        for m in range(2):
            w1_part(*jp(jnp.int32(m + 2))).start()
        with jax.named_scope("swap3"):
            for cc in range(2):
                swap_end(1, cc)
            swap_mid(1)
        with jax.named_scope("halo"):
            halo_wait(0)

        def pass_w1_x(e):
            j, hf = e >> 2, e & 3
            w1_x(j, hf).wait_recv()
            w1_y(j, hf).start()
            w1_fwd(j, sp, hf).start()

        def pass_w1_y(e):
            j, hf = e >> 2, e & 3
            w1_y(j, hf).wait_recv()
            w1_fwd(j, osp, hf).start()

        def pass_w2_x(e):
            n, h = pair(e)
            w2_x(n, h).wait_recv()
            w2_y(n, h).start()
            w2_fwd(n, sp, h).start()

        def pass_w2_y(e):
            n, h = pair(e)
            w2_y(n, h).wait_recv()
            w2_fwd(n, osp, h).start()

        def send_w1_x(e):
            w1_x(e >> 2, e & 3).start()

        def send_w2_x(e):
            w2_x(*pair(e)).start()

        def events(i):
            is_odd = odd(i)
            even = jnp.logical_not(is_odd)

            @rarely(i < 16)
            def _():
                @rarely(even)
                def _():
                    @rarely(i < 12)
                    def _():
                        w1_part(*jp(p_of((i >> 1) + 2))).start()

                    @rarely(i == 2)
                    def _():
                        x_copy(1).wait_recv()
                        halo_wait(1)

                    @rarely(i == 10)
                    def _():
                        lax.fori_loop(0, 4, lambda e, carry: (pass_w1_y(e), carry)[1], 0)

                    @rarely(i == 12)
                    def _():
                        lax.fori_loop(4, 6, lambda e, carry: (pass_w1_y(e), carry)[1], 0)

                @rarely(is_odd)
                def _():
                    @rarely(i == 1)
                    def _():
                        @rarely(c != sp)
                        def _():
                            halo_copy(0).start()

                        halo_copy(1).start()

                        @rarely(edge)
                        def _():
                            stage[0, 0:16] = jnp.zeros((16, cols, ni, cb), jnp.bfloat16)
                            zero_rows((rows + 1) * sp).start()

                    @rarely(i == 3)
                    def _():
                        x_copy(2).start()

                    @rarely(i == 5)
                    def _():
                        lax.fori_loop(0, 4, lambda e, carry: (pass_w1_x(e), carry)[1], 0)

                    @rarely(i == 7)
                    def _():
                        lax.fori_loop(4, 6, lambda e, carry: (pass_w1_x(e), carry)[1], 0)

                    @rarely(i == 9)
                    def _():
                        x_copy(3).start()

            @rarely((i >= 13) & (i < 23))
            def _():
                send_w1_x(i - 7)

            @rarely((i >= 16) & (i < 34))
            def _():
                @rarely((i >= 18) & (i < 28))
                def _():
                    pass_w1_x(i - 12)

                @rarely((i >= 20) & (i < 30))
                def _():
                    pass_w1_y(i - 14)

                @rarely(i < 24)
                def _():
                    e = i - 16
                    w2_part((e >> 2), ((e >> 1) & 1), (e & 1)).start()

                @rarely(even)
                def _():
                    @rarely(i == 16)
                    def _():
                        x_copy(2).wait_recv()
                        halo_wait(2)

                    @rarely(i == 30)
                    def _():
                        x_copy(1).wait_send()
                        x_copy(2).wait_send()
                        x_copy(3).wait_send()
                        for far in range(2):
                            halo_copy(far).wait_send()

                    @rarely((i >= 24) & ((i & 3) == 0))
                    def _():
                        send_w2_x(((i - 24) >> 2))

                @rarely(is_odd)
                def _():
                    @rarely(i == 17)
                    def _():
                        x_copy(3).wait_recv()
                        halo_wait(3)

                    @rarely(i >= 19)
                    def _():
                        for h in range(2):
                            hid_store(0, h).wait()

                    @rarely(i >= 27)
                    def _():
                        for d in range(2):
                            j, par = jp(i - 27 + d)
                            for h in range(2):
                                a = 4 * j + 2 * par + h

                                @pl.when(blk > 0)
                                def _():
                                    hid_up(a).start()

                                @pl.when(blk < 3)
                                def _():
                                    hid_dn(a).start()

                    @rarely(i == 31)
                    def _():
                        pass_w2_x(jnp.int32(0))

            @rarely((i >= 34) & (i < 50))
            def _():
                @rarely(i == 36)
                def _():
                    send_w2_x(jnp.int32(3))

                @rarely((i < 44) & ((i & 3) == 3))
                def _():
                    pass_w2_x(((i - 31) >> 2))

                @rarely((i >= 37) & ((i & 3) == 1))
                def _():
                    pass_w2_y(((i - 37) >> 2))

        def taps(xs_slot, ws_slot, col, lanes=slice(None)):
            total = None
            for dx in (-1, 0, 1):
                if not 0 <= col + dx < cols:
                    continue
                for dy in range(3):
                    lhs = xa[xs_slot, dy:dy + rows, col + dx].reshape(m_rows, cb)
                    prod = jnp.dot(lhs, wv[ws_slot, dy, dx + 1, :, lanes], preferred_element_type=jnp.float32)
                    total = prod if total is None else total + prod
            return total

        def step(i, carry):
            ph1 = i < 16
            ph3 = i >= 32
            n = jnp.where(ph3, ((i - 32) >> 4), 0)
            q = jnp.where(ph3, ((i - 32) & 15), 0)
            m, role = near_step(i)
            m = jnp.where(ph1, m, ((i - 16) >> 1))
            role = jnp.where(ph1, role, 2 + (i & 1))
            p = jnp.where(ph1, p_of(m), (m & 7))
            p = jnp.where(ph3, 0, p)
            last = jnp.where(ph3, q == 15, role == 3)
            first = jnp.where(ph3, q == 0, role == 0)
            a_slot = jnp.where(ph3, n, (p & 1))
            x_slot = jnp.where(ph3, 4 + (q & 1), role)
            w_slot = (i & 1)

            with jax.named_scope("ev"):
                events(i)
            with jax.named_scope("iss"):
                issue(i + 1)
            w_load(g1.at[0, 0, 0], i).wait()

            @pl.when(ph3)
            def _():
                hid_load(0, q).wait()

            @rarely((i >= 4) & (i < 32))
            def _():
                @pl.when(ph1 & first)
                def _():
                    pltpu.make_async_copy(acc.at[a_slot], part.at[0], pst.at[a_slot]).wait()

                @pl.when((i >= 20) & (role == 2))
                def _():
                    pltpu.make_async_copy(part.at[0], acc.at[a_slot], pld.at[a_slot]).wait()

            @pl.when(jnp.logical_not(last))
            def _():
                with jax.named_scope("mm"):
                    for col in range(cols):
                        total = taps(x_slot, w_slot, col)
                        acc[a_slot, col] = total + jnp.where(first, 0.0, acc[a_slot, col])

            @rarely((i < 12) & (role == 1))
            def _():
                pltpu.make_async_copy(acc.at[a_slot], part.at[p], pst.at[a_slot]).start()

            @pl.when(last & (i < N_STEPS - 1))
            def _():
                @pl.when((i == 17) & edge)
                def _():
                    zero_rows(0).wait()

                keep = jnp.where(ph3, 1.0, 0.0)
                floor = jnp.where(ph3, -jnp.inf, 0.0)
                j, par = jp(p)
                shift = b1[tile_of(x, j, par)] * (1.0 - keep)
                with jax.named_scope("mmo"):
                    for col in range(cols):
                        total = taps(x_slot, w_slot, col) + acc[a_slot, col] + shift
                        for h in range(2):
                            role = 2 + ((c + h) & 1)
                            res = xa[role, 1:rows + 1, col].reshape(m_rows, cb).astype(jnp.float32)
                            val = jnp.maximum(total[:, h * cb:(h + 1) * cb] + res * keep, floor)
                            stage[h, :, col] = val.astype(jnp.bfloat16).reshape(rows, ni, cb)

                @pl.when(i < 32)
                def _():
                    for h in range(2):
                        hid_store(4 * j + 2 * par + h, h).start()

                    @pl.when(p < 6)
                    def _():
                        pltpu.make_async_copy(part.at[p + 2], acc.at[a_slot], pld.at[a_slot]).start()

                @pl.when(i == 47)
                def _():
                    for h in range(2):
                        y_far(h).start()

            @pl.when(i == N_STEPS - 1)
            def _():
                for h in range(2):
                    y_far(h).wait_send()

                def half_step(own, carry):
                    h = jnp.where(own == 1, c, 1 - c)
                    lanes = pl.ds(pl.multiple_of(h * cb, cb), cb)
                    with jax.named_scope("half"):
                        for col in range(cols):
                            total = taps(x_slot, w_slot, col, lanes) + acc[a_slot, col, :, lanes]
                            res = xa[1 - own, 1:rows + 1, col].reshape(m_rows, cb).astype(jnp.float32)
                            stage[h, :, col] = (total + res).astype(jnp.bfloat16).reshape(rows, ni, cb)

                    @pl.when(own == 0)
                    def _():
                        y_near().start()

                    return carry

                lax.fori_loop(0, 2, half_step, 0)
                y_own().start()

            return carry

        lax.fori_loop(0, N_STEPS, step, 0)

        def drain(e, carry):
            hi, lo = pair(e)
            w1_part(hi, lo).wait_send()
            for hf in (lo, lo + 2):
                w1_x(hi, hf).wait_send()
                w1_y(hi, hf).wait_send()
            for hf in range(4):
                w1_fwd(hi, lo, hf).wait_send()
            n, par = e >> 2, (e >> 1) & 1
            w2_part(n, par, lo).wait_send()
            w2_fwd(n, par, lo).wait_send()
            return carry

        lax.fori_loop(0, 8, drain, 0)

        def drain_rows(a, carry):
            @pl.when(blk > 0)
            def _():
                hid_up(a).wait_send()

            @pl.when(blk < 3)
            def _():
                hid_dn(a).wait_send()

            return carry

        lax.fori_loop(0, 16, drain_rows, 0)

        def drain_two(e, carry):
            w2_x(*pair(e)).wait_send()
            w2_y(*pair(e)).wait_send()
            return carry

        lax.fori_loop(0, 4, drain_two, 0)
        for e in range(2):
            remote(stage.at[0], yt.at[0, pl.ds(0, rows)], ys.at[0], yr.at[e], sp, k).wait_recv()
        y_near().wait()
        y_own().wait()

    dma = pltpu.SemaphoreType.DMA
    bf16, f32 = jnp.bfloat16, jnp.float32
    any_space = pl.BlockSpec(memory_space=pl.ANY)
    outs = pl.pallas_call(
        kernel,
        out_shape=[
            jax.ShapeDtypeStruct((2, h_loc, cols, ni, cb), bf16),
            jax.ShapeDtypeStruct((3, 4, 2, 3, 3, cb, tile), bf16),
            jax.ShapeDtypeStruct((3, 2, 2, 2, 3, 3, cb, tile), bf16),
            jax.ShapeDtypeStruct((8, cols, m_rows, tile), f32),
            jax.ShapeDtypeStruct((16, rows + 2, cols, ni, cb), bf16),
        ],
        in_specs=[any_space, any_space, any_space, pl.BlockSpec(memory_space=pltpu.VMEM)],
        out_specs=[any_space] * 5,
        scratch_shapes=[
            pltpu.VMEM((7, rows + 2, cols, ni, cb), bf16),
            pltpu.VMEM((2, cols, m_rows, tile), f32),
            pltpu.VMEM((2, 3, 3, cb, tile), bf16),
            pltpu.VMEM((2, rows, cols, ni, cb), bf16),
            pltpu.VMEM((2, ni, cols, h_loc, cb), bf16),
            pltpu.VMEM((ni * ni, ni * ni), bf16),
            pltpu.VMEM((8, 128), f32),
            *map(dma, SEMS),
        ],
        compiler_params=pltpu.CompilerParams(collective_id=0, has_side_effects=True, vmem_limit_bytes=63 * MIB),
        name="fused_block",
    )(xw, w_one, w_two, bias)
    return outs[0]


def images_major(yt):
    groups, h_loc, cols, ni, cb = yt.shape
    parts = h_loc // ni
    width = cols // 2
    chunks = groups * parts * 2
    assert ni == 16

    def kernel(y, out, y_in, y_out, swap, in_sem, out_sem):
        def place(e):
            block, side = pair(e)
            group, part = lax.div(block, parts), lax.rem(block, parts)
            n0, h0 = pl.multiple_of(ni * group, ni), pl.multiple_of(ni * part, ni)
            return group, n0, h0, width * side

        def load(e):
            group, _, h0, col = place(e)
            cut = (group, pl.ds(h0, ni), pl.ds(col, width))
            return pltpu.make_async_copy(y.at[cut], y_in.at[cut], in_sem.at[e])

        def store(e):
            _, n0, h0, col = place(e)
            cut = (pl.ds(n0, ni), pl.ds(col, width), pl.ds(h0, ni))
            return pltpu.make_async_copy(y_out.at[cut], out.at[cut], out_sem.at[e])

        for e in range(chunks):
            load(jnp.int32(e)).start()
        swap[...] = swap_matrix(ni)

        def chunk(e, carry):
            load(e).wait()
            group, n0, h0, base = place(e)
            for col in range(width):
                rows_in = y_in[group, pl.ds(h0, ni), base + col].reshape(ni * ni, cb)
                res = jnp.dot(swap[...], rows_in, preferred_element_type=jnp.float32)
                y_out[pl.ds(n0, ni), base + col, pl.ds(h0, ni)] = res.astype(jnp.bfloat16).reshape(ni, ni, cb)
            store(e).start()
            return carry

        lax.fori_loop(0, chunks, chunk, 0)
        for e in range(chunks):
            store(jnp.int32(e)).wait()

    dma = pltpu.SemaphoreType.DMA
    out_shape = (groups * ni, cols, h_loc, cb)
    return pl.pallas_call(
        kernel,
        out_shape=jax.ShapeDtypeStruct(out_shape, jnp.bfloat16),
        in_specs=[pl.BlockSpec(memory_space=pl.ANY)],
        out_specs=pl.BlockSpec(memory_space=pl.ANY),
        scratch_shapes=[pltpu.VMEM(yt.shape, jnp.bfloat16), pltpu.VMEM(out_shape, jnp.bfloat16), pltpu.VMEM((ni * ni, ni * ni), jnp.bfloat16),
                        dma((chunks,)), dma((chunks,))],
        compiler_params=pltpu.CompilerParams(vmem_limit_bytes=63 * MIB),
        name="images_major",
    )(yt)


def solution(mesh):
    act_spec = P("dp", "sp", None, "cp")
    kernel_spec = P(None, None, "cp", None)

    def local_block(x_tile, w_one_part, w_two_part, bias_one):
        xw = x_tile.transpose(0, 2, 1, 3)
        yt = fused_block(xw, w_one_part, w_two_part, bias_one.reshape(8, 1, 2 * x_tile.shape[3]))
        return images_major(yt).transpose(0, 2, 1, 3)

    return jax.shard_map(local_block, mesh=mesh, in_specs=(act_spec, kernel_spec, kernel_spec, P()), out_specs=act_spec, check_vma=False)
```

```python
import functools

import jax
import jax.numpy as jnp
from jax import lax
from jax.experimental import pallas as pl
from jax.experimental.pallas import tpu as pltpu
from jax.sharding import PartitionSpec as P

MESH = pl.DeviceIdType.MESH
N_STEPS = 64
MIB = 1024 * 1024
ONE, TWO, THREE, FOUR, ALL = (1,), (2,), (3,), (4,), (2, 16)
GRID, CUBE, HALVES = (2, 2), (2, 2, 2), (4, 2)
QUARTERS, ROWS = (4, 4), (4, 2, 4)
SEMS = (
    TWO, TWO, TWO, TWO, TWO, ONE, (2, 3), THREE, THREE, TWO, FOUR,
    HALVES, HALVES, QUARTERS, QUARTERS, QUARTERS, QUARTERS, ROWS, ROWS,
    CUBE, CUBE, GRID, GRID, GRID, GRID, CUBE, CUBE,
    ALL, ALL, TWO, TWO, ONE, ONE, ONE,
)


def pair(e):
    return e >> 1, e & 1


def each(first, stop, act):
    lax.fori_loop(first, stop, lambda e, carry: (act(e), carry)[1], 0)


def odd(i):
    return (i & 1) == 1


def swap_matrix(n):
    shift = n.bit_length() - 1
    to = lax.broadcasted_iota(jnp.int32, (n * n, n * n), 0)
    frm = lax.broadcasted_iota(jnp.int32, (n * n, n * n), 1)
    hit = ((to >> shift) == (frm & (n - 1))) & ((to & (n - 1)) == (frm >> shift))
    return jnp.where(hit, 1.0, 0.0).astype(jnp.bfloat16)


def fused_block(xw, w_one, w_two, bias):
    images, cols, h_loc, cb = xw.shape
    ni = images // 2
    rows = h_loc // 2
    m_rows = rows * ni
    tile = 2 * cb
    assert ni == 16 and h_loc == 48

    def remote(src, dst, send_sem, recv_sem, sp, cp):
        return pltpu.make_async_remote_copy(src_ref=src, dst_ref=dst, send_sem=send_sem, recv_sem=recv_sem,
                                            device_id={"sp": sp, "cp": cp}, device_id_type=MESH)

    def kernel(xw, w1, w2, b1, yt, g1, g2, part, hid,
               xa, acc, wv, stage, raw, swap, mark,
               wsem, asem, pst, pld, stl, zsem, rsem, xs, xr, hs, hr,
               p1s, p1r, x1s, x1r, y1s, y1r, f1s, f1r,
               p2s, p2r, x2s, x2r, y2s, y2r, f2s, f2r,
               as_, ar, ys, yr, zs, zr, yl):
        sp = lax.axis_index("sp")
        k = lax.axis_index("cp")
        x = (k >> 1)
        c = (k & 1)
        blk = 2 * sp + c
        osp = 1 - sp
        k1 = 2 * x + (1 - c)
        k2 = 2 * (1 - x) + c
        k3 = 2 * (1 - x) + (1 - c)

        def rarely(cond):
            def wrap(body):
                @pl.when(cond)
                def _():
                    mark[...] = jnp.zeros(mark.shape, jnp.float32)
                    body()

            return wrap

        def tile_of(xx, j, par):
            return 4 * ((xx + (j >> 1)) & 1) + 2 * (j & 1) + par

        barrier = pltpu.get_barrier_semaphore()
        for d_sp in range(2):
            for d_cp in range(4):
                if d_sp or d_cp:
                    pl.semaphore_signal(barrier, inc=1, device_id={"sp": ((sp + d_sp) & 1), "cp": ((k + d_cp) & 3)},
                                        device_id_type=MESH)

        def raw_load(far, part):
            cut = pl.ds(pl.multiple_of(ni * part, ni), ni)
            group = pl.ds(ni * (1 - x if far else x), ni)
            return pltpu.make_async_copy(xw.at[group, :, cut], raw.at[far, :, :, cut], rsem.at[far, part])

        def block(far, col, part):
            rows_in = raw[far, :, col, pl.ds(pl.multiple_of(ni * part, ni), ni), :].reshape(ni * ni, cb)
            out = jnp.dot(swap[...], rows_in, preferred_element_type=jnp.float32)
            return out.astype(jnp.bfloat16).reshape(ni, ni, cb)

        def slot_of(far, cc):
            return jnp.where(cc == c, 5 if far else 0, 6 if far else 4)

        def swap_end(far, cc):
            for col in range(cols):
                xa[slot_of(far, cc), pl.ds(1 + 8 * cc, ni), col] = block(far, col, 2 * cc)

        def swap_mid(far):
            for col in range(cols):
                mid = block(far, col, 1)
                xa[slot_of(far, 0), 17:26, col] = mid[0:9]
                xa[slot_of(far, 1), 0:9, col] = mid[7:16]

        def x_copy(role):
            cc = c if role == 2 else 1 - c
            cut = pl.ds(1 - cc, rows + 1)
            return remote(xa.at[3 + role, cut], xa.at[role, cut], xs.at[role - 1], xr.at[role - 1], sp,
                          {1: k1, 2: k2, 3: k3}[role])

        def halo_copy(far):
            xx = 1 - x if far else x
            role = 2 * ((x + xx) & 1) + ((c + sp) & 1)
            src = xa.at[slot_of(far, osp), jnp.where(sp == 0, rows, 1)]
            return remote(src, xa.at[role, (rows + 1) * sp], hs.at[far], hr.at[role], osp, 2 * xx + sp)

        piece = cb // 4

        def w1_own(j, par, xx):
            return w1.at[:, :, :, pl.ds(pl.multiple_of(tile_of(xx, j, par) * tile, tile), tile)]

        def w1_part(j, par):
            return remote(w1_own(j, par, x), g1.at[0, j, par], p1s.at[j, par], p1r.at[j, par], sp, k1)

        def w1_x(j, hf):
            cut = pl.ds(pl.multiple_of(hf * piece, piece), piece)
            src = w1.at[:, :, cut, pl.ds(pl.multiple_of(tile_of(1 - x, j, sp) * tile, tile), tile)]
            return remote(src, g1.at[1, j, sp, :, :, cut], x1s.at[j, hf], x1r.at[j, hf], sp, k2)

        def w1_y(j, hf):
            cut = pl.ds(pl.multiple_of(hf * piece, piece), piece)
            ref = g1.at[1, j, sp, :, :, cut]
            return remote(ref, ref, y1s.at[j, hf], y1r.at[j, hf], osp, k)

        def w1_fwd(j, par, hf):
            cut = pl.ds(pl.multiple_of(hf * piece, piece), piece)
            return remote(g1.at[1, j, par, :, :, cut], g1.at[2, j, par, :, :, cut], f1s.at[j, par, hf], f1r.at[j, par, hf], sp, k1)

        def w2_cut(n, par, h, xx):
            row = pl.multiple_of(par * tile + h * cb, cb)
            col = pl.multiple_of(tile * ((1 + xx + n) & 1), tile)
            return w2.at[:, :, pl.ds(row, cb), pl.ds(col, tile)]

        def w2_part(n, par, h):
            return remote(w2_cut(n, par, h, x), g2.at[0, n, par, h], p2s.at[n, par, h], p2r.at[n, par, h], sp, k1)

        def w2_x(n, h):
            return remote(w2_cut(n, sp, h, 1 - x), g2.at[1, n, sp, h], x2s.at[n, h], x2r.at[n, h], sp, k2)

        def w2_y(n, h):
            ref = g2.at[1, n, sp, h]
            return remote(ref, ref, y2s.at[n, h], y2r.at[n, h], osp, k)

        def w2_fwd(n, par, h):
            return remote(g2.at[1, n, par, h], g2.at[2, n, par, h], f2s.at[n, par, h], f2r.at[n, par, h], sp, k1)

        up_blk = lax.max(blk - 1, 0)
        dn_blk = lax.min(blk + 1, 3)

        def hid_up(a):
            return remote(hid.at[a, 1], hid.at[a, rows + 1], as_.at[0, a], ar.at[1, a], (up_blk >> 1), 2 * x + (up_blk & 1))

        def hid_dn(a):
            return remote(hid.at[a, rows], hid.at[a, 0], as_.at[1, a], ar.at[0, a], (dn_blk >> 1), 2 * x + (dn_blk & 1))

        def hid_store(a, h):
            return pltpu.make_async_copy(stage.at[h], hid.at[a, pl.ds(1, rows)], stl.at[h])

        y_rows = pl.ds(rows * c, rows)

        def y_far(h):
            return remote(stage.at[h], yt.at[x, y_rows], ys.at[h], yr.at[((h + c) & 1)], sp, 2 * (1 - x) + h)

        def y_near():
            return remote(stage.at[1 - c], yt.at[x, y_rows], zs.at[0], zr.at[0], sp, k1)

        def y_own():
            return pltpu.make_async_copy(stage.at[c], yt.at[x, y_rows], yl.at[0])

        def zero_rows(row):
            return pltpu.make_async_copy(stage.at[0, pl.ds(0, 16)], hid.at[:, row], zsem.at[0])

        def p_of(m):
            return (m + 2) & 7

        def jp(p):
            return p >> 1, (sp + p) & 1

        def send_w1_x(e):
            w1_x(e >> 2, e & 3).start()

        def near_step(i):
            return 2 * (i >> 2) + (i & 1), (i & 2) >> 1

        def halo_wait(role):
            @pl.when(c != sp)
            def _():
                remote(xa.at[0, 0], xa.at[role, 0], hs.at[0], hr.at[role], osp, k).wait_recv()

        for part_no in (2 * osp, 2 * sp, 1):
            raw_load(0, part_no).start()
        swap[...] = swap_matrix(ni)
        edge = c == sp

        @pl.when(edge)
        def _():
            xa[0:4, (rows + 1) * sp] = jnp.zeros((4, cols, ni, cb), jnp.bfloat16)

        def w_load(src, t):
            return pltpu.make_async_copy(src, wv.at[(t & 1)], wsem.at[(t & 1)])

        def hid_load(a, q):
            slot = (q & 1)
            return pltpu.make_async_copy(hid.at[a], xa.at[4 + slot], asem.at[slot])

        def issue(t):
            @rarely(t < 16)
            def _():
                m, role = near_step(t)
                j, par = jp(p_of(m))

                @rarely(role == 0)
                def _():
                    w_load(w1_own(j, par, x), t).start()

                @rarely(role == 1)
                def _():
                    w1_part(j, par).wait_recv()
                    w_load(g1.at[0, j, par], t).start()

            @rarely((t >= 16) & (t < 32))
            def _():
                j, par = jp(((t - 16) >> 1))

                @rarely((t & 1) == 1)
                def _():
                    for hf in range(4):
                        w1_fwd(j, par, hf).wait_recv()

                w_load(g1.at[1 + (t & 1), j, par], t).start()

            @rarely((t >= 32) & (t < N_STEPS))
            def _():
                n = ((t - 32) >> 4)
                q = ((t - 32) & 15)
                h = (q & 1)
                p = (q >> 1)
                j, par = jp(p)
                a = 4 * j + 2 * par + h
                same = (j & 1) == c

                @rarely(n == 0)
                def _():
                    @pl.when(blk > 0)
                    def _():
                        hid_dn(a).wait_recv()

                    @pl.when(blk < 3)
                    def _():
                        hid_up(a).wait_recv()

                hid_load(a, q).start()

                @rarely(p < 4)
                def _():
                    @rarely(same)
                    def _():
                        w_load(w2_cut(n, par, h, x), t).start()

                    @rarely(jnp.logical_not(same))
                    def _():
                        w2_part(n, par, h).wait_recv()
                        w_load(g2.at[0, n, par, h], t).start()

                @rarely(p >= 4)
                def _():
                    @pl.when(jnp.logical_not(same))
                    def _():
                        w2_fwd(n, par, h).wait_recv()

                    w_load(g2.at[jnp.where(same, 1, 2), n, par, h], t).start()

        raw_load(0, 2 * osp).wait()
        issue(jnp.int32(0))
        for part_no in range(3):
            raw_load(1, part_no).start()
        swap_end(0, osp)
        pl.semaphore_wait(barrier, 7)

        @pl.when(edge)
        def _():
            halo_copy(0).start()

        each(0, 6, send_w1_x)
        raw_load(0, 2 * sp).wait()
        raw_load(0, 1).wait()
        swap_end(0, sp)
        swap_mid(0)
        x_copy(1).start()
        for m in range(2):
            w1_part(*jp(jnp.int32(m + 2))).start()
        for part_no in range(3):
            raw_load(1, part_no).wait()
        for cc in range(2):
            swap_end(1, cc)
        swap_mid(1)
        halo_wait(0)

        def pass_w1_x(e):
            j, hf = e >> 2, e & 3
            w1_x(j, hf).wait_recv()
            w1_y(j, hf).start()
            w1_fwd(j, sp, hf).start()

        def pass_w1_y(e):
            j, hf = e >> 2, e & 3
            w1_y(j, hf).wait_recv()
            w1_fwd(j, osp, hf).start()

        def pass_w2_x(e):
            n, h = pair(e)
            w2_x(n, h).wait_recv()
            w2_y(n, h).start()
            w2_fwd(n, sp, h).start()

        def pass_w2_y(e):
            n, h = pair(e)
            w2_y(n, h).wait_recv()
            w2_fwd(n, osp, h).start()

        def send_w2_x(e):
            w2_x(*pair(e)).start()

        def events(i):
            is_odd = odd(i)
            even = jnp.logical_not(is_odd)

            @rarely(i < 16)
            def _():
                @rarely(even)
                def _():
                    @rarely(i < 12)
                    def _():
                        w1_part(*jp(p_of((i >> 1) + 2))).start()

                    @rarely(i == 2)
                    def _():
                        x_copy(1).wait_recv()
                        halo_wait(1)

                    @rarely(i == 10)
                    def _():
                        each(0, 4, pass_w1_y)

                    @rarely(i == 12)
                    def _():
                        each(4, 6, pass_w1_y)

                @rarely(is_odd)
                def _():
                    @rarely(i == 1)
                    def _():
                        @rarely(c != sp)
                        def _():
                            halo_copy(0).start()

                        halo_copy(1).start()

                        @rarely(edge)
                        def _():
                            stage[0, 0:16] = jnp.zeros((16, cols, ni, cb), jnp.bfloat16)
                            zero_rows((rows + 1) * sp).start()

                    @rarely(i == 3)
                    def _():
                        x_copy(2).start()

                    @rarely(i == 5)
                    def _():
                        each(0, 4, pass_w1_x)

                    @rarely(i == 7)
                    def _():
                        each(4, 6, pass_w1_x)

                    @rarely(i == 9)
                    def _():
                        x_copy(3).start()

            @rarely((i >= 13) & (i < 23))
            def _():
                send_w1_x(i - 7)

            @rarely((i >= 16) & (i < 34))
            def _():
                @rarely((i >= 18) & (i < 28))
                def _():
                    pass_w1_x(i - 12)

                @rarely((i >= 20) & (i < 30))
                def _():
                    pass_w1_y(i - 14)

                @rarely(i < 24)
                def _():
                    e = i - 16
                    w2_part((e >> 2), ((e >> 1) & 1), (e & 1)).start()

                @rarely(even)
                def _():
                    @rarely(i == 16)
                    def _():
                        x_copy(2).wait_recv()
                        halo_wait(2)

                    @rarely(i == 30)
                    def _():
                        x_copy(1).wait_send()
                        x_copy(2).wait_send()
                        x_copy(3).wait_send()
                        for far in range(2):
                            halo_copy(far).wait_send()

                    @rarely((i >= 24) & ((i & 3) == 0))
                    def _():
                        send_w2_x(((i - 24) >> 2))

                @rarely(is_odd)
                def _():
                    @rarely(i == 17)
                    def _():
                        x_copy(3).wait_recv()
                        halo_wait(3)

                    @rarely(i >= 19)
                    def _():
                        for h in range(2):
                            hid_store(0, h).wait()

                    @rarely(i >= 27)
                    def _():
                        for d in range(2):
                            j, par = jp(i - 27 + d)
                            for h in range(2):
                                a = 4 * j + 2 * par + h

                                @pl.when(blk > 0)
                                def _():
                                    hid_up(a).start()

                                @pl.when(blk < 3)
                                def _():
                                    hid_dn(a).start()

                    @rarely(i == 31)
                    def _():
                        pass_w2_x(jnp.int32(0))

            @rarely((i >= 34) & (i < 50))
            def _():
                @rarely(i == 36)
                def _():
                    send_w2_x(jnp.int32(3))

                @rarely((i < 44) & ((i & 3) == 3))
                def _():
                    pass_w2_x(((i - 31) >> 2))

                @rarely((i >= 37) & ((i & 3) == 1))
                def _():
                    pass_w2_y(((i - 37) >> 2))

        def taps(xs_slot, ws_slot, col, lanes=slice(None)):
            total = None
            for dx in (-1, 0, 1):
                if not 0 <= col + dx < cols:
                    continue
                for dy in range(3):
                    lhs = xa[xs_slot, dy:dy + rows, col + dx].reshape(m_rows, cb)
                    prod = jnp.dot(lhs, wv[ws_slot, dy, dx + 1, :, lanes], preferred_element_type=jnp.float32)
                    total = prod if total is None else total + prod
            return total

        def step(i, carry):
            ph1 = i < 16
            ph3 = i >= 32
            n = jnp.where(ph3, ((i - 32) >> 4), 0)
            q = jnp.where(ph3, ((i - 32) & 15), 0)
            m, role = near_step(i)
            m = jnp.where(ph1, m, ((i - 16) >> 1))
            role = jnp.where(ph1, role, 2 + (i & 1))
            p = jnp.where(ph1, p_of(m), (m & 7))
            p = jnp.where(ph3, 0, p)
            last = jnp.where(ph3, q == 15, role == 3)
            first = jnp.where(ph3, q == 0, role == 0)
            a_slot = jnp.where(ph3, n, (p & 1))
            x_slot = jnp.where(ph3, 4 + (q & 1), role)
            w_slot = (i & 1)

            events(i)
            issue(i + 1)
            w_load(g1.at[0, 0, 0], i).wait()

            @pl.when(ph3)
            def _():
                hid_load(0, q).wait()

            @rarely((i >= 4) & (i < 32))
            def _():
                @pl.when(ph1 & first)
                def _():
                    pltpu.make_async_copy(acc.at[a_slot], part.at[0], pst.at[a_slot]).wait()

                @pl.when((i >= 20) & (role == 2))
                def _():
                    pltpu.make_async_copy(part.at[0], acc.at[a_slot], pld.at[a_slot]).wait()

            @pl.when(jnp.logical_not(last))
            def _():
                for col in range(cols):
                    total = taps(x_slot, w_slot, col)
                    acc[a_slot, col] = total + jnp.where(first, 0.0, acc[a_slot, col])

            @rarely((i < 12) & (role == 1))
            def _():
                pltpu.make_async_copy(acc.at[a_slot], part.at[p], pst.at[a_slot]).start()

            @pl.when(last & (i < N_STEPS - 1))
            def _():
                @pl.when((i == 17) & edge)
                def _():
                    zero_rows(0).wait()

                keep = jnp.where(ph3, 1.0, 0.0)
                floor = jnp.where(ph3, -jnp.inf, 0.0)
                j, par = jp(p)
                shift = b1[tile_of(x, j, par)] * (1.0 - keep)
                for col in range(cols):
                    total = taps(x_slot, w_slot, col) + acc[a_slot, col] + shift
                    for h in range(2):
                        role = 2 + ((c + h) & 1)
                        res = xa[role, 1:rows + 1, col].reshape(m_rows, cb).astype(jnp.float32)
                        val = jnp.maximum(total[:, h * cb:(h + 1) * cb] + res * keep, floor)
                        stage[h, :, col] = val.astype(jnp.bfloat16).reshape(rows, ni, cb)

                @pl.when(i < 32)
                def _():
                    for h in range(2):
                        hid_store(4 * j + 2 * par + h, h).start()

                    @pl.when(p < 6)
                    def _():
                        pltpu.make_async_copy(part.at[p + 2], acc.at[a_slot], pld.at[a_slot]).start()

                @pl.when(i == 47)
                def _():
                    for h in range(2):
                        y_far(h).start()

            @pl.when(i == N_STEPS - 1)
            def _():
                for h in range(2):
                    y_far(h).wait_send()

                def half_step(own, carry):
                    h = jnp.where(own == 1, c, 1 - c)
                    lanes = pl.ds(pl.multiple_of(h * cb, cb), cb)
                    for col in range(cols):
                        total = taps(x_slot, w_slot, col, lanes) + acc[a_slot, col, :, lanes]
                        res = xa[1 - own, 1:rows + 1, col].reshape(m_rows, cb).astype(jnp.float32)
                        stage[h, :, col] = (total + res).astype(jnp.bfloat16).reshape(rows, ni, cb)

                    @pl.when(own == 0)
                    def _():
                        y_near().start()

                    return carry

                lax.fori_loop(0, 2, half_step, 0)
                y_own().start()

            return carry

        lax.fori_loop(0, N_STEPS, step, 0)

        def drain(e, carry):
            hi, lo = pair(e)
            w1_part(hi, lo).wait_send()
            for hf in (lo, lo + 2):
                w1_x(hi, hf).wait_send()
                w1_y(hi, hf).wait_send()
            for hf in range(4):
                w1_fwd(hi, lo, hf).wait_send()
            n, par = e >> 2, (e >> 1) & 1
            w2_part(n, par, lo).wait_send()
            w2_fwd(n, par, lo).wait_send()
            return carry

        lax.fori_loop(0, 8, drain, 0)

        def drain_rows(a, carry):
            @pl.when(blk > 0)
            def _():
                hid_up(a).wait_send()

            @pl.when(blk < 3)
            def _():
                hid_dn(a).wait_send()

            return carry

        lax.fori_loop(0, 16, drain_rows, 0)

        def drain_two(e, carry):
            w2_x(*pair(e)).wait_send()
            w2_y(*pair(e)).wait_send()
            return carry

        lax.fori_loop(0, 4, drain_two, 0)
        for e in range(2):
            remote(stage.at[0], yt.at[0, pl.ds(0, rows)], ys.at[0], yr.at[e], sp, k).wait_recv()
        y_near().wait()
        y_own().wait()

    dma = pltpu.SemaphoreType.DMA
    bf16, f32 = jnp.bfloat16, jnp.float32
    any_space = pl.BlockSpec(memory_space=pl.ANY)
    outs = pl.pallas_call(
        kernel,
        out_shape=[
            jax.ShapeDtypeStruct((2, h_loc, cols, ni, cb), bf16),
            jax.ShapeDtypeStruct((3, 4, 2, 3, 3, cb, tile), bf16),
            jax.ShapeDtypeStruct((3, 2, 2, 2, 3, 3, cb, tile), bf16),
            jax.ShapeDtypeStruct((8, cols, m_rows, tile), f32),
            jax.ShapeDtypeStruct((16, rows + 2, cols, ni, cb), bf16),
        ],
        in_specs=[any_space, any_space, any_space, pl.BlockSpec(memory_space=pltpu.VMEM)],
        out_specs=[any_space] * 5,
        scratch_shapes=[
            pltpu.VMEM((7, rows + 2, cols, ni, cb), bf16),
            pltpu.VMEM((2, cols, m_rows, tile), f32),
            pltpu.VMEM((2, 3, 3, cb, tile), bf16),
            pltpu.VMEM((2, rows, cols, ni, cb), bf16),
            pltpu.VMEM((2, ni, cols, h_loc, cb), bf16),
            pltpu.VMEM((ni * ni, ni * ni), bf16),
            pltpu.VMEM((8, 128), f32),
            *map(dma, SEMS),
        ],
        compiler_params=pltpu.CompilerParams(collective_id=0, has_side_effects=True, vmem_limit_bytes=63 * MIB),
        name="fused_block",
    )(xw, w_one, w_two, bias)
    return outs[0]


def images_major(yt):
    groups, h_loc, cols, ni, cb = yt.shape
    parts = h_loc // ni
    width = cols // 2
    chunks = groups * parts * 2
    assert ni == 16

    def kernel(y, out, y_in, y_out, swap, in_sem, out_sem):
        def place(e):
            block, side = pair(e)
            group, part = lax.div(block, parts), lax.rem(block, parts)
            n0, h0 = pl.multiple_of(ni * group, ni), pl.multiple_of(ni * part, ni)
            return group, n0, h0, width * side

        def load(e):
            group, _, h0, col = place(e)
            cut = (group, pl.ds(h0, ni), pl.ds(col, width))
            return pltpu.make_async_copy(y.at[cut], y_in.at[cut], in_sem.at[e])

        def store(e):
            _, n0, h0, col = place(e)
            cut = (pl.ds(n0, ni), pl.ds(col, width), pl.ds(h0, ni))
            return pltpu.make_async_copy(y_out.at[cut], out.at[cut], out_sem.at[e])

        for e in range(chunks):
            load(jnp.int32(e)).start()
        swap[...] = swap_matrix(ni)

        def chunk(e, carry):
            load(e).wait()
            group, n0, h0, base = place(e)
            for col in range(width):
                rows_in = y_in[group, pl.ds(h0, ni), base + col].reshape(ni * ni, cb)
                res = jnp.dot(swap[...], rows_in, preferred_element_type=jnp.float32)
                y_out[pl.ds(n0, ni), base + col, pl.ds(h0, ni)] = res.astype(jnp.bfloat16).reshape(ni, ni, cb)
            store(e).start()
            return carry

        lax.fori_loop(0, chunks, chunk, 0)
        for e in range(chunks):
            store(jnp.int32(e)).wait()

    dma = pltpu.SemaphoreType.DMA
    out_shape = (groups * ni, cols, h_loc, cb)
    return pl.pallas_call(
        kernel,
        out_shape=jax.ShapeDtypeStruct(out_shape, jnp.bfloat16),
        in_specs=[pl.BlockSpec(memory_space=pl.ANY)],
        out_specs=pl.BlockSpec(memory_space=pl.ANY),
        scratch_shapes=[pltpu.VMEM(yt.shape, jnp.bfloat16), pltpu.VMEM(out_shape, jnp.bfloat16), pltpu.VMEM((ni * ni, ni * ni), jnp.bfloat16),
                        dma((chunks,)), dma((chunks,))],
        compiler_params=pltpu.CompilerParams(vmem_limit_bytes=63 * MIB),
        name="images_major",
    )(yt)


def solution(mesh):
    act_spec = P("dp", "sp", None, "cp")
    kernel_spec = P(None, None, "cp", None)

    def local_block(x_tile, w_one_part, w_two_part, bias_one):
        xw = x_tile.transpose(0, 2, 1, 3)
        yt = fused_block(xw, w_one_part, w_two_part, bias_one.reshape(8, 1, 2 * x_tile.shape[3]))
        return images_major(yt).transpose(0, 2, 1, 3)

    return jax.shard_map(local_block, mesh=mesh, in_specs=(act_spec, kernel_spec, kernel_spec, P()), out_specs=act_spec, check_vma=False)
```

```python
import functools

import jax
import jax.numpy as jnp
from jax import lax
from jax.experimental import pallas as pl
from jax.experimental.pallas import tpu as pltpu
from jax.sharding import PartitionSpec as P

MESH = pl.DeviceIdType.MESH
N_STEPS = 64
MIB = 1024 * 1024
ONE, TWO, THREE, FOUR, ALL = (1,), (2,), (3,), (4,), (2, 16)
GRID, CUBE, HALVES = (2, 2), (2, 2, 2), (4, 2)
QUARTERS, ROWS = (4, 4), (4, 2, 4)
SEMS = (
    TWO, TWO, TWO, TWO, TWO, ONE, (2, 3), THREE, THREE, TWO, FOUR,
    HALVES, HALVES, QUARTERS, QUARTERS, QUARTERS, QUARTERS, ROWS, ROWS,
    CUBE, CUBE, GRID, GRID, GRID, GRID, CUBE, CUBE,
    ALL, ALL, TWO, TWO, ONE, ONE, ONE,
)


def pair(e):
    return e >> 1, e & 1


def each(first, stop, act):
    lax.fori_loop(first, stop, lambda e, carry: (act(e), carry)[1], 0)


def odd(i):
    return (i & 1) == 1


def swap_matrix(n):
    shift = n.bit_length() - 1
    to = lax.broadcasted_iota(jnp.int32, (n * n, n * n), 0)
    frm = lax.broadcasted_iota(jnp.int32, (n * n, n * n), 1)
    hit = ((to >> shift) == (frm & (n - 1))) & ((to & (n - 1)) == (frm >> shift))
    return jnp.where(hit, 1.0, 0.0).astype(jnp.bfloat16)


def fused_block(xw, w_one, w_two, bias):
    images, cols, h_loc, cb = xw.shape
    ni = images // 2
    rows = h_loc // 2
    m_rows = rows * ni
    tile = 2 * cb
    assert ni == 16 and h_loc == 48

    def remote(src, dst, send_sem, recv_sem, sp, cp):
        return pltpu.make_async_remote_copy(src_ref=src, dst_ref=dst, send_sem=send_sem, recv_sem=recv_sem,
                                            device_id={"sp": sp, "cp": cp}, device_id_type=MESH)

    def kernel(xw, w1, w2, b1, yt, g1, g2, part, hid,
               xa, acc, wv, stage, raw, swap, mark,
               wsem, asem, pst, pld, stl, zsem, rsem, xs, xr, hs, hr,
               p1s, p1r, x1s, x1r, y1s, y1r, f1s, f1r,
               p2s, p2r, x2s, x2r, y2s, y2r, f2s, f2r,
               as_, ar, ys, yr, zs, zr, yl):
        sp = lax.axis_index("sp")
        k = lax.axis_index("cp")
        x = (k >> 1)
        c = (k & 1)
        blk = 2 * sp + c
        osp = 1 - sp
        k1 = 2 * x + (1 - c)
        k2 = 2 * (1 - x) + c
        k3 = 2 * (1 - x) + (1 - c)

        def rarely(cond):
            def wrap(body):
                @pl.when(cond)
                def _():
                    mark[...] = jnp.zeros(mark.shape, jnp.float32)
                    body()

            return wrap

        def tile_of(xx, j, par):
            return 4 * ((xx + (j >> 1)) & 1) + 2 * (j & 1) + par

        barrier = pltpu.get_barrier_semaphore()
        for d_sp in range(2):
            for d_cp in range(4):
                if d_sp or d_cp:
                    pl.semaphore_signal(barrier, inc=1, device_id={"sp": ((sp + d_sp) & 1), "cp": ((k + d_cp) & 3)},
                                        device_id_type=MESH)

        def raw_load(far, part):
            cut = pl.ds(pl.multiple_of(ni * part, ni), ni)
            group = pl.ds(ni * (1 - x if far else x), ni)
            return pltpu.make_async_copy(xw.at[group, :, cut], raw.at[far, :, :, cut], rsem.at[far, part])

        def block(far, col, part):
            rows_in = raw[far, :, col, pl.ds(pl.multiple_of(ni * part, ni), ni), :].reshape(ni * ni, cb)
            out = jnp.dot(swap[...], rows_in, preferred_element_type=jnp.float32)
            return out.astype(jnp.bfloat16).reshape(ni, ni, cb)

        def slot_of(far, cc):
            return jnp.where(cc == c, 5 if far else 0, 6 if far else 4)

        def swap_end(far, cc):
            for col in range(cols):
                xa[slot_of(far, cc), pl.ds(1 + 8 * cc, ni), col] = block(far, col, 2 * cc)

        def swap_mid(far):
            for col in range(cols):
                mid = block(far, col, 1)
                xa[slot_of(far, 0), 17:26, col] = mid[0:9]
                xa[slot_of(far, 1), 0:9, col] = mid[7:16]

        def x_copy(role):
            cc = c if role == 2 else 1 - c
            cut = pl.ds(1 - cc, rows + 1)
            return remote(xa.at[3 + role, cut], xa.at[role, cut], xs.at[role - 1], xr.at[role - 1], sp,
                          {1: k1, 2: k2, 3: k3}[role])

        def halo_copy(far):
            xx = 1 - x if far else x
            role = 2 * ((x + xx) & 1) + ((c + sp) & 1)
            src = xa.at[slot_of(far, osp), jnp.where(sp == 0, rows, 1)]
            return remote(src, xa.at[role, (rows + 1) * sp], hs.at[far], hr.at[role], osp, 2 * xx + sp)

        piece = cb // 4

        def w1_own(j, par, xx):
            return w1.at[:, :, :, pl.ds(pl.multiple_of(tile_of(xx, j, par) * tile, tile), tile)]

        def w1_part(j, par):
            return remote(w1_own(j, par, x), g1.at[0, j, par], p1s.at[j, par], p1r.at[j, par], sp, k1)

        def w1_x(j, hf):
            cut = pl.ds(pl.multiple_of(hf * piece, piece), piece)
            src = w1.at[:, :, cut, pl.ds(pl.multiple_of(tile_of(1 - x, j, sp) * tile, tile), tile)]
            return remote(src, g1.at[1, j, sp, :, :, cut], x1s.at[j, hf], x1r.at[j, hf], sp, k2)

        def w1_y(j, hf):
            cut = pl.ds(pl.multiple_of(hf * piece, piece), piece)
            ref = g1.at[1, j, sp, :, :, cut]
            return remote(ref, ref, y1s.at[j, hf], y1r.at[j, hf], osp, k)

        def w1_fwd(j, par, hf):
            cut = pl.ds(pl.multiple_of(hf * piece, piece), piece)
            return remote(g1.at[1, j, par, :, :, cut], g1.at[2, j, par, :, :, cut], f1s.at[j, par, hf], f1r.at[j, par, hf], sp, k1)

        def w2_cut(n, par, h, xx):
            row = pl.multiple_of(par * tile + h * cb, cb)
            col = pl.multiple_of(tile * ((1 + xx + n) & 1), tile)
            return w2.at[:, :, pl.ds(row, cb), pl.ds(col, tile)]

        def w2_part(n, par, h):
            return remote(w2_cut(n, par, h, x), g2.at[0, n, par, h], p2s.at[n, par, h], p2r.at[n, par, h], sp, k1)

        def w2_x(n, h):
            return remote(w2_cut(n, sp, h, 1 - x), g2.at[1, n, sp, h], x2s.at[n, h], x2r.at[n, h], sp, k2)

        def w2_y(n, h):
            ref = g2.at[1, n, sp, h]
            return remote(ref, ref, y2s.at[n, h], y2r.at[n, h], osp, k)

        def w2_fwd(n, par, h):
            return remote(g2.at[1, n, par, h], g2.at[2, n, par, h], f2s.at[n, par, h], f2r.at[n, par, h], sp, k1)

        up_blk = lax.max(blk - 1, 0)
        dn_blk = lax.min(blk + 1, 3)

        def hid_up(a):
            return remote(hid.at[a, 1], hid.at[a, rows + 1], as_.at[0, a], ar.at[1, a], (up_blk >> 1), 2 * x + (up_blk & 1))

        def hid_dn(a):
            return remote(hid.at[a, rows], hid.at[a, 0], as_.at[1, a], ar.at[0, a], (dn_blk >> 1), 2 * x + (dn_blk & 1))

        def hid_store(a, h):
            return pltpu.make_async_copy(stage.at[h], hid.at[a, pl.ds(1, rows)], stl.at[h])

        y_rows = pl.ds(rows * c, rows)

        def y_far(h):
            return remote(stage.at[h], yt.at[x, y_rows], ys.at[h], yr.at[((h + c) & 1)], sp, 2 * (1 - x) + h)

        def y_near():
            return remote(stage.at[1 - c], yt.at[x, y_rows], zs.at[0], zr.at[0], sp, k1)

        def y_own():
            return pltpu.make_async_copy(stage.at[c], yt.at[x, y_rows], yl.at[0])

        def zero_rows(row):
            return pltpu.make_async_copy(stage.at[0, pl.ds(0, 16)], hid.at[:, row], zsem.at[0])

        def p_of(m):
            return (m + 2) & 7

        def jp(p):
            return p >> 1, (sp + p) & 1

        def send_w1_x(e):
            w1_x(e >> 2, e & 3).start()

        def near_step(i):
            return 2 * (i >> 2) + (i & 1), (i & 2) >> 1

        def halo_wait(role):
            @pl.when(c != sp)
            def _():
                remote(xa.at[0, 0], xa.at[role, 0], hs.at[0], hr.at[role], osp, k).wait_recv()

        for part_no in (2 * osp, 2 * sp, 1):
            raw_load(0, part_no).start()
        swap[...] = swap_matrix(ni)
        edge = c == sp

        @pl.when(edge)
        def _():
            xa[0:4, (rows + 1) * sp] = jnp.zeros((4, cols, ni, cb), jnp.bfloat16)

        def w_load(src, t):
            return pltpu.make_async_copy(src, wv.at[(t & 1)], wsem.at[(t & 1)])

        def hid_load(a, q):
            slot = (q & 1)
            return pltpu.make_async_copy(hid.at[a], xa.at[4 + slot], asem.at[slot])

        def issue(t):
            @rarely(t < 16)
            def _():
                m, role = near_step(t)
                j, par = jp(p_of(m))

                @rarely(role == 0)
                def _():
                    w_load(w1_own(j, par, x), t).start()

                @rarely(role == 1)
                def _():
                    w1_part(j, par).wait_recv()
                    w_load(g1.at[0, j, par], t).start()

            @rarely((t >= 16) & (t < 32))
            def _():
                j, par = jp(((t - 16) >> 1))

                @rarely((t & 1) == 1)
                def _():
                    for hf in range(4):
                        w1_fwd(j, par, hf).wait_recv()

                w_load(g1.at[1 + (t & 1), j, par], t).start()

            @rarely((t >= 32) & (t < N_STEPS))
            def _():
                n = ((t - 32) >> 4)
                q = ((t - 32) & 15)
                h = (q & 1)
                p = (q >> 1)
                j, par = jp(p)
                a = 4 * j + 2 * par + h
                same = (j & 1) == c

                @rarely(n == 0)
                def _():
                    @pl.when(blk > 0)
                    def _():
                        hid_dn(a).wait_recv()

                    @pl.when(blk < 3)
                    def _():
                        hid_up(a).wait_recv()

                hid_load(a, q).start()

                own = (p < 4) & same

                @rarely(own)
                def _():
                    w_load(w2_cut(n, par, h, x), t).start()

                @rarely(jnp.logical_not(own))
                def _():
                    @pl.when(p < 4)
                    def _():
                        w2_part(n, par, h).wait_recv()

                    @pl.when((p >= 4) & jnp.logical_not(same))
                    def _():
                        w2_fwd(n, par, h).wait_recv()

                    w_load(g2.at[jnp.where(p < 4, 0, jnp.where(same, 1, 2)), n, par, h], t).start()

        raw_load(0, 2 * osp).wait()
        issue(jnp.int32(0))
        for part_no in range(3):
            raw_load(1, part_no).start()
        swap_end(0, osp)
        pl.semaphore_wait(barrier, 7)

        @pl.when(edge)
        def _():
            halo_copy(0).start()

        each(0, 6, send_w1_x)
        raw_load(0, 2 * sp).wait()
        raw_load(0, 1).wait()
        swap_end(0, sp)
        swap_mid(0)
        x_copy(1).start()
        for m in range(2):
            w1_part(*jp(jnp.int32(m + 2))).start()
        for part_no in range(3):
            raw_load(1, part_no).wait()
        for cc in range(2):
            swap_end(1, cc)
        swap_mid(1)
        halo_wait(0)

        def pass_w1_x(e):
            j, hf = e >> 2, e & 3
            w1_x(j, hf).wait_recv()
            w1_y(j, hf).start()
            w1_fwd(j, sp, hf).start()

        def pass_w1_y(e):
            j, hf = e >> 2, e & 3
            w1_y(j, hf).wait_recv()
            w1_fwd(j, osp, hf).start()

        def pass_w2_x(e):
            n, h = pair(e)
            w2_x(n, h).wait_recv()
            w2_y(n, h).start()
            w2_fwd(n, sp, h).start()

        def pass_w2_y(e):
            n, h = pair(e)
            w2_y(n, h).wait_recv()
            w2_fwd(n, osp, h).start()

        def send_w2_x(e):
            w2_x(*pair(e)).start()

        def events(i):
            @rarely(i < 50)
            def _():
                early_events(i)

        def early_events(i):
            is_odd = odd(i)
            even = jnp.logical_not(is_odd)

            @rarely(i < 16)
            def _():
                @rarely(even)
                def _():
                    @rarely(i < 12)
                    def _():
                        w1_part(*jp(p_of((i >> 1) + 2))).start()

                    @rarely(i == 2)
                    def _():
                        x_copy(1).wait_recv()
                        halo_wait(1)

                    @rarely(i == 10)
                    def _():
                        each(0, 4, pass_w1_y)

                    @rarely(i == 12)
                    def _():
                        each(4, 6, pass_w1_y)

                @rarely(is_odd)
                def _():
                    @rarely(i == 1)
                    def _():
                        @rarely(c != sp)
                        def _():
                            halo_copy(0).start()

                        halo_copy(1).start()

                        @rarely(edge)
                        def _():
                            stage[0, 0:16] = jnp.zeros((16, cols, ni, cb), jnp.bfloat16)
                            zero_rows((rows + 1) * sp).start()

                    @rarely(i == 3)
                    def _():
                        x_copy(2).start()

                    @rarely(i == 5)
                    def _():
                        each(0, 4, pass_w1_x)

                    @rarely(i == 7)
                    def _():
                        each(4, 6, pass_w1_x)

                    @rarely(i == 9)
                    def _():
                        x_copy(3).start()

            @rarely((i >= 13) & (i < 23))
            def _():
                send_w1_x(i - 7)

            @rarely((i >= 16) & (i < 34))
            def _():
                @rarely((i >= 18) & (i < 28))
                def _():
                    pass_w1_x(i - 12)

                @rarely((i >= 20) & (i < 30))
                def _():
                    pass_w1_y(i - 14)

                @rarely(i < 24)
                def _():
                    e = i - 16
                    w2_part((e >> 2), ((e >> 1) & 1), (e & 1)).start()

                @rarely(even)
                def _():
                    @rarely(i == 16)
                    def _():
                        x_copy(2).wait_recv()
                        halo_wait(2)

                    @rarely(i == 30)
                    def _():
                        x_copy(1).wait_send()
                        x_copy(2).wait_send()
                        x_copy(3).wait_send()
                        for far in range(2):
                            halo_copy(far).wait_send()

                    @rarely((i >= 24) & ((i & 3) == 0))
                    def _():
                        send_w2_x(((i - 24) >> 2))

                @rarely(is_odd)
                def _():
                    @rarely(i == 17)
                    def _():
                        x_copy(3).wait_recv()
                        halo_wait(3)

                    @rarely(i >= 19)
                    def _():
                        for h in range(2):
                            hid_store(0, h).wait()

                    @rarely(i >= 27)
                    def _():
                        for d in range(2):
                            j, par = jp(i - 27 + d)
                            for h in range(2):
                                a = 4 * j + 2 * par + h

                                @pl.when(blk > 0)
                                def _():
                                    hid_up(a).start()

                                @pl.when(blk < 3)
                                def _():
                                    hid_dn(a).start()

                    @rarely(i == 31)
                    def _():
                        pass_w2_x(jnp.int32(0))

            @rarely(i >= 34)
            def _():
                @rarely(i == 36)
                def _():
                    send_w2_x(jnp.int32(3))

                @rarely((i < 44) & ((i & 3) == 3))
                def _():
                    pass_w2_x(((i - 31) >> 2))

                @rarely((i >= 37) & ((i & 3) == 1))
                def _():
                    pass_w2_y(((i - 37) >> 2))

        def taps(xs_slot, ws_slot, col, lanes=slice(None)):
            total = None
            for dx in (-1, 0, 1):
                if not 0 <= col + dx < cols:
                    continue
                for dy in range(3):
                    lhs = xa[xs_slot, dy:dy + rows, col + dx].reshape(m_rows, cb)
                    prod = jnp.dot(lhs, wv[ws_slot, dy, dx + 1, :, lanes], preferred_element_type=jnp.float32)
                    total = prod if total is None else total + prod
            return total

        def step(i, carry):
            ph1 = i < 16
            ph3 = i >= 32
            n = jnp.where(ph3, ((i - 32) >> 4), 0)
            q = jnp.where(ph3, ((i - 32) & 15), 0)
            m, role = near_step(i)
            m = jnp.where(ph1, m, ((i - 16) >> 1))
            role = jnp.where(ph1, role, 2 + (i & 1))
            p = jnp.where(ph1, p_of(m), (m & 7))
            p = jnp.where(ph3, 0, p)
            last = jnp.where(ph3, q == 15, role == 3)
            first = jnp.where(ph3, q == 0, role == 0)
            a_slot = jnp.where(ph3, n, (p & 1))
            x_slot = jnp.where(ph3, 4 + (q & 1), role)
            w_slot = (i & 1)

            events(i)
            issue(i + 1)
            w_load(g1.at[0, 0, 0], i).wait()

            @pl.when(ph3)
            def _():
                hid_load(0, q).wait()

            @rarely((i >= 4) & (i < 32))
            def _():
                @pl.when(ph1 & first)
                def _():
                    pltpu.make_async_copy(acc.at[a_slot], part.at[0], pst.at[a_slot]).wait()

                @pl.when((i >= 20) & (role == 2))
                def _():
                    pltpu.make_async_copy(part.at[0], acc.at[a_slot], pld.at[a_slot]).wait()

            @pl.when(jnp.logical_not(last))
            def _():
                for col in range(cols):
                    total = taps(x_slot, w_slot, col)
                    acc[a_slot, col] = total + jnp.where(first, 0.0, acc[a_slot, col])

                @rarely((i < 12) & (role == 1))
                def _():
                    pltpu.make_async_copy(acc.at[a_slot], part.at[p], pst.at[a_slot]).start()

            def finish_hidden():
                @pl.when((i == 17) & edge)
                def _():
                    zero_rows(0).wait()

                j, par = jp(p)
                shift = b1[tile_of(x, j, par)]
                for col in range(cols):
                    val = jnp.maximum(taps(x_slot, w_slot, col) + acc[a_slot, col] + shift, 0.0).astype(jnp.bfloat16)
                    for h in range(2):
                        stage[h, :, col] = val[:, h * cb:(h + 1) * cb].reshape(rows, ni, cb)
                for h in range(2):
                    hid_store(4 * j + 2 * par + h, h).start()

                @pl.when(p < 6)
                def _():
                    pltpu.make_async_copy(part.at[p + 2], acc.at[a_slot], pld.at[a_slot]).start()

            def finish_out():
                @pl.when(n == 1)
                def _():
                    for h in range(2):
                        y_far(h).wait_send()

                def half_step(same, carry):
                    h = jnp.where(same == 1, c, 1 - c)
                    lanes = pl.ds(pl.multiple_of(h * cb, cb), cb)
                    for col in range(cols):
                        total = taps(x_slot, w_slot, col, lanes) + acc[a_slot, col, :, lanes]
                        res = xa[3 - 2 * n - same, 1:rows + 1, col].reshape(m_rows, cb).astype(jnp.float32)
                        stage[h, :, col] = (total + res).astype(jnp.bfloat16).reshape(rows, ni, cb)

                    @pl.when(n == 0)
                    def _():
                        y_far(h).start()

                    @pl.when((n == 1) & (same == 0))
                    def _():
                        y_near().start()

                    return carry

                lax.fori_loop(0, 2, half_step, 0)

                @pl.when(n == 1)
                def _():
                    y_own().start()

            @pl.when(last)
            def _():
                pl.when(jnp.logical_not(ph3))(finish_hidden)
                pl.when(ph3)(finish_out)

            return carry

        lax.fori_loop(0, N_STEPS, step, 0)

        def drain(e, carry):
            hi, lo = pair(e)
            w1_part(hi, lo).wait_send()
            for hf in (lo, lo + 2):
                w1_x(hi, hf).wait_send()
                w1_y(hi, hf).wait_send()
            for hf in range(4):
                w1_fwd(hi, lo, hf).wait_send()
            n, par = e >> 2, (e >> 1) & 1
            w2_part(n, par, lo).wait_send()
            w2_fwd(n, par, lo).wait_send()
            return carry

        lax.fori_loop(0, 8, drain, 0)

        def drain_rows(a, carry):
            @pl.when(blk > 0)
            def _():
                hid_up(a).wait_send()

            @pl.when(blk < 3)
            def _():
                hid_dn(a).wait_send()

            return carry

        lax.fori_loop(0, 16, drain_rows, 0)

        def drain_two(e, carry):
            w2_x(*pair(e)).wait_send()
            w2_y(*pair(e)).wait_send()
            return carry

        lax.fori_loop(0, 4, drain_two, 0)
        for e in range(2):
            remote(stage.at[0], yt.at[0, pl.ds(0, rows)], ys.at[0], yr.at[e], sp, k).wait_recv()
        y_near().wait()
        y_own().wait()

    dma = pltpu.SemaphoreType.DMA
    bf16, f32 = jnp.bfloat16, jnp.float32
    any_space = pl.BlockSpec(memory_space=pl.ANY)
    outs = pl.pallas_call(
        kernel,
        out_shape=[
            jax.ShapeDtypeStruct((2, h_loc, cols, ni, cb), bf16),
            jax.ShapeDtypeStruct((3, 4, 2, 3, 3, cb, tile), bf16),
            jax.ShapeDtypeStruct((3, 2, 2, 2, 3, 3, cb, tile), bf16),
            jax.ShapeDtypeStruct((8, cols, m_rows, tile), f32),
            jax.ShapeDtypeStruct((16, rows + 2, cols, ni, cb), bf16),
        ],
        in_specs=[any_space, any_space, any_space, pl.BlockSpec(memory_space=pltpu.VMEM)],
        out_specs=[any_space] * 5,
        scratch_shapes=[
            pltpu.VMEM((7, rows + 2, cols, ni, cb), bf16),
            pltpu.VMEM((2, cols, m_rows, tile), f32),
            pltpu.VMEM((2, 3, 3, cb, tile), bf16),
            pltpu.VMEM((2, rows, cols, ni, cb), bf16),
            pltpu.VMEM((2, ni, cols, h_loc, cb), bf16),
            pltpu.VMEM((ni * ni, ni * ni), bf16),
            pltpu.VMEM((8, 128), f32),
            *map(dma, SEMS),
        ],
        compiler_params=pltpu.CompilerParams(collective_id=0, has_side_effects=True, vmem_limit_bytes=63 * MIB),
        name="fused_block",
    )(xw, w_one, w_two, bias)
    return outs[0]


def images_major(yt):
    groups, h_loc, cols, ni, cb = yt.shape
    parts = h_loc // ni
    width = cols // 2
    chunks = groups * parts * 2
    assert ni == 16

    def kernel(y, out, y_in, y_out, swap, in_sem, out_sem):
        def place(e):
            block, side = pair(e)
            group, part = lax.div(block, parts), lax.rem(block, parts)
            n0, h0 = pl.multiple_of(ni * group, ni), pl.multiple_of(ni * part, ni)
            return group, n0, h0, width * side

        def load(e):
            group, _, h0, col = place(e)
            cut = (group, pl.ds(h0, ni), pl.ds(col, width))
            return pltpu.make_async_copy(y.at[cut], y_in.at[cut], in_sem.at[e])

        def store(e):
            _, n0, h0, col = place(e)
            cut = (pl.ds(n0, ni), pl.ds(col, width), pl.ds(h0, ni))
            return pltpu.make_async_copy(y_out.at[cut], out.at[cut], out_sem.at[e])

        for e in range(chunks):
            load(jnp.int32(e)).start()
        swap[...] = swap_matrix(ni)

        def chunk(e, carry):
            load(e).wait()
            group, n0, h0, base = place(e)
            for col in range(width):
                rows_in = y_in[group, pl.ds(h0, ni), base + col].reshape(ni * ni, cb)
                res = jnp.dot(swap[...], rows_in, preferred_element_type=jnp.float32)
                y_out[pl.ds(n0, ni), base + col, pl.ds(h0, ni)] = res.astype(jnp.bfloat16).reshape(ni, ni, cb)
            store(e).start()
            return carry

        lax.fori_loop(0, chunks, chunk, 0)
        for e in range(chunks):
            store(jnp.int32(e)).wait()

    dma = pltpu.SemaphoreType.DMA
    out_shape = (groups * ni, cols, h_loc, cb)
    return pl.pallas_call(
        kernel,
        out_shape=jax.ShapeDtypeStruct(out_shape, jnp.bfloat16),
        in_specs=[pl.BlockSpec(memory_space=pl.ANY)],
        out_specs=pl.BlockSpec(memory_space=pl.ANY),
        scratch_shapes=[pltpu.VMEM(yt.shape, jnp.bfloat16), pltpu.VMEM(out_shape, jnp.bfloat16), pltpu.VMEM((ni * ni, ni * ni), jnp.bfloat16),
                        dma((chunks,)), dma((chunks,))],
        compiler_params=pltpu.CompilerParams(vmem_limit_bytes=63 * MIB),
        name="images_major",
    )(yt)


def solution(mesh):
    act_spec = P("dp", "sp", None, "cp")
    kernel_spec = P(None, None, "cp", None)

    def local_block(x_tile, w_one_part, w_two_part, bias_one):
        xw = x_tile.transpose(0, 2, 1, 3)
        yt = fused_block(xw, w_one_part, w_two_part, bias_one.reshape(8, 1, 2 * x_tile.shape[3]))
        return images_major(yt).transpose(0, 2, 1, 3)

    return jax.shard_map(local_block, mesh=mesh, in_specs=(act_spec, kernel_spec, kernel_spec, P()), out_specs=act_spec, check_vma=False)
```

```python
import functools

import jax
import jax.numpy as jnp
from jax import lax
from jax.experimental import pallas as pl
from jax.experimental.pallas import tpu as pltpu
from jax.sharding import PartitionSpec as P

MESH = pl.DeviceIdType.MESH
N_STEPS = 64
MIB = 1024 * 1024
ONE, TWO, THREE, FOUR, ALL = (1,), (2,), (3,), (4,), (2, 16)
GRID, CUBE, HALVES = (2, 2), (2, 2, 2), (4, 2)
QUARTERS, ROWS = (4, 4), (4, 2, 4)
SEMS = (
    TWO, TWO, TWO, TWO, TWO, ONE, (2, 3), THREE, THREE, TWO, FOUR,
    HALVES, HALVES, QUARTERS, QUARTERS, QUARTERS, QUARTERS, ROWS, ROWS,
    CUBE, CUBE, GRID, GRID, GRID, GRID, CUBE, CUBE,
    ALL, ALL, TWO, TWO, ONE, ONE, ONE,
)


def pair(e):
    return e >> 1, e & 1


def each(first, stop, act):
    lax.fori_loop(first, stop, lambda e, carry: (act(e), carry)[1], 0)


def odd(i):
    return (i & 1) == 1


def swap_matrix(n):
    shift = n.bit_length() - 1
    to = lax.broadcasted_iota(jnp.int32, (n * n, n * n), 0)
    frm = lax.broadcasted_iota(jnp.int32, (n * n, n * n), 1)
    hit = ((to >> shift) == (frm & (n - 1))) & ((to & (n - 1)) == (frm >> shift))
    return jnp.where(hit, 1.0, 0.0).astype(jnp.bfloat16)


def fused_block(xw, w_one, w_two, bias):
    images, cols, h_loc, cb = xw.shape
    ni = images // 2
    rows = h_loc // 2
    m_rows = rows * ni
    tile = 2 * cb
    assert ni == 16 and h_loc == 48

    def remote(src, dst, send_sem, recv_sem, sp, cp):
        return pltpu.make_async_remote_copy(src_ref=src, dst_ref=dst, send_sem=send_sem, recv_sem=recv_sem,
                                            device_id={"sp": sp, "cp": cp}, device_id_type=MESH)

    def kernel(xw, w1, w2, b1, yt, g1, g2, part, hid,
               xa, acc, wv, stage, raw, swap, mark,
               wsem, asem, pst, pld, stl, zsem, rsem, xs, xr, hs, hr,
               p1s, p1r, x1s, x1r, y1s, y1r, f1s, f1r,
               p2s, p2r, x2s, x2r, y2s, y2r, f2s, f2r,
               as_, ar, ys, yr, zs, zr, yl):
        sp = lax.axis_index("sp")
        k = lax.axis_index("cp")
        x = (k >> 1)
        c = (k & 1)
        blk = 2 * sp + c
        osp = 1 - sp
        k1 = 2 * x + (1 - c)
        k2 = 2 * (1 - x) + c
        k3 = 2 * (1 - x) + (1 - c)

        def rarely(cond):
            def wrap(body):
                @pl.when(cond)
                def _():
                    mark[...] = jnp.zeros(mark.shape, jnp.float32)
                    body()

            return wrap

        def tile_of(xx, j, par):
            return 4 * ((xx + (j >> 1)) & 1) + 2 * (j & 1) + par

        barrier = pltpu.get_barrier_semaphore()
        for to_sp, to_cp in ((sp, k1), (sp, k2), (sp, k3), (osp, k), (osp, k1)):
            pl.semaphore_signal(barrier, inc=1, device_id={"sp": to_sp, "cp": to_cp}, device_id_type=MESH)

        def raw_load(far, part):
            cut = pl.ds(pl.multiple_of(ni * part, ni), ni)
            group = pl.ds(ni * (1 - x if far else x), ni)
            return pltpu.make_async_copy(xw.at[group, :, cut], raw.at[far, :, :, cut], rsem.at[far, part])

        def block(far, col, part):
            rows_in = raw[far, :, col, pl.ds(pl.multiple_of(ni * part, ni), ni), :].reshape(ni * ni, cb)
            out = jnp.dot(swap[...], rows_in, preferred_element_type=jnp.float32)
            return out.astype(jnp.bfloat16).reshape(ni, ni, cb)

        def slot_of(far, cc):
            return jnp.where(cc == c, 5 if far else 0, 6 if far else 4)

        def swap_end(far, cc):
            for col in range(cols):
                xa[slot_of(far, cc), pl.ds(1 + 8 * cc, ni), col] = block(far, col, 2 * cc)

        def swap_mid(far):
            for col in range(cols):
                mid = block(far, col, 1)
                xa[slot_of(far, 0), 17:26, col] = mid[0:9]
                xa[slot_of(far, 1), 0:9, col] = mid[7:16]

        def x_copy(role):
            cc = c if role == 2 else 1 - c
            cut = pl.ds(1 - cc, rows + 1)
            return remote(xa.at[3 + role, cut], xa.at[role, cut], xs.at[role - 1], xr.at[role - 1], sp,
                          {1: k1, 2: k2, 3: k3}[role])

        def halo_copy(far):
            xx = 1 - x if far else x
            role = 2 * ((x + xx) & 1) + ((c + sp) & 1)
            src = xa.at[slot_of(far, osp), jnp.where(sp == 0, rows, 1)]
            return remote(src, xa.at[role, (rows + 1) * sp], hs.at[far], hr.at[role], osp, 2 * xx + sp)

        piece = cb // 4

        def w1_own(j, par, xx):
            return w1.at[:, :, :, pl.ds(pl.multiple_of(tile_of(xx, j, par) * tile, tile), tile)]

        def w1_part(j, par):
            return remote(w1_own(j, par, x), g1.at[0, j, par], p1s.at[j, par], p1r.at[j, par], sp, k1)

        def w1_x(j, hf):
            cut = pl.ds(pl.multiple_of(hf * piece, piece), piece)
            src = w1.at[:, :, cut, pl.ds(pl.multiple_of(tile_of(1 - x, j, sp) * tile, tile), tile)]
            return remote(src, g1.at[1, j, sp, :, :, cut], x1s.at[j, hf], x1r.at[j, hf], sp, k2)

        def w1_y(j, hf):
            cut = pl.ds(pl.multiple_of(hf * piece, piece), piece)
            ref = g1.at[1, j, sp, :, :, cut]
            return remote(ref, ref, y1s.at[j, hf], y1r.at[j, hf], osp, k)

        def w1_fwd(j, par, hf):
            cut = pl.ds(pl.multiple_of(hf * piece, piece), piece)
            return remote(g1.at[1, j, par, :, :, cut], g1.at[2, j, par, :, :, cut], f1s.at[j, par, hf], f1r.at[j, par, hf], sp, k1)

        def w2_cut(n, par, h, xx):
            row = pl.multiple_of(par * tile + h * cb, cb)
            col = pl.multiple_of(tile * ((1 + xx + n) & 1), tile)
            return w2.at[:, :, pl.ds(row, cb), pl.ds(col, tile)]

        def w2_part(n, par, h):
            return remote(w2_cut(n, par, h, x), g2.at[0, n, par, h], p2s.at[n, par, h], p2r.at[n, par, h], sp, k1)

        def w2_x(n, h):
            return remote(w2_cut(n, sp, h, 1 - x), g2.at[1, n, sp, h], x2s.at[n, h], x2r.at[n, h], sp, k2)

        def w2_y(n, h):
            ref = g2.at[1, n, sp, h]
            return remote(ref, ref, y2s.at[n, h], y2r.at[n, h], osp, k)

        def w2_fwd(n, par, h):
            return remote(g2.at[1, n, par, h], g2.at[2, n, par, h], f2s.at[n, par, h], f2r.at[n, par, h], sp, k1)

        up_blk = lax.max(blk - 1, 0)
        dn_blk = lax.min(blk + 1, 3)

        def hid_up(a):
            return remote(hid.at[a, 1], hid.at[a, rows + 1], as_.at[0, a], ar.at[1, a], (up_blk >> 1), 2 * x + (up_blk & 1))

        def hid_dn(a):
            return remote(hid.at[a, rows], hid.at[a, 0], as_.at[1, a], ar.at[0, a], (dn_blk >> 1), 2 * x + (dn_blk & 1))

        def hid_store(a, h):
            return pltpu.make_async_copy(stage.at[h], hid.at[a, pl.ds(1, rows)], stl.at[h])

        y_rows = pl.ds(rows * c, rows)

        def y_far(h):
            return remote(stage.at[h], yt.at[x, y_rows], ys.at[h], yr.at[((h + c) & 1)], sp, 2 * (1 - x) + h)

        def y_near():
            return remote(stage.at[1 - c], yt.at[x, y_rows], zs.at[0], zr.at[0], sp, k1)

        def y_own():
            return pltpu.make_async_copy(stage.at[c], yt.at[x, y_rows], yl.at[0])

        def zero_rows(row):
            return pltpu.make_async_copy(stage.at[0, pl.ds(0, 16)], hid.at[:, row], zsem.at[0])

        def p_of(m):
            return (m + 2) & 7

        def jp(p):
            return p >> 1, (sp + p) & 1

        def send_w1_x(e):
            w1_x(e >> 2, e & 3).start()

        def near_step(i):
            return 2 * (i >> 2) + (i & 1), (i & 2) >> 1

        def halo_wait(role):
            @pl.when(c != sp)
            def _():
                remote(xa.at[0, 0], xa.at[role, 0], hs.at[0], hr.at[role], osp, k).wait_recv()

        for part_no in (2 * osp, 2 * sp, 1):
            raw_load(0, part_no).start()
        swap[...] = swap_matrix(ni)
        edge = c == sp

        @pl.when(edge)
        def _():
            xa[0:4, (rows + 1) * sp] = jnp.zeros((4, cols, ni, cb), jnp.bfloat16)

        def w_load(src, t):
            return pltpu.make_async_copy(src, wv.at[(t & 1)], wsem.at[(t & 1)])

        def hid_load(a, q):
            slot = (q & 1)
            return pltpu.make_async_copy(hid.at[a], xa.at[4 + slot], asem.at[slot])

        def issue(t):
            @rarely(t < 16)
            def _():
                m, role = near_step(t)
                j, par = jp(p_of(m))

                @rarely(role == 0)
                def _():
                    w_load(w1_own(j, par, x), t).start()

                @rarely(role == 1)
                def _():
                    w1_part(j, par).wait_recv()
                    w_load(g1.at[0, j, par], t).start()

            @rarely((t >= 16) & (t < 32))
            def _():
                j, par = jp(((t - 16) >> 1))

                @rarely((t & 1) == 1)
                def _():
                    for hf in range(4):
                        w1_fwd(j, par, hf).wait_recv()

                w_load(g1.at[1 + (t & 1), j, par], t).start()

            @rarely((t >= 32) & (t < N_STEPS))
            def _():
                n = ((t - 32) >> 4)
                q = ((t - 32) & 15)
                h = (q & 1)
                p = (q >> 1)
                j, par = jp(p)
                a = 4 * j + 2 * par + h
                same = (j & 1) == c

                @rarely(n == 0)
                def _():
                    @pl.when(blk > 0)
                    def _():
                        hid_dn(a).wait_recv()

                    @pl.when(blk < 3)
                    def _():
                        hid_up(a).wait_recv()

                hid_load(a, q).start()

                own = (p < 4) & same

                @rarely(own)
                def _():
                    w_load(w2_cut(n, par, h, x), t).start()

                @rarely(jnp.logical_not(own))
                def _():
                    @pl.when(p < 4)
                    def _():
                        w2_part(n, par, h).wait_recv()

                    @pl.when((p >= 4) & jnp.logical_not(same))
                    def _():
                        w2_fwd(n, par, h).wait_recv()

                    w_load(g2.at[jnp.where(p < 4, 0, jnp.where(same, 1, 2)), n, par, h], t).start()

        raw_load(0, 2 * osp).wait()
        issue(jnp.int32(0))
        for part_no in range(3):
            raw_load(1, part_no).start()
        swap_end(0, osp)
        pl.semaphore_wait(barrier, 5)

        @pl.when(edge)
        def _():
            halo_copy(0).start()

        each(0, 6, send_w1_x)
        raw_load(0, 2 * sp).wait()
        raw_load(0, 1).wait()
        swap_end(0, sp)
        swap_mid(0)
        x_copy(1).start()
        for m in range(2):
            w1_part(*jp(jnp.int32(m + 2))).start()
        for part_no in range(3):
            raw_load(1, part_no).wait()
        for cc in range(2):
            swap_end(1, cc)
        swap_mid(1)
        halo_wait(0)

        def pass_w1_x(e):
            j, hf = e >> 2, e & 3
            w1_x(j, hf).wait_recv()
            w1_y(j, hf).start()
            w1_fwd(j, sp, hf).start()

        def pass_w1_y(e):
            j, hf = e >> 2, e & 3
            w1_y(j, hf).wait_recv()
            w1_fwd(j, osp, hf).start()

        def pass_w2_x(e):
            n, h = pair(e)
            w2_x(n, h).wait_recv()
            w2_y(n, h).start()
            w2_fwd(n, sp, h).start()

        def pass_w2_y(e):
            n, h = pair(e)
            w2_y(n, h).wait_recv()
            w2_fwd(n, osp, h).start()

        def send_w2_x(e):
            w2_x(*pair(e)).start()

        def events(i):
            @rarely(i < 50)
            def _():
                early_events(i)

        def early_events(i):
            is_odd = odd(i)
            even = jnp.logical_not(is_odd)

            @rarely(i < 16)
            def _():
                @rarely(even)
                def _():
                    @rarely(i < 12)
                    def _():
                        w1_part(*jp(p_of((i >> 1) + 2))).start()

                    @rarely(i == 2)
                    def _():
                        x_copy(1).wait_recv()
                        halo_wait(1)

                    @rarely(i == 10)
                    def _():
                        each(0, 4, pass_w1_y)

                    @rarely(i == 12)
                    def _():
                        each(4, 6, pass_w1_y)

                @rarely(is_odd)
                def _():
                    @rarely(i == 1)
                    def _():
                        @rarely(c != sp)
                        def _():
                            halo_copy(0).start()

                        @rarely(edge)
                        def _():
                            stage[0, 0:16] = jnp.zeros((16, cols, ni, cb), jnp.bfloat16)
                            zero_rows((rows + 1) * sp).start()

                    @rarely(i == 3)
                    def _():
                        x_copy(2).start()

                    @rarely(i == 5)
                    def _():
                        each(0, 4, pass_w1_x)

                    @rarely(i == 7)
                    def _():
                        each(4, 6, pass_w1_x)
                        halo_copy(1).start()

                    @rarely(i == 9)
                    def _():
                        x_copy(3).start()

            @rarely((i >= 13) & (i < 23))
            def _():
                send_w1_x(i - 7)

            @rarely((i >= 16) & (i < 34))
            def _():
                @rarely((i >= 18) & (i < 28))
                def _():
                    pass_w1_x(i - 12)

                @rarely((i >= 20) & (i < 30))
                def _():
                    pass_w1_y(i - 14)

                @rarely(i < 24)
                def _():
                    e = i - 16
                    w2_part((e >> 2), ((e >> 1) & 1), (e & 1)).start()

                @rarely(even)
                def _():
                    @rarely(i == 16)
                    def _():
                        x_copy(2).wait_recv()
                        halo_wait(2)

                    @rarely(i == 30)
                    def _():
                        x_copy(1).wait_send()
                        x_copy(2).wait_send()
                        x_copy(3).wait_send()
                        for far in range(2):
                            halo_copy(far).wait_send()

                    @rarely((i >= 24) & ((i & 3) == 0))
                    def _():
                        send_w2_x(((i - 24) >> 2))

                @rarely(is_odd)
                def _():
                    @rarely(i == 17)
                    def _():
                        x_copy(3).wait_recv()
                        halo_wait(3)

                    @rarely(i >= 19)
                    def _():
                        for h in range(2):
                            hid_store(0, h).wait()

                    @rarely(i >= 27)
                    def _():
                        for d in range(2):
                            j, par = jp(i - 27 + d)
                            for h in range(2):
                                a = 4 * j + 2 * par + h

                                @pl.when(blk > 0)
                                def _():
                                    hid_up(a).start()

                                @pl.when(blk < 3)
                                def _():
                                    hid_dn(a).start()

                    @rarely(i == 31)
                    def _():
                        pass_w2_x(jnp.int32(0))

            @rarely(i >= 34)
            def _():
                @rarely(i == 36)
                def _():
                    send_w2_x(jnp.int32(3))

                @rarely((i < 44) & ((i & 3) == 3))
                def _():
                    pass_w2_x(((i - 31) >> 2))

                @rarely((i >= 37) & ((i & 3) == 1))
                def _():
                    pass_w2_y(((i - 37) >> 2))

        def taps(xs_slot, ws_slot, col, lanes=slice(None)):
            total = None
            for dx in (-1, 0, 1):
                if not 0 <= col + dx < cols:
                    continue
                for dy in range(3):
                    lhs = xa[xs_slot, dy:dy + rows, col + dx].reshape(m_rows, cb)
                    prod = jnp.dot(lhs, wv[ws_slot, dy, dx + 1, :, lanes], preferred_element_type=jnp.float32)
                    total = prod if total is None else total + prod
            return total

        def step(i, carry):
            ph1 = i < 16
            ph3 = i >= 32
            n = jnp.where(ph3, ((i - 32) >> 4), 0)
            q = jnp.where(ph3, ((i - 32) & 15), 0)
            m, role = near_step(i)
            m = jnp.where(ph1, m, ((i - 16) >> 1))
            role = jnp.where(ph1, role, 2 + (i & 1))
            p = jnp.where(ph1, p_of(m), (m & 7))
            p = jnp.where(ph3, 0, p)
            last = jnp.where(ph3, q == 15, role == 3)
            first = jnp.where(ph3, q == 0, role == 0)
            a_slot = jnp.where(ph3, n, (p & 1))
            x_slot = jnp.where(ph3, 4 + (q & 1), role)
            w_slot = (i & 1)

            events(i)
            issue(i + 1)
            w_load(g1.at[0, 0, 0], i).wait()

            @pl.when(ph3)
            def _():
                hid_load(0, q).wait()

            @rarely((i >= 4) & (i < 32))
            def _():
                @pl.when(ph1 & first)
                def _():
                    pltpu.make_async_copy(acc.at[a_slot], part.at[0], pst.at[a_slot]).wait()

                @pl.when((i >= 20) & (role == 2))
                def _():
                    pltpu.make_async_copy(part.at[0], acc.at[a_slot], pld.at[a_slot]).wait()

            @pl.when(jnp.logical_not(last))
            def _():
                for col in range(cols):
                    total = taps(x_slot, w_slot, col)
                    acc[a_slot, col] = total + jnp.where(first, 0.0, acc[a_slot, col])

                @rarely((i < 12) & (role == 1))
                def _():
                    pltpu.make_async_copy(acc.at[a_slot], part.at[p], pst.at[a_slot]).start()

            def finish_hidden():
                @pl.when((i == 17) & edge)
                def _():
                    zero_rows(0).wait()

                j, par = jp(p)
                shift = b1[tile_of(x, j, par)]
                for col in range(cols):
                    val = jnp.maximum(taps(x_slot, w_slot, col) + acc[a_slot, col] + shift, 0.0).astype(jnp.bfloat16)
                    for h in range(2):
                        stage[h, :, col] = val[:, h * cb:(h + 1) * cb].reshape(rows, ni, cb)
                for h in range(2):
                    hid_store(4 * j + 2 * par + h, h).start()

                @pl.when(p < 6)
                def _():
                    pltpu.make_async_copy(part.at[p + 2], acc.at[a_slot], pld.at[a_slot]).start()

            def finish_out():
                @pl.when(n == 1)
                def _():
                    for h in range(2):
                        y_far(h).wait_send()

                def half_step(same, carry):
                    h = jnp.where(same == 1, c, 1 - c)
                    lanes = pl.ds(pl.multiple_of(h * cb, cb), cb)
                    for col in range(cols):
                        total = taps(x_slot, w_slot, col, lanes) + acc[a_slot, col, :, lanes]
                        res = xa[3 - 2 * n - same, 1:rows + 1, col].reshape(m_rows, cb).astype(jnp.float32)
                        stage[h, :, col] = (total + res).astype(jnp.bfloat16).reshape(rows, ni, cb)

                    @pl.when(n == 0)
                    def _():
                        y_far(h).start()

                    @pl.when((n == 1) & (same == 0))
                    def _():
                        y_near().start()

                    return carry

                lax.fori_loop(0, 2, half_step, 0)

                @pl.when(n == 1)
                def _():
                    y_own().start()

            @pl.when(last)
            def _():
                pl.when(jnp.logical_not(ph3))(finish_hidden)
                pl.when(ph3)(finish_out)

            return carry

        lax.fori_loop(0, N_STEPS, step, 0)

        def drain(e, carry):
            hi, lo = pair(e)
            w1_part(hi, lo).wait_send()
            for hf in (lo, lo + 2):
                w1_x(hi, hf).wait_send()
                w1_y(hi, hf).wait_send()
            for hf in range(4):
                w1_fwd(hi, lo, hf).wait_send()
            n, par = e >> 2, (e >> 1) & 1
            w2_part(n, par, lo).wait_send()
            w2_fwd(n, par, lo).wait_send()
            return carry

        lax.fori_loop(0, 8, drain, 0)

        def drain_rows(a, carry):
            @pl.when(blk > 0)
            def _():
                hid_up(a).wait_send()

            @pl.when(blk < 3)
            def _():
                hid_dn(a).wait_send()

            return carry

        lax.fori_loop(0, 16, drain_rows, 0)

        def drain_two(e, carry):
            w2_x(*pair(e)).wait_send()
            w2_y(*pair(e)).wait_send()
            return carry

        lax.fori_loop(0, 4, drain_two, 0)
        for e in range(2):
            remote(stage.at[0], yt.at[0, pl.ds(0, rows)], ys.at[0], yr.at[e], sp, k).wait_recv()
        y_near().wait()
        y_own().wait()

    dma = pltpu.SemaphoreType.DMA
    bf16, f32 = jnp.bfloat16, jnp.float32
    any_space = pl.BlockSpec(memory_space=pl.ANY)
    outs = pl.pallas_call(
        kernel,
        out_shape=[
            jax.ShapeDtypeStruct((2, h_loc, cols, ni, cb), bf16),
            jax.ShapeDtypeStruct((3, 4, 2, 3, 3, cb, tile), bf16),
            jax.ShapeDtypeStruct((3, 2, 2, 2, 3, 3, cb, tile), bf16),
            jax.ShapeDtypeStruct((8, cols, m_rows, tile), f32),
            jax.ShapeDtypeStruct((16, rows + 2, cols, ni, cb), bf16),
        ],
        in_specs=[any_space, any_space, any_space, pl.BlockSpec(memory_space=pltpu.VMEM)],
        out_specs=[any_space] * 5,
        scratch_shapes=[
            pltpu.VMEM((7, rows + 2, cols, ni, cb), bf16),
            pltpu.VMEM((2, cols, m_rows, tile), f32),
            pltpu.VMEM((2, 3, 3, cb, tile), bf16),
            pltpu.VMEM((2, rows, cols, ni, cb), bf16),
            pltpu.VMEM((2, ni, cols, h_loc, cb), bf16),
            pltpu.VMEM((ni * ni, ni * ni), bf16),
            pltpu.VMEM((8, 128), f32),
            *map(dma, SEMS),
        ],
        compiler_params=pltpu.CompilerParams(collective_id=0, has_side_effects=True, vmem_limit_bytes=63 * MIB),
        name="fused_block",
    )(xw, w_one, w_two, bias)
    return outs[0]


def images_major(yt):
    groups, h_loc, cols, ni, cb = yt.shape
    parts = h_loc // ni
    width = cols // 2
    chunks = groups * parts * 2
    assert ni == 16

    def kernel(y, out, y_in, y_out, swap, in_sem, out_sem):
        def place(e):
            block, side = pair(e)
            group, part = lax.div(block, parts), lax.rem(block, parts)
            n0, h0 = pl.multiple_of(ni * group, ni), pl.multiple_of(ni * part, ni)
            return group, n0, h0, width * side

        def load(e):
            group, _, h0, col = place(e)
            cut = (group, pl.ds(h0, ni), pl.ds(col, width))
            return pltpu.make_async_copy(y.at[cut], y_in.at[cut], in_sem.at[e])

        def store(e):
            _, n0, h0, col = place(e)
            cut = (pl.ds(n0, ni), pl.ds(col, width), pl.ds(h0, ni))
            return pltpu.make_async_copy(y_out.at[cut], out.at[cut], out_sem.at[e])

        for e in range(chunks):
            load(jnp.int32(e)).start()
        swap[...] = swap_matrix(ni)

        def chunk(e, carry):
            load(e).wait()
            group, n0, h0, base = place(e)
            for col in range(width):
                rows_in = y_in[group, pl.ds(h0, ni), base + col].reshape(ni * ni, cb)
                res = jnp.dot(swap[...], rows_in, preferred_element_type=jnp.float32)
                y_out[pl.ds(n0, ni), base + col, pl.ds(h0, ni)] = res.astype(jnp.bfloat16).reshape(ni, ni, cb)
            store(e).start()
            return carry

        lax.fori_loop(0, chunks, chunk, 0)
        for e in range(chunks):
            store(jnp.int32(e)).wait()

    dma = pltpu.SemaphoreType.DMA
    out_shape = (groups * ni, cols, h_loc, cb)
    return pl.pallas_call(
        kernel,
        out_shape=jax.ShapeDtypeStruct(out_shape, jnp.bfloat16),
        in_specs=[pl.BlockSpec(memory_space=pl.ANY)],
        out_specs=pl.BlockSpec(memory_space=pl.ANY),
        scratch_shapes=[pltpu.VMEM(yt.shape, jnp.bfloat16), pltpu.VMEM(out_shape, jnp.bfloat16), pltpu.VMEM((ni * ni, ni * ni), jnp.bfloat16),
                        dma((chunks,)), dma((chunks,))],
        compiler_params=pltpu.CompilerParams(vmem_limit_bytes=63 * MIB),
        name="images_major",
    )(yt)


def solution(mesh):
    act_spec = P("dp", "sp", None, "cp")
    kernel_spec = P(None, None, "cp", None)

    def local_block(x_tile, w_one_part, w_two_part, bias_one):
        xw = x_tile.transpose(0, 2, 1, 3)
        yt = fused_block(xw, w_one_part, w_two_part, bias_one.reshape(8, 1, 2 * x_tile.shape[3]))
        return images_major(yt).transpose(0, 2, 1, 3)

    return jax.shard_map(local_block, mesh=mesh, in_specs=(act_spec, kernel_spec, kernel_spec, P()), out_specs=act_spec, check_vma=False)
```

```python
import functools

import jax
import jax.numpy as jnp
from jax import lax
from jax.experimental import pallas as pl
from jax.experimental.pallas import tpu as pltpu
from jax.sharding import PartitionSpec as P

MESH = pl.DeviceIdType.MESH
N_STEPS = 64
MIB = 1024 * 1024
ONE, TWO, THREE, FOUR, ALL = (1,), (2,), (3,), (4,), (2, 16)
GRID, CUBE, HALVES = (2, 2), (2, 2, 2), (4, 2)
QUARTERS, ROWS = (4, 4), (4, 2, 4)
SEMS = (
    TWO, TWO, TWO, TWO, TWO, ONE, (2, 3), THREE, THREE, TWO, FOUR,
    HALVES, HALVES, QUARTERS, QUARTERS, QUARTERS, QUARTERS, ROWS, ROWS,
    CUBE, CUBE, GRID, GRID, GRID, GRID, CUBE, CUBE,
    ALL, ALL, TWO, TWO, ONE, ONE, ONE,
)


def pair(e):
    return e >> 1, e & 1


def each(first, stop, act):
    lax.fori_loop(first, stop, lambda e, carry: (act(e), carry)[1], 0)


def odd(i):
    return (i & 1) == 1


def swap_matrix(n):
    shift = n.bit_length() - 1
    to = lax.broadcasted_iota(jnp.int32, (n * n, n * n), 0)
    frm = lax.broadcasted_iota(jnp.int32, (n * n, n * n), 1)
    hit = ((to >> shift) == (frm & (n - 1))) & ((to & (n - 1)) == (frm >> shift))
    return jnp.where(hit, 1.0, 0.0).astype(jnp.bfloat16)


def fused_block(xw, w_one, w_two, bias):
    images, cols, h_loc, cb = xw.shape
    ni = images // 2
    rows = h_loc // 2
    m_rows = rows * ni
    tile = 2 * cb
    assert ni == 16 and h_loc == 48

    def remote(src, dst, send_sem, recv_sem, sp, cp):
        return pltpu.make_async_remote_copy(src_ref=src, dst_ref=dst, send_sem=send_sem, recv_sem=recv_sem,
                                            device_id={"sp": sp, "cp": cp}, device_id_type=MESH)

    def kernel(xw, w1, w2, b1, yt, g1, g2, part, hid,
               xa, acc, wv, stage, raw, swap, mark, shifts, bsem,
               wsem, asem, pst, pld, stl, zsem, rsem, xs, xr, hs, hr,
               p1s, p1r, x1s, x1r, y1s, y1r, f1s, f1r,
               p2s, p2r, x2s, x2r, y2s, y2r, f2s, f2r,
               as_, ar, ys, yr, zs, zr, yl):
        sp = lax.axis_index("sp")
        k = lax.axis_index("cp")
        x = (k >> 1)
        c = (k & 1)
        blk = 2 * sp + c
        osp = 1 - sp
        k1 = 2 * x + (1 - c)
        k2 = 2 * (1 - x) + c
        k3 = 2 * (1 - x) + (1 - c)

        def rarely(cond):
            def wrap(body):
                @pl.when(cond)
                def _():
                    mark[...] = jnp.zeros(mark.shape, jnp.float32)
                    body()

            return wrap

        def tile_of(xx, j, par):
            return 4 * ((xx + (j >> 1)) & 1) + 2 * (j & 1) + par

        barrier = pltpu.get_barrier_semaphore()
        for to_sp, to_cp in ((sp, k1), (sp, k2), (sp, k3), (osp, k), (osp, k1)):
            pl.semaphore_signal(barrier, inc=1, device_id={"sp": to_sp, "cp": to_cp}, device_id_type=MESH)

        def raw_load(far, part):
            cut = pl.ds(pl.multiple_of(ni * part, ni), ni)
            group = pl.ds(ni * (1 - x if far else x), ni)
            return pltpu.make_async_copy(xw.at[group, :, cut], raw.at[far, :, :, cut], rsem.at[far, part])

        def block(far, col, part):
            rows_in = raw[far, :, col, pl.ds(pl.multiple_of(ni * part, ni), ni), :].reshape(ni * ni, cb)
            out = jnp.dot(swap[...], rows_in, preferred_element_type=jnp.float32)
            return out.astype(jnp.bfloat16).reshape(ni, ni, cb)

        def slot_of(far, cc):
            return jnp.where(cc == c, 5 if far else 0, 6 if far else 4)

        def swap_end(far, cc):
            for col in range(cols):
                xa[slot_of(far, cc), pl.ds(1 + 8 * cc, ni), col] = block(far, col, 2 * cc)

        def swap_mid(far):
            for col in range(cols):
                mid = block(far, col, 1)
                xa[slot_of(far, 0), 17:26, col] = mid[0:9]
                xa[slot_of(far, 1), 0:9, col] = mid[7:16]

        def x_copy(role):
            cc = c if role == 2 else 1 - c
            cut = pl.ds(1 - cc, rows + 1)
            return remote(xa.at[3 + role, cut], xa.at[role, cut], xs.at[role - 1], xr.at[role - 1], sp,
                          {1: k1, 2: k2, 3: k3}[role])

        def halo_copy(far):
            xx = 1 - x if far else x
            role = 2 * ((x + xx) & 1) + ((c + sp) & 1)
            src = xa.at[slot_of(far, osp), jnp.where(sp == 0, rows, 1)]
            return remote(src, xa.at[role, (rows + 1) * sp], hs.at[far], hr.at[role], osp, 2 * xx + sp)

        def bias_load():
            return pltpu.make_async_copy(b1, shifts, bsem.at[0])

        piece = cb // 4

        def w1_own(j, par, xx):
            return w1.at[:, :, :, pl.ds(pl.multiple_of(tile_of(xx, j, par) * tile, tile), tile)]

        def w1_part(j, par):
            return remote(w1_own(j, par, x), g1.at[0, j, par], p1s.at[j, par], p1r.at[j, par], sp, k1)

        def w1_x(j, hf):
            cut = pl.ds(pl.multiple_of(hf * piece, piece), piece)
            src = w1.at[:, :, cut, pl.ds(pl.multiple_of(tile_of(1 - x, j, sp) * tile, tile), tile)]
            return remote(src, g1.at[1, j, sp, :, :, cut], x1s.at[j, hf], x1r.at[j, hf], sp, k2)

        def w1_y(j, hf):
            cut = pl.ds(pl.multiple_of(hf * piece, piece), piece)
            ref = g1.at[1, j, sp, :, :, cut]
            return remote(ref, ref, y1s.at[j, hf], y1r.at[j, hf], osp, k)

        def w1_fwd(j, par, hf):
            cut = pl.ds(pl.multiple_of(hf * piece, piece), piece)
            return remote(g1.at[1, j, par, :, :, cut], g1.at[2, j, par, :, :, cut], f1s.at[j, par, hf], f1r.at[j, par, hf], sp, k1)

        def w2_cut(n, par, h, xx):
            row = pl.multiple_of(par * tile + h * cb, cb)
            col = pl.multiple_of(tile * ((1 + xx + n) & 1), tile)
            return w2.at[:, :, pl.ds(row, cb), pl.ds(col, tile)]

        def w2_part(n, par, h):
            return remote(w2_cut(n, par, h, x), g2.at[0, n, par, h], p2s.at[n, par, h], p2r.at[n, par, h], sp, k1)

        def w2_x(n, h):
            return remote(w2_cut(n, sp, h, 1 - x), g2.at[1, n, sp, h], x2s.at[n, h], x2r.at[n, h], sp, k2)

        def w2_y(n, h):
            ref = g2.at[1, n, sp, h]
            return remote(ref, ref, y2s.at[n, h], y2r.at[n, h], osp, k)

        def w2_fwd(n, par, h):
            return remote(g2.at[1, n, par, h], g2.at[2, n, par, h], f2s.at[n, par, h], f2r.at[n, par, h], sp, k1)

        up_blk = lax.max(blk - 1, 0)
        dn_blk = lax.min(blk + 1, 3)

        def hid_up(a):
            return remote(hid.at[a, 1], hid.at[a, rows + 1], as_.at[0, a], ar.at[1, a], (up_blk >> 1), 2 * x + (up_blk & 1))

        def hid_dn(a):
            return remote(hid.at[a, rows], hid.at[a, 0], as_.at[1, a], ar.at[0, a], (dn_blk >> 1), 2 * x + (dn_blk & 1))

        def hid_store(a, h):
            return pltpu.make_async_copy(stage.at[h], hid.at[a, pl.ds(1, rows)], stl.at[h])

        y_rows = pl.ds(rows * c, rows)

        def y_far(h):
            return remote(stage.at[h], yt.at[x, y_rows], ys.at[h], yr.at[((h + c) & 1)], sp, 2 * (1 - x) + h)

        def y_near():
            return remote(stage.at[1 - c], yt.at[x, y_rows], zs.at[0], zr.at[0], sp, k1)

        def y_own():
            return pltpu.make_async_copy(stage.at[c], yt.at[x, y_rows], yl.at[0])

        def zero_rows(row):
            return pltpu.make_async_copy(stage.at[0, pl.ds(0, 16)], hid.at[:, row], zsem.at[0])

        def p_of(m):
            return (m + 2) & 7

        def jp(p):
            return p >> 1, (sp + p) & 1

        def send_w1_x(e):
            w1_x(e >> 2, e & 3).start()

        def near_step(i):
            return 2 * (i >> 2) + (i & 1), (i & 2) >> 1

        def halo_wait(role):
            @pl.when(c != sp)
            def _():
                remote(xa.at[0, 0], xa.at[role, 0], hs.at[0], hr.at[role], osp, k).wait_recv()

        for part_no in (2 * osp, 2 * sp, 1):
            raw_load(0, part_no).start()
        swap[...] = swap_matrix(ni)
        edge = c == sp

        @pl.when(edge)
        def _():
            xa[0:4, (rows + 1) * sp] = jnp.zeros((4, cols, ni, cb), jnp.bfloat16)

        def w_load(src, t):
            return pltpu.make_async_copy(src, wv.at[(t & 1)], wsem.at[(t & 1)])

        def hid_load(a, q):
            slot = (q & 1)
            return pltpu.make_async_copy(hid.at[a], xa.at[4 + slot], asem.at[slot])

        def issue(t):
            @rarely(t < 16)
            def _():
                m, role = near_step(t)
                j, par = jp(p_of(m))

                @rarely(role == 0)
                def _():
                    w_load(w1_own(j, par, x), t).start()

                @rarely(role == 1)
                def _():
                    w1_part(j, par).wait_recv()
                    w_load(g1.at[0, j, par], t).start()

            @rarely((t >= 16) & (t < 32))
            def _():
                j, par = jp(((t - 16) >> 1))

                @rarely((t & 1) == 1)
                def _():
                    for hf in range(4):
                        w1_fwd(j, par, hf).wait_recv()

                w_load(g1.at[1 + (t & 1), j, par], t).start()

            @rarely((t >= 32) & (t < N_STEPS))
            def _():
                n = ((t - 32) >> 4)
                q = ((t - 32) & 15)
                h = (q & 1)
                p = (q >> 1)
                j, par = jp(p)
                a = 4 * j + 2 * par + h
                same = (j & 1) == c

                @rarely(n == 0)
                def _():
                    @pl.when(blk > 0)
                    def _():
                        hid_dn(a).wait_recv()

                    @pl.when(blk < 3)
                    def _():
                        hid_up(a).wait_recv()

                hid_load(a, q).start()

                own = (p < 4) & same

                @rarely(own)
                def _():
                    w_load(w2_cut(n, par, h, x), t).start()

                @rarely(jnp.logical_not(own))
                def _():
                    @pl.when(p < 4)
                    def _():
                        w2_part(n, par, h).wait_recv()

                    @pl.when((p >= 4) & jnp.logical_not(same))
                    def _():
                        w2_fwd(n, par, h).wait_recv()

                    w_load(g2.at[jnp.where(p < 4, 0, jnp.where(same, 1, 2)), n, par, h], t).start()

        raw_load(0, 2 * osp).wait()
        issue(jnp.int32(0))
        for part_no in range(3):
            raw_load(1, part_no).start()
        bias_load().start()
        swap_end(0, osp)
        pl.semaphore_wait(barrier, 5)

        @pl.when(edge)
        def _():
            halo_copy(0).start()

        each(0, 6, send_w1_x)
        raw_load(0, 2 * sp).wait()
        raw_load(0, 1).wait()
        swap_end(0, sp)
        swap_mid(0)
        x_copy(1).start()
        for m in range(2):
            w1_part(*jp(jnp.int32(m + 2))).start()
        for part_no in range(3):
            raw_load(1, part_no).wait()
        for cc in range(2):
            swap_end(1, cc)
        swap_mid(1)
        halo_wait(0)

        def pass_w1_x(e):
            j, hf = e >> 2, e & 3
            w1_x(j, hf).wait_recv()
            w1_y(j, hf).start()
            w1_fwd(j, sp, hf).start()

        def pass_w1_y(e):
            j, hf = e >> 2, e & 3
            w1_y(j, hf).wait_recv()
            w1_fwd(j, osp, hf).start()

        def pass_w2_x(e):
            n, h = pair(e)
            w2_x(n, h).wait_recv()
            w2_y(n, h).start()
            w2_fwd(n, sp, h).start()

        def pass_w2_y(e):
            n, h = pair(e)
            w2_y(n, h).wait_recv()
            w2_fwd(n, osp, h).start()

        def send_w2_x(e):
            w2_x(*pair(e)).start()

        def events(i):
            @rarely(i < 50)
            def _():
                early_events(i)

        def early_events(i):
            is_odd = odd(i)
            even = jnp.logical_not(is_odd)

            @rarely(i < 16)
            def _():
                @rarely(even)
                def _():
                    @rarely(i < 12)
                    def _():
                        w1_part(*jp(p_of((i >> 1) + 2))).start()

                    @rarely(i == 2)
                    def _():
                        x_copy(1).wait_recv()
                        halo_wait(1)

                    @rarely(i == 10)
                    def _():
                        each(0, 4, pass_w1_y)

                    @rarely(i == 12)
                    def _():
                        each(4, 6, pass_w1_y)

                @rarely(is_odd)
                def _():
                    @rarely(i == 1)
                    def _():
                        @rarely(c != sp)
                        def _():
                            halo_copy(0).start()

                        @rarely(edge)
                        def _():
                            stage[0, 0:16] = jnp.zeros((16, cols, ni, cb), jnp.bfloat16)
                            zero_rows((rows + 1) * sp).start()

                    @rarely(i == 3)
                    def _():
                        x_copy(2).start()

                    @rarely(i == 5)
                    def _():
                        each(0, 4, pass_w1_x)

                    @rarely(i == 7)
                    def _():
                        each(4, 6, pass_w1_x)
                        halo_copy(1).start()

                    @rarely(i == 9)
                    def _():
                        x_copy(3).start()

            @rarely((i >= 13) & (i < 23))
            def _():
                send_w1_x(i - 7)

            @rarely((i >= 16) & (i < 34))
            def _():
                @rarely((i >= 18) & (i < 28))
                def _():
                    pass_w1_x(i - 12)

                @rarely((i >= 20) & (i < 30))
                def _():
                    pass_w1_y(i - 14)

                @rarely(i < 24)
                def _():
                    e = i - 16
                    w2_part((e >> 2), ((e >> 1) & 1), (e & 1)).start()

                @rarely(even)
                def _():
                    @rarely(i == 16)
                    def _():
                        bias_load().wait()
                        x_copy(2).wait_recv()
                        halo_wait(2)

                    @rarely(i == 30)
                    def _():
                        x_copy(1).wait_send()
                        x_copy(2).wait_send()
                        x_copy(3).wait_send()
                        for far in range(2):
                            halo_copy(far).wait_send()

                    @rarely((i >= 24) & ((i & 3) == 0))
                    def _():
                        send_w2_x(((i - 24) >> 2))

                @rarely(is_odd)
                def _():
                    @rarely(i == 17)
                    def _():
                        x_copy(3).wait_recv()
                        halo_wait(3)

                    @rarely(i >= 19)
                    def _():
                        for h in range(2):
                            hid_store(0, h).wait()

                    @rarely(i >= 27)
                    def _():
                        for d in range(2):
                            j, par = jp(i - 27 + d)
                            for h in range(2):
                                a = 4 * j + 2 * par + h

                                @pl.when(blk > 0)
                                def _():
                                    hid_up(a).start()

                                @pl.when(blk < 3)
                                def _():
                                    hid_dn(a).start()

                    @rarely(i == 31)
                    def _():
                        pass_w2_x(jnp.int32(0))

            @rarely(i >= 34)
            def _():
                @rarely(i == 36)
                def _():
                    send_w2_x(jnp.int32(3))

                @rarely((i < 44) & ((i & 3) == 3))
                def _():
                    pass_w2_x(((i - 31) >> 2))

                @rarely((i >= 37) & ((i & 3) == 1))
                def _():
                    pass_w2_y(((i - 37) >> 2))

        def taps(xs_slot, ws_slot, col, lanes=slice(None)):
            total = None
            for dx in (-1, 0, 1):
                if not 0 <= col + dx < cols:
                    continue
                for dy in range(3):
                    lhs = xa[xs_slot, dy:dy + rows, col + dx].reshape(m_rows, cb)
                    prod = jnp.dot(lhs, wv[ws_slot, dy, dx + 1, :, lanes], preferred_element_type=jnp.float32)
                    total = prod if total is None else total + prod
            return total

        def step(i, carry):
            ph1 = i < 16
            ph3 = i >= 32
            n = jnp.where(ph3, ((i - 32) >> 4), 0)
            q = jnp.where(ph3, ((i - 32) & 15), 0)
            m, role = near_step(i)
            m = jnp.where(ph1, m, ((i - 16) >> 1))
            role = jnp.where(ph1, role, 2 + (i & 1))
            p = jnp.where(ph1, p_of(m), (m & 7))
            p = jnp.where(ph3, 0, p)
            last = jnp.where(ph3, q == 15, role == 3)
            first = jnp.where(ph3, q == 0, role == 0)
            a_slot = jnp.where(ph3, n, (p & 1))
            x_slot = jnp.where(ph3, 4 + (q & 1), role)
            w_slot = (i & 1)

            events(i)
            issue(i + 1)
            w_load(g1.at[0, 0, 0], i).wait()

            @pl.when(ph3)
            def _():
                hid_load(0, q).wait()

            @rarely((i >= 4) & (i < 32))
            def _():
                @pl.when(ph1 & first)
                def _():
                    pltpu.make_async_copy(acc.at[a_slot], part.at[0], pst.at[a_slot]).wait()

                @pl.when((i >= 20) & (role == 2))
                def _():
                    pltpu.make_async_copy(part.at[0], acc.at[a_slot], pld.at[a_slot]).wait()

            @pl.when(jnp.logical_not(last))
            def _():
                for col in range(cols):
                    total = taps(x_slot, w_slot, col)
                    acc[a_slot, col] = total + jnp.where(first, 0.0, acc[a_slot, col])

                @rarely((i < 12) & (role == 1))
                def _():
                    pltpu.make_async_copy(acc.at[a_slot], part.at[p], pst.at[a_slot]).start()

            def finish_hidden():
                @pl.when((i == 17) & edge)
                def _():
                    zero_rows(0).wait()

                j, par = jp(p)
                shift = shifts[tile_of(x, j, par)]
                for col in range(cols):
                    val = jnp.maximum(taps(x_slot, w_slot, col) + acc[a_slot, col] + shift, 0.0).astype(jnp.bfloat16)
                    for h in range(2):
                        stage[h, :, col] = val[:, h * cb:(h + 1) * cb].reshape(rows, ni, cb)
                for h in range(2):
                    hid_store(4 * j + 2 * par + h, h).start()

                @pl.when(p < 6)
                def _():
                    pltpu.make_async_copy(part.at[p + 2], acc.at[a_slot], pld.at[a_slot]).start()

            def finish_out():
                @pl.when(n == 1)
                def _():
                    for h in range(2):
                        y_far(h).wait_send()

                def half_step(same, carry):
                    h = jnp.where(same == 1, c, 1 - c)
                    lanes = pl.ds(pl.multiple_of(h * cb, cb), cb)
                    for col in range(cols):
                        total = taps(x_slot, w_slot, col, lanes) + acc[a_slot, col, :, lanes]
                        res = xa[3 - 2 * n - same, 1:rows + 1, col].reshape(m_rows, cb).astype(jnp.float32)
                        stage[h, :, col] = (total + res).astype(jnp.bfloat16).reshape(rows, ni, cb)

                    @pl.when(n == 0)
                    def _():
                        y_far(h).start()

                    @pl.when((n == 1) & (same == 0))
                    def _():
                        y_near().start()

                    return carry

                lax.fori_loop(0, 2, half_step, 0)

                @pl.when(n == 1)
                def _():
                    y_own().start()

            @pl.when(last)
            def _():
                pl.when(jnp.logical_not(ph3))(finish_hidden)
                pl.when(ph3)(finish_out)

            return carry

        lax.fori_loop(0, N_STEPS, step, 0)

        def drain(e, carry):
            hi, lo = pair(e)
            w1_part(hi, lo).wait_send()
            for hf in (lo, lo + 2):
                w1_x(hi, hf).wait_send()
                w1_y(hi, hf).wait_send()
            for hf in range(4):
                w1_fwd(hi, lo, hf).wait_send()
            n, par = e >> 2, (e >> 1) & 1
            w2_part(n, par, lo).wait_send()
            w2_fwd(n, par, lo).wait_send()
            return carry

        lax.fori_loop(0, 8, drain, 0)

        def drain_rows(a, carry):
            @pl.when(blk > 0)
            def _():
                hid_up(a).wait_send()

            @pl.when(blk < 3)
            def _():
                hid_dn(a).wait_send()

            return carry

        lax.fori_loop(0, 16, drain_rows, 0)

        def drain_two(e, carry):
            w2_x(*pair(e)).wait_send()
            w2_y(*pair(e)).wait_send()
            return carry

        lax.fori_loop(0, 4, drain_two, 0)
        for e in range(2):
            remote(stage.at[0], yt.at[0, pl.ds(0, rows)], ys.at[0], yr.at[e], sp, k).wait_recv()
        y_near().wait()
        y_own().wait()

    dma = pltpu.SemaphoreType.DMA
    bf16, f32 = jnp.bfloat16, jnp.float32
    any_space = pl.BlockSpec(memory_space=pl.ANY)
    outs = pl.pallas_call(
        kernel,
        out_shape=[
            jax.ShapeDtypeStruct((2, h_loc, cols, ni, cb), bf16),
            jax.ShapeDtypeStruct((3, 4, 2, 3, 3, cb, tile), bf16),
            jax.ShapeDtypeStruct((3, 2, 2, 2, 3, 3, cb, tile), bf16),
            jax.ShapeDtypeStruct((8, cols, m_rows, tile), f32),
            jax.ShapeDtypeStruct((16, rows + 2, cols, ni, cb), bf16),
        ],
        in_specs=[any_space] * 4,
        out_specs=[any_space] * 5,
        scratch_shapes=[
            pltpu.VMEM((7, rows + 2, cols, ni, cb), bf16),
            pltpu.VMEM((2, cols, m_rows, tile), f32),
            pltpu.VMEM((2, 3, 3, cb, tile), bf16),
            pltpu.VMEM((2, rows, cols, ni, cb), bf16),
            pltpu.VMEM((2, ni, cols, h_loc, cb), bf16),
            pltpu.VMEM((ni * ni, ni * ni), bf16),
            pltpu.VMEM((8, 128), f32),
            pltpu.VMEM(bias.shape, f32),
            dma(ONE),
            *map(dma, SEMS),
        ],
        compiler_params=pltpu.CompilerParams(collective_id=0, has_side_effects=True, vmem_limit_bytes=63 * MIB),
        name="fused_block",
    )(xw, w_one, w_two, bias)
    return outs[0]


def images_major(yt):
    groups, h_loc, cols, ni, cb = yt.shape
    parts = h_loc // ni
    width = cols // 2
    chunks = groups * parts * 2
    assert ni == 16

    def kernel(y, out, y_in, y_out, swap, in_sem, out_sem):
        def place(e):
            block, side = pair(e)
            group, part = lax.div(block, parts), lax.rem(block, parts)
            n0, h0 = pl.multiple_of(ni * group, ni), pl.multiple_of(ni * part, ni)
            return group, n0, h0, width * side

        def load(e):
            group, _, h0, col = place(e)
            cut = (group, pl.ds(h0, ni), pl.ds(col, width))
            return pltpu.make_async_copy(y.at[cut], y_in.at[cut], in_sem.at[e])

        def store(e):
            _, n0, h0, col = place(e)
            cut = (pl.ds(n0, ni), pl.ds(col, width), pl.ds(h0, ni))
            return pltpu.make_async_copy(y_out.at[cut], out.at[cut], out_sem.at[e])

        for e in range(chunks):
            load(jnp.int32(e)).start()
        swap[...] = swap_matrix(ni)

        def chunk(e, carry):
            load(e).wait()
            group, n0, h0, base = place(e)
            for col in range(width):
                rows_in = y_in[group, pl.ds(h0, ni), base + col].reshape(ni * ni, cb)
                res = jnp.dot(swap[...], rows_in, preferred_element_type=jnp.float32)
                y_out[pl.ds(n0, ni), base + col, pl.ds(h0, ni)] = res.astype(jnp.bfloat16).reshape(ni, ni, cb)
            store(e).start()
            return carry

        lax.fori_loop(0, chunks, chunk, 0)
        for e in range(chunks):
            store(jnp.int32(e)).wait()

    dma = pltpu.SemaphoreType.DMA
    out_shape = (groups * ni, cols, h_loc, cb)
    return pl.pallas_call(
        kernel,
        out_shape=jax.ShapeDtypeStruct(out_shape, jnp.bfloat16),
        in_specs=[pl.BlockSpec(memory_space=pl.ANY)],
        out_specs=pl.BlockSpec(memory_space=pl.ANY),
        scratch_shapes=[pltpu.VMEM(yt.shape, jnp.bfloat16), pltpu.VMEM(out_shape, jnp.bfloat16), pltpu.VMEM((ni * ni, ni * ni), jnp.bfloat16),
                        dma((chunks,)), dma((chunks,))],
        compiler_params=pltpu.CompilerParams(vmem_limit_bytes=63 * MIB),
        name="images_major",
    )(yt)


def solution(mesh):
    act_spec = P("dp", "sp", None, "cp")
    kernel_spec = P(None, None, "cp", None)

    def local_block(x_tile, w_one_part, w_two_part, bias_one):
        xw = x_tile.transpose(0, 2, 1, 3)
        yt = fused_block(xw, w_one_part, w_two_part, bias_one.reshape(8, 1, 2 * x_tile.shape[3]))
        return images_major(yt).transpose(0, 2, 1, 3)

    return jax.shard_map(local_block, mesh=mesh, in_specs=(act_spec, kernel_spec, kernel_spec, P()), out_specs=act_spec, check_vma=False)
```

```python
import functools

import jax
import jax.numpy as jnp
from jax import lax
from jax.experimental import pallas as pl
from jax.experimental.pallas import tpu as pltpu
from jax.sharding import PartitionSpec as P

MESH = pl.DeviceIdType.MESH
N_STEPS = 64
MIB = 1024 * 1024
ONE, TWO, THREE, FOUR, ALL = (1,), (2,), (3,), (4,), (2, 16)
GRID, CUBE, HALVES = (2, 2), (2, 2, 2), (4, 2)
QUARTERS, ROWS = (4, 4), (4, 2, 4)
SEMS = (
    TWO, TWO, TWO, TWO, TWO, ONE, (2, 3), THREE, THREE, TWO, FOUR,
    ONE, HALVES, ONE, QUARTERS, ONE, QUARTERS, ONE, ROWS,
    ONE, CUBE, ONE, GRID, ONE, GRID, ONE, CUBE,
    TWO, ALL, TWO, TWO, ONE, ONE, ONE,
)


def pair(e):
    return e >> 1, e & 1


def each(first, stop, act):
    lax.fori_loop(first, stop, lambda e, carry: (act(e), carry)[1], 0)


def odd(i):
    return (i & 1) == 1


def swap_matrix(n):
    shift = n.bit_length() - 1
    to = lax.broadcasted_iota(jnp.int32, (n * n, n * n), 0)
    frm = lax.broadcasted_iota(jnp.int32, (n * n, n * n), 1)
    hit = ((to >> shift) == (frm & (n - 1))) & ((to & (n - 1)) == (frm >> shift))
    return jnp.where(hit, 1.0, 0.0).astype(jnp.bfloat16)


def fused_block(xw, w_one, w_two, bias):
    images, cols, h_loc, cb = xw.shape
    ni = images // 2
    rows = h_loc // 2
    m_rows = rows * ni
    tile = 2 * cb
    assert ni == 16 and h_loc == 48

    def remote(src, dst, send_sem, recv_sem, sp, cp):
        return pltpu.make_async_remote_copy(src_ref=src, dst_ref=dst, send_sem=send_sem, recv_sem=recv_sem,
                                            device_id={"sp": sp, "cp": cp}, device_id_type=MESH)

    def kernel(xw, w1, w2, b1, yt, g1, g2, part, hid,
               xa, acc, wv, stage, raw, swap, mark, shifts, bsem,
               wsem, asem, pst, pld, stl, zsem, rsem, xs, xr, hs, hr,
               p1s, p1r, x1s, x1r, y1s, y1r, f1s, f1r,
               p2s, p2r, x2s, x2r, y2s, y2r, f2s, f2r,
               as_, ar, ys, yr, zs, zr, yl):
        sp = lax.axis_index("sp")
        k = lax.axis_index("cp")
        x = (k >> 1)
        c = (k & 1)
        blk = 2 * sp + c
        osp = 1 - sp
        k1 = 2 * x + (1 - c)
        k2 = 2 * (1 - x) + c
        k3 = 2 * (1 - x) + (1 - c)

        def rarely(cond):
            def wrap(body):
                @pl.when(cond)
                def _():
                    mark[...] = jnp.zeros(mark.shape, jnp.float32)
                    body()

            return wrap

        def tile_of(xx, j, par):
            return 4 * ((xx + (j >> 1)) & 1) + 2 * (j & 1) + par

        barrier = pltpu.get_barrier_semaphore()
        for to_sp, to_cp in ((sp, k1), (sp, k2), (sp, k3), (osp, k), (osp, k1)):
            pl.semaphore_signal(barrier, inc=1, device_id={"sp": to_sp, "cp": to_cp}, device_id_type=MESH)

        def raw_load(far, part):
            cut = pl.ds(pl.multiple_of(ni * part, ni), ni)
            group = pl.ds(ni * (1 - x if far else x), ni)
            return pltpu.make_async_copy(xw.at[group, :, cut], raw.at[far, :, :, cut], rsem.at[far, part])

        def block(far, col, part):
            rows_in = raw[far, :, col, pl.ds(pl.multiple_of(ni * part, ni), ni), :].reshape(ni * ni, cb)
            out = jnp.dot(swap[...], rows_in, preferred_element_type=jnp.float32)
            return out.astype(jnp.bfloat16).reshape(ni, ni, cb)

        def slot_of(far, cc):
            return jnp.where(cc == c, 5 if far else 0, 6 if far else 4)

        def swap_end(far, cc):
            for col in range(cols):
                xa[slot_of(far, cc), pl.ds(1 + 8 * cc, ni), col] = block(far, col, 2 * cc)

        def swap_mid(far):
            for col in range(cols):
                mid = block(far, col, 1)
                xa[slot_of(far, 0), 17:26, col] = mid[0:9]
                xa[slot_of(far, 1), 0:9, col] = mid[7:16]

        def x_copy(role):
            cc = c if role == 2 else 1 - c
            cut = pl.ds(1 - cc, rows + 1)
            return remote(xa.at[3 + role, cut], xa.at[role, cut], xs.at[role - 1], xr.at[role - 1], sp,
                          {1: k1, 2: k2, 3: k3}[role])

        def halo_copy(far):
            xx = 1 - x if far else x
            role = 2 * ((x + xx) & 1) + ((c + sp) & 1)
            src = xa.at[slot_of(far, osp), jnp.where(sp == 0, rows, 1)]
            return remote(src, xa.at[role, (rows + 1) * sp], hs.at[far], hr.at[role], osp, 2 * xx + sp)

        def bias_load():
            return pltpu.make_async_copy(b1, shifts, bsem.at[0])

        piece = cb // 4

        def w1_own(j, par, xx):
            return w1.at[:, :, :, pl.ds(pl.multiple_of(tile_of(xx, j, par) * tile, tile), tile)]

        def w1_part(j, par):
            return remote(w1_own(j, par, x), g1.at[0, j, par], p1s.at[0], p1r.at[j, par], sp, k1)

        def w1_x(j, hf):
            cut = pl.ds(pl.multiple_of(hf * piece, piece), piece)
            src = w1.at[:, :, cut, pl.ds(pl.multiple_of(tile_of(1 - x, j, sp) * tile, tile), tile)]
            return remote(src, g1.at[1, j, sp, :, :, cut], x1s.at[0], x1r.at[j, hf], sp, k2)

        def w1_y(j, hf):
            cut = pl.ds(pl.multiple_of(hf * piece, piece), piece)
            ref = g1.at[1, j, sp, :, :, cut]
            return remote(ref, ref, y1s.at[0], y1r.at[j, hf], osp, k)

        def w1_fwd(j, par, hf):
            cut = pl.ds(pl.multiple_of(hf * piece, piece), piece)
            return remote(g1.at[1, j, par, :, :, cut], g1.at[2, j, par, :, :, cut], f1s.at[0], f1r.at[j, par, hf], sp, k1)

        def w2_cut(n, par, h, xx):
            row = pl.multiple_of(par * tile + h * cb, cb)
            col = pl.multiple_of(tile * ((1 + xx + n) & 1), tile)
            return w2.at[:, :, pl.ds(row, cb), pl.ds(col, tile)]

        def w2_part(n, par, h):
            return remote(w2_cut(n, par, h, x), g2.at[0, n, par, h], p2s.at[0], p2r.at[n, par, h], sp, k1)

        def w2_x(n, h):
            return remote(w2_cut(n, sp, h, 1 - x), g2.at[1, n, sp, h], x2s.at[0], x2r.at[n, h], sp, k2)

        def w2_y(n, h):
            ref = g2.at[1, n, sp, h]
            return remote(ref, ref, y2s.at[0], y2r.at[n, h], osp, k)

        def w2_fwd(n, par, h):
            return remote(g2.at[1, n, par, h], g2.at[2, n, par, h], f2s.at[0], f2r.at[n, par, h], sp, k1)

        up_blk = lax.max(blk - 1, 0)
        dn_blk = lax.min(blk + 1, 3)

        def hid_up(a):
            return remote(hid.at[a, 1], hid.at[a, rows + 1], as_.at[0], ar.at[1, a], (up_blk >> 1), 2 * x + (up_blk & 1))

        def hid_dn(a):
            return remote(hid.at[a, rows], hid.at[a, 0], as_.at[1], ar.at[0, a], (dn_blk >> 1), 2 * x + (dn_blk & 1))

        def hid_store(a, h):
            return pltpu.make_async_copy(stage.at[h], hid.at[a, pl.ds(1, rows)], stl.at[h])

        y_rows = pl.ds(rows * c, rows)

        def y_far(h):
            return remote(stage.at[h], yt.at[x, y_rows], ys.at[h], yr.at[((h + c) & 1)], sp, 2 * (1 - x) + h)

        def y_near():
            return remote(stage.at[1 - c], yt.at[x, y_rows], zs.at[0], zr.at[0], sp, k1)

        def y_own():
            return pltpu.make_async_copy(stage.at[c], yt.at[x, y_rows], yl.at[0])

        def zero_rows(row):
            return pltpu.make_async_copy(stage.at[0, pl.ds(0, 16)], hid.at[:, row], zsem.at[0])

        def p_of(m):
            return (m + 2) & 7

        def jp(p):
            return p >> 1, (sp + p) & 1

        def send_w1_x(e):
            w1_x(e >> 2, e & 3).start()

        def near_step(i):
            return 2 * (i >> 2) + (i & 1), (i & 2) >> 1

        def halo_wait(role):
            @pl.when(c != sp)
            def _():
                remote(xa.at[0, 0], xa.at[role, 0], hs.at[0], hr.at[role], osp, k).wait_recv()

        for part_no in (2 * osp, 2 * sp, 1):
            raw_load(0, part_no).start()
        swap[...] = swap_matrix(ni)
        edge = c == sp

        @pl.when(edge)
        def _():
            xa[0:4, (rows + 1) * sp] = jnp.zeros((4, cols, ni, cb), jnp.bfloat16)

        def w_load(src, t):
            return pltpu.make_async_copy(src, wv.at[(t & 1)], wsem.at[(t & 1)])

        def hid_load(a, q):
            slot = (q & 1)
            return pltpu.make_async_copy(hid.at[a], xa.at[4 + slot], asem.at[slot])

        def issue(t):
            @rarely(t < 16)
            def _():
                m, role = near_step(t)
                j, par = jp(p_of(m))

                @rarely(role == 0)
                def _():
                    w_load(w1_own(j, par, x), t).start()

                @rarely(role == 1)
                def _():
                    w1_part(j, par).wait_recv()
                    w_load(g1.at[0, j, par], t).start()

            @rarely((t >= 16) & (t < 32))
            def _():
                j, par = jp(((t - 16) >> 1))

                @rarely((t & 1) == 1)
                def _():
                    for hf in range(4):
                        w1_fwd(j, par, hf).wait_recv()

                w_load(g1.at[1 + (t & 1), j, par], t).start()

            @rarely((t >= 32) & (t < N_STEPS))
            def _():
                n = ((t - 32) >> 4)
                q = ((t - 32) & 15)
                h = (q & 1)
                p = (q >> 1)
                j, par = jp(p)
                a = 4 * j + 2 * par + h
                same = (j & 1) == c

                @rarely(n == 0)
                def _():
                    @pl.when(blk > 0)
                    def _():
                        hid_dn(a).wait_recv()

                    @pl.when(blk < 3)
                    def _():
                        hid_up(a).wait_recv()

                hid_load(a, q).start()

                own = (p < 4) & same

                @rarely(own)
                def _():
                    w_load(w2_cut(n, par, h, x), t).start()

                @rarely(jnp.logical_not(own))
                def _():
                    @pl.when(p < 4)
                    def _():
                        w2_part(n, par, h).wait_recv()

                    @pl.when((p >= 4) & jnp.logical_not(same))
                    def _():
                        w2_fwd(n, par, h).wait_recv()

                    w_load(g2.at[jnp.where(p < 4, 0, jnp.where(same, 1, 2)), n, par, h], t).start()

        raw_load(0, 2 * osp).wait()
        issue(jnp.int32(0))
        for part_no in range(3):
            raw_load(1, part_no).start()
        bias_load().start()
        swap_end(0, osp)
        pl.semaphore_wait(barrier, 5)

        @pl.when(edge)
        def _():
            halo_copy(0).start()

        each(0, 6, send_w1_x)
        raw_load(0, 2 * sp).wait()
        raw_load(0, 1).wait()
        swap_end(0, sp)
        swap_mid(0)
        x_copy(1).start()
        for m in range(2):
            w1_part(*jp(jnp.int32(m + 2))).start()
        for part_no in range(3):
            raw_load(1, part_no).wait()
        for cc in range(2):
            swap_end(1, cc)
        swap_mid(1)
        halo_wait(0)

        def pass_w1_x(e):
            j, hf = e >> 2, e & 3
            w1_x(j, hf).wait_recv()
            w1_y(j, hf).start()
            w1_fwd(j, sp, hf).start()

        def pass_w1_y(e):
            j, hf = e >> 2, e & 3
            w1_y(j, hf).wait_recv()
            w1_fwd(j, osp, hf).start()

        def pass_w2_x(e):
            n, h = pair(e)
            w2_x(n, h).wait_recv()
            w2_y(n, h).start()
            w2_fwd(n, sp, h).start()

        def pass_w2_y(e):
            n, h = pair(e)
            w2_y(n, h).wait_recv()
            w2_fwd(n, osp, h).start()

        def send_w2_x(e):
            w2_x(*pair(e)).start()

        def events(i):
            @rarely(i < 50)
            def _():
                early_events(i)

        def early_events(i):
            is_odd = odd(i)
            even = jnp.logical_not(is_odd)

            @rarely(i < 16)
            def _():
                @rarely(even)
                def _():
                    @rarely(i < 12)
                    def _():
                        w1_part(*jp(p_of((i >> 1) + 2))).start()

                    @rarely(i == 2)
                    def _():
                        x_copy(1).wait_recv()
                        halo_wait(1)

                    @rarely(i == 10)
                    def _():
                        each(0, 4, pass_w1_y)

                    @rarely(i == 12)
                    def _():
                        each(4, 6, pass_w1_y)

                @rarely(is_odd)
                def _():
                    @rarely(i == 1)
                    def _():
                        @rarely(c != sp)
                        def _():
                            halo_copy(0).start()

                        @rarely(edge)
                        def _():
                            stage[0, 0:16] = jnp.zeros((16, cols, ni, cb), jnp.bfloat16)
                            zero_rows((rows + 1) * sp).start()

                    @rarely(i == 3)
                    def _():
                        x_copy(2).start()

                    @rarely(i == 5)
                    def _():
                        each(0, 4, pass_w1_x)

                    @rarely(i == 7)
                    def _():
                        each(4, 6, pass_w1_x)
                        halo_copy(1).start()

                    @rarely(i == 9)
                    def _():
                        x_copy(3).start()

            @rarely((i >= 13) & (i < 23))
            def _():
                send_w1_x(i - 7)

            @rarely((i >= 16) & (i < 34))
            def _():
                @rarely((i >= 18) & (i < 28))
                def _():
                    pass_w1_x(i - 12)

                @rarely((i >= 20) & (i < 30))
                def _():
                    pass_w1_y(i - 14)

                @rarely(i < 24)
                def _():
                    e = i - 16
                    w2_part((e >> 2), ((e >> 1) & 1), (e & 1)).start()

                @rarely(even)
                def _():
                    @rarely(i == 16)
                    def _():
                        bias_load().wait()
                        x_copy(2).wait_recv()
                        halo_wait(2)

                    @rarely(i == 30)
                    def _():
                        x_copy(1).wait_send()
                        x_copy(2).wait_send()
                        x_copy(3).wait_send()
                        for far in range(2):
                            halo_copy(far).wait_send()

                    @rarely((i >= 24) & ((i & 3) == 0))
                    def _():
                        send_w2_x(((i - 24) >> 2))

                @rarely(is_odd)
                def _():
                    @rarely(i == 17)
                    def _():
                        x_copy(3).wait_recv()
                        halo_wait(3)

                    @rarely(i >= 19)
                    def _():
                        for h in range(2):
                            hid_store(0, h).wait()

                    @rarely(i >= 27)
                    def _():
                        for d in range(2):
                            j, par = jp(i - 27 + d)
                            for h in range(2):
                                a = 4 * j + 2 * par + h

                                @pl.when(blk > 0)
                                def _():
                                    hid_up(a).start()

                                @pl.when(blk < 3)
                                def _():
                                    hid_dn(a).start()

                    @rarely(i == 31)
                    def _():
                        pass_w2_x(jnp.int32(0))

            @rarely(i >= 34)
            def _():
                @rarely(i == 36)
                def _():
                    send_w2_x(jnp.int32(3))

                @rarely((i < 44) & ((i & 3) == 3))
                def _():
                    pass_w2_x(((i - 31) >> 2))

                @rarely((i >= 37) & ((i & 3) == 1))
                def _():
                    pass_w2_y(((i - 37) >> 2))

        def taps(xs_slot, ws_slot, col, lanes=slice(None)):
            total = None
            for dx in (-1, 0, 1):
                if not 0 <= col + dx < cols:
                    continue
                for dy in range(3):
                    lhs = xa[xs_slot, dy:dy + rows, col + dx].reshape(m_rows, cb)
                    prod = jnp.dot(lhs, wv[ws_slot, dy, dx + 1, :, lanes], preferred_element_type=jnp.float32)
                    total = prod if total is None else total + prod
            return total

        def step(i, carry):
            ph1 = i < 16
            ph3 = i >= 32
            n = jnp.where(ph3, ((i - 32) >> 4), 0)
            q = jnp.where(ph3, ((i - 32) & 15), 0)
            m, role = near_step(i)
            m = jnp.where(ph1, m, ((i - 16) >> 1))
            role = jnp.where(ph1, role, 2 + (i & 1))
            p = jnp.where(ph1, p_of(m), (m & 7))
            p = jnp.where(ph3, 0, p)
            last = jnp.where(ph3, q == 15, role == 3)
            first = jnp.where(ph3, q == 0, role == 0)
            a_slot = jnp.where(ph3, n, (p & 1))
            x_slot = jnp.where(ph3, 4 + (q & 1), role)
            w_slot = (i & 1)

            events(i)
            issue(i + 1)
            w_load(g1.at[0, 0, 0], i).wait()

            @pl.when(ph3)
            def _():
                hid_load(0, q).wait()

            @rarely((i >= 4) & (i < 32))
            def _():
                @pl.when(ph1 & first)
                def _():
                    pltpu.make_async_copy(acc.at[a_slot], part.at[0], pst.at[a_slot]).wait()

                @pl.when((i >= 20) & (role == 2))
                def _():
                    pltpu.make_async_copy(part.at[0], acc.at[a_slot], pld.at[a_slot]).wait()

            @pl.when(jnp.logical_not(last))
            def _():
                for col in range(cols):
                    total = taps(x_slot, w_slot, col)
                    acc[a_slot, col] = total + jnp.where(first, 0.0, acc[a_slot, col])

                @rarely((i < 12) & (role == 1))
                def _():
                    pltpu.make_async_copy(acc.at[a_slot], part.at[p], pst.at[a_slot]).start()

            def finish_hidden():
                @pl.when((i == 17) & edge)
                def _():
                    zero_rows(0).wait()

                j, par = jp(p)
                shift = shifts[tile_of(x, j, par)]
                for col in range(cols):
                    val = jnp.maximum(taps(x_slot, w_slot, col) + acc[a_slot, col] + shift, 0.0).astype(jnp.bfloat16)
                    for h in range(2):
                        stage[h, :, col] = val[:, h * cb:(h + 1) * cb].reshape(rows, ni, cb)
                for h in range(2):
                    hid_store(4 * j + 2 * par + h, h).start()

                @pl.when(p < 6)
                def _():
                    pltpu.make_async_copy(part.at[p + 2], acc.at[a_slot], pld.at[a_slot]).start()

            def finish_out():
                @pl.when(n == 1)
                def _():
                    for h in range(2):
                        y_far(h).wait_send()

                def half_step(same, carry):
                    h = jnp.where(same == 1, c, 1 - c)
                    lanes = pl.ds(pl.multiple_of(h * cb, cb), cb)
                    for col in range(cols):
                        total = taps(x_slot, w_slot, col, lanes) + acc[a_slot, col, :, lanes]
                        res = xa[3 - 2 * n - same, 1:rows + 1, col].reshape(m_rows, cb).astype(jnp.float32)
                        stage[h, :, col] = (total + res).astype(jnp.bfloat16).reshape(rows, ni, cb)

                    @pl.when(n == 0)
                    def _():
                        y_far(h).start()

                    @pl.when((n == 1) & (same == 0))
                    def _():
                        y_near().start()

                    return carry

                lax.fori_loop(0, 2, half_step, 0)

                @pl.when(n == 1)
                def _():
                    y_own().start()

            @pl.when(last)
            def _():
                pl.when(jnp.logical_not(ph3))(finish_hidden)
                pl.when(ph3)(finish_out)

            return carry

        lax.fori_loop(0, N_STEPS, step, 0)

        for ref, sem in ((g1.at[0], p1s), (g1.at[1, :, 0], x1s), (g1.at[1, :, 0], y1s), (g1.at[2], f1s),
                         (g2.at[0], p2s), (g2.at[1, :, 0], x2s), (g2.at[1, :, 0], y2s), (g2.at[2], f2s)):
            remote(ref, ref, sem.at[0], zr.at[0], sp, k1).wait_send()

        @pl.when(blk > 0)
        def _():
            remote(hid.at[:, 0], hid.at[:, 0], as_.at[0], zr.at[0], sp, k1).wait_send()

        @pl.when(blk < 3)
        def _():
            remote(hid.at[:, 0], hid.at[:, 0], as_.at[1], zr.at[0], sp, k1).wait_send()

        for e in range(2):
            remote(stage.at[0], yt.at[0, pl.ds(0, rows)], ys.at[0], yr.at[e], sp, k).wait_recv()
        y_near().wait()
        y_own().wait()

    dma = pltpu.SemaphoreType.DMA
    bf16, f32 = jnp.bfloat16, jnp.float32
    any_space = pl.BlockSpec(memory_space=pl.ANY)
    outs = pl.pallas_call(
        kernel,
        out_shape=[
            jax.ShapeDtypeStruct((2, h_loc, cols, ni, cb), bf16),
            jax.ShapeDtypeStruct((3, 4, 2, 3, 3, cb, tile), bf16),
            jax.ShapeDtypeStruct((3, 2, 2, 2, 3, 3, cb, tile), bf16),
            jax.ShapeDtypeStruct((8, cols, m_rows, tile), f32),
            jax.ShapeDtypeStruct((16, rows + 2, cols, ni, cb), bf16),
        ],
        in_specs=[any_space] * 4,
        out_specs=[any_space] * 5,
        scratch_shapes=[
            pltpu.VMEM((7, rows + 2, cols, ni, cb), bf16),
            pltpu.VMEM((2, cols, m_rows, tile), f32),
            pltpu.VMEM((2, 3, 3, cb, tile), bf16),
            pltpu.VMEM((2, rows, cols, ni, cb), bf16),
            pltpu.VMEM((2, ni, cols, h_loc, cb), bf16),
            pltpu.VMEM((ni * ni, ni * ni), bf16),
            pltpu.VMEM((8, 128), f32),
            pltpu.VMEM(bias.shape, f32),
            dma(ONE),
            *map(dma, SEMS),
        ],
        compiler_params=pltpu.CompilerParams(collective_id=0, has_side_effects=True, vmem_limit_bytes=63 * MIB),
        name="fused_block",
    )(xw, w_one, w_two, bias)
    return outs[0]


def images_major(yt):
    groups, h_loc, cols, ni, cb = yt.shape
    parts = h_loc // ni
    width = cols // 2
    chunks = groups * parts * 2
    assert ni == 16

    def kernel(y, out, y_in, y_out, swap, in_sem, out_sem):
        def place(e):
            block, side = pair(e)
            group, part = lax.div(block, parts), lax.rem(block, parts)
            n0, h0 = pl.multiple_of(ni * group, ni), pl.multiple_of(ni * part, ni)
            return group, n0, h0, width * side

        def load(e):
            group, _, h0, col = place(e)
            cut = (group, pl.ds(h0, ni), pl.ds(col, width))
            return pltpu.make_async_copy(y.at[cut], y_in.at[cut], in_sem.at[e])

        def store(e):
            _, n0, h0, col = place(e)
            cut = (pl.ds(n0, ni), pl.ds(col, width), pl.ds(h0, ni))
            return pltpu.make_async_copy(y_out.at[cut], out.at[cut], out_sem.at[e])

        for e in range(chunks):
            load(jnp.int32(e)).start()
        swap[...] = swap_matrix(ni)

        def chunk(e, carry):
            load(e).wait()
            group, n0, h0, base = place(e)
            for col in range(width):
                rows_in = y_in[group, pl.ds(h0, ni), base + col].reshape(ni * ni, cb)
                res = jnp.dot(swap[...], rows_in, preferred_element_type=jnp.float32)
                y_out[pl.ds(n0, ni), base + col, pl.ds(h0, ni)] = res.astype(jnp.bfloat16).reshape(ni, ni, cb)
            store(e).start()
            return carry

        lax.fori_loop(0, chunks, chunk, 0)
        for e in range(chunks):
            store(jnp.int32(e)).wait()

    dma = pltpu.SemaphoreType.DMA
    out_shape = (groups * ni, cols, h_loc, cb)
    return pl.pallas_call(
        kernel,
        out_shape=jax.ShapeDtypeStruct(out_shape, jnp.bfloat16),
        in_specs=[pl.BlockSpec(memory_space=pl.ANY)],
        out_specs=pl.BlockSpec(memory_space=pl.ANY),
        scratch_shapes=[pltpu.VMEM(yt.shape, jnp.bfloat16), pltpu.VMEM(out_shape, jnp.bfloat16), pltpu.VMEM((ni * ni, ni * ni), jnp.bfloat16),
                        dma((chunks,)), dma((chunks,))],
        compiler_params=pltpu.CompilerParams(vmem_limit_bytes=63 * MIB),
        name="images_major",
    )(yt)


def solution(mesh):
    act_spec = P("dp", "sp", None, "cp")
    kernel_spec = P(None, None, "cp", None)

    def local_block(x_tile, w_one_part, w_two_part, bias_one):
        xw = x_tile.transpose(0, 2, 1, 3)
        yt = fused_block(xw, w_one_part, w_two_part, bias_one.reshape(8, 1, 2 * x_tile.shape[3]))
        return images_major(yt).transpose(0, 2, 1, 3)

    return jax.shard_map(local_block, mesh=mesh, in_specs=(act_spec, kernel_spec, kernel_spec, P()), out_specs=act_spec, check_vma=False)
```
